8 devices in a mesh: data: 2 (over z, y), expert: 4 (over x, core).
Axes of the slice: x: 2, y: 2, z: 1, core: 2. Of those that a mesh axis runs over, the one named last changes fastest.
Arguments:
- x_in: bfloat16 [1024, 1024], P(('data', 'expert')), parts along dimension 0
- expert_idx: int32 [1024, 8], P(('data', 'expert')), parts along dimension 0
- gate_weight: float32 [1024, 8], P(('data', 'expert')), parts along dimension 0
- grad_y: bfloat16 [1024, 1024], P(('data', 'expert')), parts along dimension 0
- w_in: bfloat16 [128, 1024, 384], P('expert')
- w_out: bfloat16 [128, 384, 1024], P('expert')
Outputs:
- output 1: bfloat16 [1024, 1024], P(('data', 'expert')), parts along dimension 0
- output 2: bfloat16 [1024, 1024], P(('data', 'expert')), parts along dimension 0
- output 3: float32 [1024, 8], P(('data', 'expert')), parts along dimension 0
- output 4: bfloat16 [256, 1024, 384], P(('data', 'expert')), parts along dimension 0
- output 5: bfloat16 [256, 384, 1024], P(('data', 'expert')), parts along dimension 0
There are 2 independent parts. The reference program is written for one: setup_inputs(seed, part) draws one part's arguments, and reference() takes and returns one part's arrays. A program takes and returns all parts, laid end to end along the dimension named above; an argument that names none is the same for every part.
All inputs are finite; a program needn't handle non-finite values.
Results may differ from the reference program's by a relative error of at most 0.0102157.
Values are sent between devices in bfloat16 or wider.
A program may use at most 1 GiB of HBM per device.

```python
import jax
import jax.numpy as jnp
from jax import lax

TOKENS = 128
GROUP_SIZE = 4
D_MODEL = 1024
D_FF = 384
EXPERTS = 128
TOP_K = 8
CAPACITY = 40

LOCAL_EXPERTS = EXPERTS // GROUP_SIZE
DEVICE_PAIRS = TOKENS * TOP_K
FAIR_SHARE = DEVICE_PAIRS // GROUP_SIZE
GROUP_ROWS = GROUP_SIZE * TOKENS
GROUP_PAIRS = GROUP_ROWS * TOP_K


def route_device(rng_key, hot_offset):
    key_perm, key_shift, key_quartet, key_pick, key_shuffle = jax.random.split(rng_key, 5)
    owner_perm = jax.random.permutation(key_perm, GROUP_SIZE)
    shift_size = jax.random.randint(key_shift, (GROUP_SIZE // 2,), 0, FAIR_SHARE + 1)
    shift_size = shift_size.at[0].set(FAIR_SHARE)
    per_owner = jnp.full((GROUP_SIZE,), FAIR_SHARE, jnp.int32)
    per_owner = per_owner.at[owner_perm[0::2]].add(shift_size).at[owner_perm[1::2]].add(-shift_size)
    owner_dev = jnp.searchsorted(jnp.cumsum(per_owner), jnp.arange(DEVICE_PAIRS, dtype=jnp.int32), side='right')
    quartet = jax.random.randint(key_quartet, (DEVICE_PAIRS,), 0, LOCAL_EXPERTS // 4)
    pick_draw = jax.random.randint(key_pick, (DEVICE_PAIRS,), 0, 8)
    hot_slot = hot_offset[owner_dev, quartet]
    within = jnp.where(pick_draw < 5, hot_slot, (hot_slot + pick_draw - 4) % 4)
    expert_id = owner_dev * LOCAL_EXPERTS + quartet * 4 + within
    return expert_id[jax.random.permutation(key_shuffle, DEVICE_PAIRS)].astype(jnp.int32)


def setup_inputs(seed: int = 0, part: int = 0) -> dict:
    part_key = jax.random.fold_in(jax.random.key(seed), part)
    key_x, key_gate, key_dy, key_hot, key_route = jax.random.split(part_key, 5)
    key_in, key_out = jax.random.split(jax.random.key(seed + 1), 2)
    hot_offset = jax.random.randint(key_hot, (GROUP_SIZE, LOCAL_EXPERTS // 4), 0, 4)
    route_keys = jax.random.split(key_route, GROUP_SIZE)
    expert_idx = jax.vmap(route_device, in_axes=(0, None))(route_keys, hot_offset).reshape(GROUP_ROWS, TOP_K)
    x_in = jax.random.normal(key_x, (GROUP_ROWS, D_MODEL), jnp.float32).astype(jnp.bfloat16)
    gate_weight = jax.random.uniform(key_gate, (GROUP_ROWS, TOP_K), jnp.float32, 0.5, 1.5) * TOP_K ** -0.5
    grad_y = jax.random.normal(key_dy, (GROUP_ROWS, D_MODEL), jnp.float32).astype(jnp.bfloat16)
    w_in = (jax.random.normal(key_in, (EXPERTS, D_MODEL, D_FF), jnp.float32) * D_MODEL ** -0.5).astype(jnp.bfloat16)
    w_out = (jax.random.normal(key_out, (EXPERTS, D_FF, D_MODEL), jnp.float32) * D_FF ** -0.5).astype(jnp.bfloat16)
    return {'x_in': x_in, 'expert_idx': expert_idx, 'gate_weight': gate_weight, 'grad_y': grad_y, 'w_in': w_in, 'w_out': w_out}


def reference(x_in, expert_idx, gate_weight, grad_y, w_in, w_out):
    flat_idx = expert_idx.reshape(GROUP_PAIRS)
    pair_ids = jnp.arange(GROUP_PAIRS, dtype=jnp.int32)
    sort_order = jnp.argsort(flat_idx, stable=True)
    counts = jnp.zeros((EXPERTS,), jnp.int32).at[flat_idx].add(1)
    starts = jnp.cumsum(counts) - counts
    sorted_rank = pair_ids - starts[flat_idx[sort_order]]
    pair_slot = jnp.zeros((GROUP_PAIRS,), jnp.int32).at[sort_order].set(sorted_rank)
    dest_row = jnp.where(pair_slot < CAPACITY, flat_idx * CAPACITY + pair_slot, EXPERTS * CAPACITY)
    source_pair = jnp.full((EXPERTS * CAPACITY,), GROUP_PAIRS, jnp.int32).at[dest_row].set(pair_ids, mode='drop')
    exp_rows = jnp.take(x_in, source_pair // TOP_K, axis=0, mode='fill', fill_value=0).reshape(EXPERTS, CAPACITY, D_MODEL)
    scaled_grad = (gate_weight[:, :, None] * grad_y[:, None, :].astype(jnp.float32)).astype(jnp.bfloat16).reshape(GROUP_PAIRS, D_MODEL)
    grad_rows = jnp.take(scaled_grad, source_pair, axis=0, mode='fill', fill_value=0).reshape(EXPERTS, CAPACITY, D_MODEL)

    def expert_pass(operands):
        rows_in, rows_grad, weight_in, weight_out = operands
        pre_act = jnp.dot(rows_in, weight_in, preferred_element_type=jnp.float32)
        act_full, gelu_pull = jax.vjp(jax.nn.gelu, pre_act)
        act_bf = act_full.astype(jnp.bfloat16)
        rows_out = jnp.dot(act_bf, weight_out, preferred_element_type=jnp.float32).astype(jnp.bfloat16)
        grad_act = jnp.dot(rows_grad, weight_out.T, preferred_element_type=jnp.float32).astype(jnp.bfloat16)
        grad_pre = gelu_pull(grad_act.astype(jnp.float32))[0].astype(jnp.bfloat16)
        grad_weight_out = jnp.dot(act_bf.T, rows_grad, preferred_element_type=jnp.float32).astype(jnp.bfloat16)
        grad_weight_in = jnp.dot(rows_in.T, grad_pre, preferred_element_type=jnp.float32).astype(jnp.bfloat16)
        grad_in = jnp.dot(grad_pre, weight_in.T, preferred_element_type=jnp.float32).astype(jnp.bfloat16)
        return rows_out, grad_in, grad_weight_in, grad_weight_out

    out_rows, grad_in_rows, grad_w_in, grad_w_out = lax.map(expert_pass, (exp_rows, grad_rows, w_in, w_out))
    out_pair = jnp.take(out_rows.reshape(EXPERTS * CAPACITY, D_MODEL), dest_row, axis=0, mode='fill', fill_value=0).reshape(GROUP_ROWS, TOP_K, D_MODEL).astype(jnp.float32)
    grad_pair = jnp.take(grad_in_rows.reshape(EXPERTS * CAPACITY, D_MODEL), dest_row, axis=0, mode='fill', fill_value=0).reshape(GROUP_ROWS, TOP_K, D_MODEL).astype(jnp.float32)
    y_out = (x_in.astype(jnp.float32) + jnp.sum(gate_weight[:, :, None] * out_pair, axis=1)).astype(jnp.bfloat16)
    grad_gate = jnp.sum(grad_y.astype(jnp.float32)[:, None, :] * out_pair, axis=2)
    grad_x = (grad_y.astype(jnp.float32) + jnp.sum(grad_pair, axis=1)).astype(jnp.bfloat16)
    return y_out, grad_x, grad_gate, grad_w_in, grad_w_out
```

```python
import functools

import jax
import jax.numpy as jnp
from jax import lax
from jax.experimental import pallas as pl
from jax.experimental.pallas import tpu as pltpu
from jax.sharding import PartitionSpec as P

MESH = pl.DeviceIdType.MESH
CAP = 40
SLOTS = 48
PAIR = 2
C0 = 0.7978845608028654
C1 = 0.044715


def dot(a, b, dims=((1,), (0,))):
    return lax.dot_general(a, b, (dims, ((), ())), preferred_element_type=jnp.float32)


def gather_kernel(x_ref, dy_ref, idx_ref, gate_ref, xa, dya, ida, ga, small_s, small_r, sib_s, sib_r,
                  cross_s, cross_r, fwd_s, fwd_r):
    me = lax.axis_index("expert")
    sib, cross = me + 1 - 2 * lax.rem(me, 2), lax.rem(me + 2, 4)
    diag = lax.rem(sib + 2, 4)
    barrier = pltpu.get_barrier_semaphore()
    for peer in (sib, cross, diag):
        pl.semaphore_signal(barrier, inc=1, device_id={"expert": peer}, device_id_type=MESH)
    pl.semaphore_wait(barrier, 3)

    def send(src, dst, s, r, peer):
        copy = pltpu.make_async_remote_copy(src_ref=src, dst_ref=dst, send_sem=s, recv_sem=r,
                                            device_id={"expert": peer}, device_id_type=MESH)
        copy.start()
        return copy

    copies = []
    for k, peer in enumerate((cross, diag, sib)):
        copies.append(send(idx_ref, ida.at[me], small_s.at[2 * k], small_r.at[2 * k], peer))
        copies.append(send(gate_ref, ga.at[me], small_s.at[2 * k + 1], small_r.at[2 * k + 1], peer))
    over = []
    for a, (src, dst) in enumerate(((x_ref, xa), (dy_ref, dya))):
        for c in range(2):
            rows = pl.ds(64 * c, 64)
            over.append((dst, rows, send(src.at[rows], dst.at[me, rows], cross_s.at[2 * a + c], cross_r.at[2 * a + c], cross)))
        copies.append(send(src, dst.at[me], sib_s.at[a], sib_r.at[a], sib))
    xa[me] = x_ref[...]
    dya[me] = dy_ref[...]
    ida[me] = idx_ref[...]
    ga[me] = gate_ref[...]
    for n, (dst, rows, copy) in enumerate(over):
        copy.wait_recv()
        copies.append(send(dst.at[cross, rows], dst.at[cross, rows], fwd_s.at[n], fwd_r.at[n], sib))
    for _, _, copy in over:
        copy.wait_send()
    for copy in copies:
        copy.wait()


def gather_group(x, dy, idx_t, gate_t):
    rows, width = x.shape
    vmem = pl.BlockSpec(memory_space=pltpu.VMEM)
    dma = pltpu.SemaphoreType.DMA
    return pl.pallas_call(
        gather_kernel,
        out_shape=[jax.ShapeDtypeStruct((4, rows, width), jnp.bfloat16)] * 2
        + [jax.ShapeDtypeStruct((4, 8, rows), jnp.int32), jax.ShapeDtypeStruct((4, 8, rows), jnp.float32)],
        in_specs=[vmem] * 4,
        out_specs=[vmem] * 4,
        scratch_shapes=[dma((6,)), dma((6,)), dma((2,)), dma((2,)), dma((4,)), dma((4,)), dma((4,)), dma((4,))],
        compiler_params=pltpu.CompilerParams(collective_id=0, has_side_effects=True),
    )(x, dy, idx_t, gate_t)


def route(idx, gate, first, rj, r0s, r1s, pm, pt, gs):
    eid = lax.broadcasted_iota(jnp.int32, (32, 128), 0) + first
    earlier = (lax.broadcasted_iota(jnp.int32, (128, 128), 0) < lax.broadcasted_iota(jnp.int32, (128, 128), 1)).astype(jnp.bfloat16)
    offset = jnp.zeros((32, 1), jnp.float32)
    for d in range(4):
        ids = idx[d]
        hits = [(ids[j:j + 1, :] == eid).astype(jnp.float32) for j in range(8)]
        count = sum(hits[1:], hits[0])
        rank = dot(count.astype(jnp.bfloat16), earlier) + offset
        r0s[d] = rank
        for j in range(8):
            rj[j, d] = jnp.where((hits[j] > 0.0) & (rank < CAP), rank, -1.0)
            rank = rank + hits[j]
        r1s[d] = jnp.minimum(rank, CAP)
        offset = offset + jnp.sum(count, axis=1, keepdims=True)

    rows = lax.broadcasted_iota(jnp.int32, (SLOTS, 128), 0).astype(jnp.float32)

    def one(e, _):
        at = pl.ds(pl.multiple_of(e * SLOTS, SLOTS), SLOTS)
        total = jnp.zeros((SLOTS, 128), jnp.float32)
        for d in range(4):
            lanes = slice(128 * d, 128 * (d + 1))
            inside = (rows >= r0s[d, pl.ds(e, 1), :]) & (rows < r1s[d, pl.ds(e, 1), :])
            pm[at, lanes] = jnp.where(inside, 1.0, 0.0).astype(jnp.bfloat16)
            for j in range(8):
                total = jnp.where(rows == rj[j, d, pl.ds(e, 1), :], total + gate[d, j:j + 1, :], total)
        gs[at, :] = jnp.sum(total, axis=1, keepdims=True)
        return 0

    lax.fori_loop(0, 32, one, 0)

    def turn(c, _):
        at = pl.ds(pl.multiple_of(c * 128, 128), 128)
        pt[:, at] = pm[at, :].astype(jnp.float32).T.astype(jnp.bfloat16)
        return 0

    lax.fori_loop(0, 32 * SLOTS // 128, turn, 0)


def expert_kernel(idx, gate, xa, dya, w_in, w_out, yp, dxp, dgp, b_out, h_out, g_out, da_out,
                  rj, r0s, r1s, pm, pt, gs, gx, sp, o_s, slope, dg_tab):
    step = pl.program_id(0)
    half = pl.num_programs(0) // 2
    slots = 32 * SLOTS

    @pl.when(step == 0)
    def _():
        route(idx, gate, lax.axis_index("expert") * 32, rj, r0s, r1s, pm, pt, gs)

        def pick(c, _):
            at = pl.ds(pl.multiple_of(c * 256, 256), 256)
            gx[at, :] = dot(pm[at, :], xa[...]).astype(jnp.bfloat16)
            return 0

        lax.fori_loop(0, slots // 256, pick, 0)

    @pl.when(step < half)
    def _():
        for p in range(PAIR):
            at = pl.ds(pl.multiple_of((step * PAIR + p) * SLOTS, SLOTS), SLOTS)
            here = pl.ds(p * SLOTS, SLOTS)
            rows = gx[at, :]
            b_out[here, :] = rows
            a = dot(rows, w_in[p])
            th = jnp.tanh(C0 * (a + C1 * (a * a * a)))
            cdf = 0.5 * (1.0 + th)
            slope[at, :] = cdf + 0.5 * a * (1.0 - th * th) * (C0 * (1.0 + 3.0 * C1 * (a * a)))
            h = (a * cdf).astype(jnp.bfloat16)
            h_out[here, :] = h
            o = dot(h, w_out[p]).astype(jnp.bfloat16)
            o_s[at, :] = o
            s = o.astype(jnp.float32) * gs[at, :]
            s1 = s.astype(jnp.bfloat16)
            s = s - s1.astype(jnp.float32)
            s2 = s.astype(jnp.bfloat16)
            s = s - s2.astype(jnp.float32)
            sp[0, at, :] = s1
            sp[1, at, :] = s2
            sp[2, at, :] = s.astype(jnp.bfloat16)

    @pl.when(step == half)
    def _():
        def combine(n, _):
            lanes = pl.ds(pl.multiple_of(n * 256, 256), 256)
            out = dot(pt[...], sp[0, :, lanes]) + dot(pt[...], sp[1, :, lanes]) + dot(pt[...], sp[2, :, lanes])
            for d in range(4):
                yp[d, :, lanes] = out[128 * d:128 * (d + 1)]
            return 0

        lax.fori_loop(0, 4, combine, 0)

        def pick(c, _):
            at = pl.ds(pl.multiple_of(c * 256, 256), 256)
            gx[at, :] = dot(pm[at, :], dya[...]).astype(jnp.bfloat16)
            return 0

        lax.fori_loop(0, slots // 256, pick, 0)

    @pl.when(step >= half)
    def _():
        for p in range(PAIR):
            e = (2 * half - 1 - step) * PAIR + p
            at = pl.ds(pl.multiple_of(e * SLOTS, SLOTS), SLOTS)
            here = pl.ds(p * SLOTS, SLOTS)
            rows = gx[at, :].astype(jnp.float32)
            g = (rows * gs[at, :]).astype(jnp.bfloat16)
            g_out[here, :] = g
            prod = rows * o_s[at, :].astype(jnp.float32)
            part = sum((prod[:, 128 * c:128 * (c + 1)] for c in range(1, 8)), prod[:, :128])
            dg_tab[pl.ds(e, 1), :SLOTS] = jnp.sum(part.T, axis=0, keepdims=True)
            dh = dot(w_out[p], g, ((1,), (1,))).T
            da = (dh.astype(jnp.bfloat16).astype(jnp.float32) * slope[at, :]).astype(jnp.bfloat16)
            da_out[here, :] = da
            sp[0, at, :] = dot(w_in[p], da, ((1,), (1,))).T.astype(jnp.bfloat16)

    @pl.when(step == 2 * half - 1)
    def _():
        def combine(n, _):
            lanes = pl.ds(pl.multiple_of(n * 256, 256), 256)
            out = dot(pt[...], sp[0, :, lanes])
            for d in range(4):
                dxp[d, :, lanes] = out[128 * d:128 * (d + 1)]
            return 0

        lax.fori_loop(0, 4, combine, 0)
        for d in range(4):
            for j in range(8):
                at = rj[j, d].astype(jnp.int32)
                got = jnp.take_along_axis(dg_tab[...], jnp.maximum(at, 0), axis=1)
                dgp[d, j:j + 1, :] = jnp.sum(jnp.where(at >= 0, got, 0.0), axis=0, keepdims=True)


def experts(idx, gate, xa, dya, w_in, w_out):
    n_e, d_model, d_ff = w_in.shape
    half = n_e // PAIR
    slots = n_e * SLOTS
    both = 2 * half - 1

    def whole(a):
        return pl.BlockSpec(a.shape, lambda i: (0,) * a.ndim)

    def weights(i):
        return (jnp.where(i < half, i, both - i), 0, 0)

    def first(i):
        return (jnp.minimum(i, half - 1), 0)

    def second(i):
        return (jnp.minimum(both - i, half - 1), 0)

    bf, f32 = jnp.bfloat16, jnp.float32
    outs = [jax.ShapeDtypeStruct((4, 128, d_model), f32), jax.ShapeDtypeStruct((4, 128, d_model), f32),
            jax.ShapeDtypeStruct((4, 8, 128), f32),
            jax.ShapeDtypeStruct((slots, d_model), bf), jax.ShapeDtypeStruct((slots, d_ff), bf),
            jax.ShapeDtypeStruct((slots, d_model), bf), jax.ShapeDtypeStruct((slots, d_ff), bf)]
    return pl.pallas_call(
        expert_kernel,
        grid=(2 * half,),
        out_shape=outs,
        in_specs=[whole(idx), whole(gate), whole(xa), whole(dya),
                  pl.BlockSpec((PAIR, d_model, d_ff), weights), pl.BlockSpec((PAIR, d_ff, d_model), weights)],
        out_specs=[whole(outs[0]), whole(outs[1]), whole(outs[2]),
                   pl.BlockSpec((PAIR * SLOTS, d_model), first), pl.BlockSpec((PAIR * SLOTS, d_ff), first),
                   pl.BlockSpec((PAIR * SLOTS, d_model), second), pl.BlockSpec((PAIR * SLOTS, d_ff), second)],
        scratch_shapes=[pltpu.VMEM((8, 4, n_e, 128), f32), pltpu.VMEM((4, n_e, 128), f32), pltpu.VMEM((4, n_e, 128), f32),
                        pltpu.VMEM((slots, 512), bf), pltpu.VMEM((512, slots), bf), pltpu.VMEM((slots, 1), f32),
                        pltpu.VMEM((slots, d_model), bf), pltpu.VMEM((3, slots, d_model), bf),
                        pltpu.VMEM((slots, d_model), bf), pltpu.VMEM((slots, d_ff), f32), pltpu.VMEM((n_e, 128), f32)],
        compiler_params=pltpu.CompilerParams(vmem_limit_bytes=62 * 1024 * 1024),
        cost_estimate=pl.CostEstimate(flops=8 * slots * d_model * d_ff, bytes_accessed=4 * n_e * d_model * d_ff, transcendentals=0),
    )(idx, gate, xa, dya, w_in, w_out)


def weight_kernel(b, h, g, da, dw_in, dw_out):
    for p in range(PAIR):
        at = slice(p * SLOTS, (p + 1) * SLOTS)
        dw_in[p] = dot(b[at, :], da[at, :], ((0,), (0,))).astype(jnp.bfloat16)
        dw_out[p] = dot(h[at, :], g[at, :], ((0,), (0,))).astype(jnp.bfloat16)


def weight_grads(b, h, g, da, n_e):
    d_model, d_ff = b.shape[1], h.shape[1]
    rows = PAIR * SLOTS
    return pl.pallas_call(
        weight_kernel,
        grid=(n_e // PAIR,),
        out_shape=[jax.ShapeDtypeStruct((n_e, d_model, d_ff), jnp.bfloat16), jax.ShapeDtypeStruct((n_e, d_ff, d_model), jnp.bfloat16)],
        in_specs=[pl.BlockSpec((rows, d_model), lambda i: (i, 0)), pl.BlockSpec((rows, d_ff), lambda i: (i, 0)),
                  pl.BlockSpec((rows, d_model), lambda i: (i, 0)), pl.BlockSpec((rows, d_ff), lambda i: (i, 0))],
        out_specs=[pl.BlockSpec((PAIR, d_model, d_ff), lambda i: (i, 0, 0)), pl.BlockSpec((PAIR, d_ff, d_model), lambda i: (i, 0, 0))],
        compiler_params=pltpu.CompilerParams(vmem_limit_bytes=48 * 1024 * 1024),
        cost_estimate=pl.CostEstimate(flops=4 * n_e * SLOTS * d_model * d_ff, bytes_accessed=4 * n_e * d_model * d_ff, transcendentals=0),
    )(b, h, g, da)


def solution(mesh):
    tok_spec = P(('data', 'expert'), None)
    weight_spec = P('expert', None, None)
    grad_spec = P(('data', 'expert'), None, None)
    to_sib = [(i, i ^ 1) for i in range(4)]
    to_cross = [(i, i ^ 2) for i in range(4)]

    def device_pass(x_in, expert_idx, gate_weight, grad_y, w_in, w_out):
        n_tokens, d_model = x_in.shape
        me = lax.axis_index('expert')
        core, chip = lax.rem(me, 2), me // 2
        xa, dya, ida, ga = gather_group(x_in, grad_y, expert_idx.T, gate_weight.T)
        yp, dxp, dgp, b, h, g, da = experts(ida, ga, xa.reshape(512, d_model), dya.reshape(512, d_model), w_in, w_out)

        def reduce_back(part):
            part = part.reshape((2, 2) + part.shape[1:])
            mine = lax.dynamic_index_in_dim(part, core, 1, keepdims=False)
            theirs = lax.dynamic_index_in_dim(part, 1 - core, 1, keepdims=False)
            mine = mine + lax.ppermute(theirs, 'expert', to_sib)
            far = lax.ppermute(lax.dynamic_index_in_dim(mine, 1 - chip, 0, keepdims=False), 'expert', to_cross)
            return lax.dynamic_index_in_dim(mine, chip, 0, keepdims=False) + far

        y_sum, dx_sum, dg_sum = reduce_back(yp), reduce_back(dxp), reduce_back(dgp)
        grad_w_in, grad_w_out = weight_grads(b, h, g, da, w_in.shape[0])
        y_out = (x_in.astype(jnp.float32) + y_sum).astype(jnp.bfloat16)
        grad_x = (grad_y.astype(jnp.float32) + dx_sum).astype(jnp.bfloat16)
        return y_out, grad_x, dg_sum.T, grad_w_in, grad_w_out

    return jax.shard_map(device_pass, mesh=mesh,
                         in_specs=(tok_spec, tok_spec, tok_spec, tok_spec, weight_spec, weight_spec),
                         out_specs=(tok_spec, tok_spec, tok_spec, grad_spec, grad_spec), check_vma=False)
```

```python
import functools

import jax
import jax.numpy as jnp
from jax import lax
from jax.experimental import pallas as pl
from jax.experimental.pallas import tpu as pltpu
from jax.sharding import PartitionSpec as P

MESH = pl.DeviceIdType.MESH
CAP = 40
SLOTS = 48
PAIR = 2
AHEAD = 4
PICK = 384
C0 = 0.7978845608028654
C1 = 0.044715


def dot(a, b, dims=((1,), (0,))):
    return lax.dot_general(a, b, (dims, ((), ())), preferred_element_type=jnp.float32)


def tables(ids_all, first, rj, r0s, r1s):
    eid = lax.broadcasted_iota(jnp.int32, (32, 128), 0) + first
    earlier = (lax.broadcasted_iota(jnp.int32, (128, 128), 0) < lax.broadcasted_iota(jnp.int32, (128, 128), 1)).astype(jnp.bfloat16)
    offset = jnp.zeros((32, 1), jnp.float32)
    for d in range(4):
        ids = ids_all[d]
        hits = [(ids[j:j + 1, :] == eid).astype(jnp.float32) for j in range(8)]
        count = sum(hits[1:], hits[0])
        rank = dot(count.astype(jnp.bfloat16), earlier) + offset
        r0s[d] = rank
        for j in range(8):
            rj[j, d] = jnp.where((hits[j] > 0.0) & (rank < CAP), rank, -1.0)
            rank = rank + hits[j]
        r1s[d] = jnp.minimum(rank, CAP)
        offset = offset + jnp.sum(count, axis=1, keepdims=True)


def slot_rows(e):
    return pl.ds(pl.multiple_of(e * SLOTS, SLOTS), SLOTS)


def expert_kernel(x, dy, idx, gate, w_in, w_out, y_out, dg_out, dx_own, dx_far, b_out, h_out, g_out, da_out,
                  xa, dya, ida, ga, rj, r0s, r1s, pm, pt, gs, b_s, g_s, h_s, da_s, o_s, slope, sp, zs, dg_tab, dgp, dgr,
                  wi, wo, yp, yr, yfar, ygot, dxp, dxr,
                  wi_sem, wo_sem, out_sem, small_s, small_r, sib_s, sib_r, cross_s, cross_r, fwd_s, fwd_r,
                  yd_s, yd_r, yx_s, yx_r, dd_s, dd_r, dg_s, dg_r):
    me = lax.axis_index("expert")
    sib, cross = me + 1 - 2 * lax.rem(me, 2), lax.rem(me + 2, 4)
    diag = lax.rem(sib + 2, 4)
    n_pairs = w_in.shape[0] // PAIR
    slots = 32 * SLOTS
    bf, f32 = jnp.bfloat16, jnp.float32

    def fetch_in(q, slot):
        return pltpu.make_async_copy(w_in.at[pl.ds(PAIR * q, PAIR)], wi.at[slot], wi_sem.at[slot])

    def fetch_out(q, slot):
        return pltpu.make_async_copy(w_out.at[pl.ds(PAIR * q, PAIR)], wo.at[slot], wo_sem.at[slot])

    def remote(src, dst, s, r, peer):
        return pltpu.make_async_remote_copy(src_ref=src, dst_ref=dst, send_sem=s, recv_sem=r,
                                            device_id={"expert": peer}, device_id_type=MESH)

    for q in range(AHEAD):
        fetch_in(q, q).start()
        fetch_out(q, q).start()

    barrier = pltpu.get_barrier_semaphore()
    for peer in (sib, cross, diag):
        pl.semaphore_signal(barrier, inc=1, device_id={"expert": peer}, device_id_type=MESH)
    pl.semaphore_wait(barrier, 3)

    small, over, near, far = [], [], [], []
    for k, peer in enumerate((cross, diag, sib)):
        small.append(remote(idx, ida.at[me], small_s.at[2 * k], small_r.at[2 * k], peer))
        small.append(remote(gate, ga.at[me], small_s.at[2 * k + 1], small_r.at[2 * k + 1], peer))
    for a, (src, dst) in enumerate(((x, xa), (dy, dya))):
        for c in range(2):
            rows = pl.ds(64 * c, 64)
            n = 2 * a + c
            over.append(remote(src.at[rows], dst.at[me, rows], cross_s.at[n], cross_r.at[n], cross))
            far.append(remote(dst.at[cross, rows], dst.at[cross, rows], fwd_s.at[n], fwd_r.at[n], sib))
        near.append(remote(src, dst.at[me], sib_s.at[a], sib_r.at[a], sib))
    for copy in small + over[:2] + near[:1] + over[2:] + near[1:]:
        copy.start()
    xa[me] = x[...]
    dya[me] = dy[...]
    ida[me] = idx[...]
    ga[me] = gate[...]
    zs[...] = jnp.zeros_like(zs)

    def forward(n):
        over[n].wait_recv()
        far[n].start()

    for copy in small:
        copy.wait_recv()
    tables(ida, me * 32, rj, r0s, r1s)
    slot_id = lax.broadcasted_iota(jnp.int32, (SLOTS, 128), 0).astype(f32)

    def one(e, _):
        total = jnp.zeros((SLOTS, 128), f32)
        for d in range(4):
            lanes = slice(128 * d, 128 * (d + 1))
            inside = (slot_id >= r0s[d, pl.ds(e, 1), :]) & (slot_id < r1s[d, pl.ds(e, 1), :])
            pm[slot_rows(e), lanes] = jnp.where(inside, 1.0, 0.0).astype(bf)
            for j in range(8):
                total = jnp.where(slot_id == rj[j, d, pl.ds(e, 1), :], ga[d, j:j + 1, :], total)
        gs[slot_rows(e), :] = jnp.sum(total, axis=1, keepdims=True)
        return 0

    lax.fori_loop(0, 32, one, 0)
    forward(0)

    def turn(c, _):
        at = pl.ds(pl.multiple_of(c * 128, 128), 128)
        pt[:, at] = pm[at, :].astype(f32).T.astype(bf)
        return 0

    lax.fori_loop(0, slots // 128, turn, 0)
    forward(1)
    near[0].wait_recv()
    far[0].wait_recv()
    far[1].wait_recv()

    def pick_x(c, _):
        at = pl.ds(pl.multiple_of(c * PICK, PICK), PICK)
        b_s[at, :] = dot(pm[at, :], xa[...].reshape(512, xa.shape[2])).astype(bf)
        return 0

    lax.fori_loop(0, slots // PICK, pick_x, 0)
    pltpu.make_async_copy(b_s, b_out, out_sem.at[0]).start()

    def fwd_step(i, _):
        slot = lax.rem(i, AHEAD)
        fetch_in(i, slot).wait()
        fetch_out(i, slot).wait()
        for p in range(PAIR):
            at = slot_rows(i * PAIR + p)
            a = dot(b_s[at, :], wi[slot, p])
            th = jnp.tanh(C0 * (a + C1 * (a * a * a)))
            cdf = 0.5 * (1.0 + th)
            slope[at, :] = cdf + 0.5 * a * (1.0 - th * th) * (C0 * (1.0 + 3.0 * C1 * (a * a)))
            h = (a * cdf).astype(bf)
            h_s[at, :] = h
            o = dot(h, wo[slot, p]).astype(bf)
            o_s[at, :] = o
            s = o.astype(f32) * gs[at, :]
            s1 = s.astype(bf)
            s = s - s1.astype(f32)
            s2 = s.astype(bf)
            s = s - s2.astype(f32)
            sp[0, at, :] = s1
            sp[1, at, :] = s2
            sp[2, at, :] = s.astype(bf)

        @pl.when(i < n_pairs - AHEAD)
        def _():
            fetch_in(i + AHEAD, slot).start()
            fetch_out(i + AHEAD, slot).start()

        @pl.when(i >= n_pairs - AHEAD)
        def _():
            fetch_in(2 * n_pairs - 1 - AHEAD - i, slot).start()
            fetch_out(2 * n_pairs - 1 - AHEAD - i, slot).start()

        for n, when in ((2, 1), (3, 4)):
            @pl.when(i == when)
            def _(n=n):
                forward(n)
        return 0

    lax.fori_loop(0, n_pairs, fwd_step, 0)
    pltpu.make_async_copy(h_s, h_out, out_sem.at[1]).start()

    def to_sib(part, got, s, r, n, k):
        return remote(part.at[n, sib if k == 0 else diag], got.at[n, k], s.at[n, k], r.at[n, k], sib)

    def y_part(n, _):
        lanes = pl.ds(pl.multiple_of(n * 256, 256), 256)
        out = dot(pt[...], sp[0, :, lanes]) + dot(pt[...], sp[1, :, lanes]) + dot(pt[...], sp[2, :, lanes])
        for d in range(4):
            yp[n, d] = out[128 * d:128 * (d + 1)]

        @pl.when(n > 0)
        def _():
            for k in range(2):
                to_sib(yp, yr, yd_s, yd_r, n - 1, k).start()
        return 0

    lax.fori_loop(0, 4, y_part, 0)
    near[1].wait_recv()
    far[2].wait_recv()
    far[3].wait_recv()
    for k in range(2):
        to_sib(yp, yr, yd_s, yd_r, 3, k).start()

    def pick_dy(c, _):
        at = pl.ds(pl.multiple_of(c * PICK, PICK), PICK)
        rows = dot(pm[at, :], dya[...].reshape(512, dya.shape[2]))
        g_s[at, :] = (rows * gs[at, :]).astype(bf)
        prod = rows * o_s[at, :].astype(f32)
        part = sum((prod[:, 128 * k:128 * (k + 1)] for k in range(1, 8)), prod[:, :128])
        for k in range(PICK // SLOTS):
            dg_tab[pl.ds(c * (PICK // SLOTS) + k, 1), :SLOTS] = jnp.sum(part[SLOTS * k:SLOTS * (k + 1)].T, axis=0, keepdims=True)
        return 0

    lax.fori_loop(0, slots // PICK, pick_dy, 0)
    pltpu.make_async_copy(g_s, g_out, out_sem.at[2]).start()
    for n in range(4):
        for k in range(2):
            to_sib(yp, yr, yd_s, yd_r, n, k).wait()
        yfar[n] = yp[n, cross] + yr[n, 1]
    for d in range(4):
        for j in range(8):
            at = rj[j, d].astype(jnp.int32)
            got = jnp.take_along_axis(dg_tab[...], jnp.maximum(at, 0), axis=1)
            dgp[d, j:j + 1, :] = jnp.sum(jnp.where(at >= 0, got, 0.0), axis=0, keepdims=True)
    y_cross = remote(yfar, ygot, yx_s, yx_r, cross)
    y_cross.start()
    dg_back = [remote(dgp.at[peer], dgr.at[k], dg_s.at[k], dg_r.at[k], peer) for k, peer in enumerate((cross, diag, sib))]

    def zero(n, like):
        return jnp.zeros((n, like.shape[1]), bf)

    def back_h(q, i):
        slot = lax.rem(i, AHEAD)
        fetch_out(q, slot).wait()
        g0, g1 = g_s[slot_rows(q * PAIR), :], g_s[slot_rows(q * PAIR + 1), :]
        both = dot(wo[slot, 0], jnp.concatenate([g0, zero(80, g0)], axis=0), ((1,), (1,)))
        both = both + dot(wo[slot, 1], jnp.concatenate([zero(64, g1), g1, zero(16, g1)], axis=0), ((1,), (1,)))
        dh = both.astype(bf).T.astype(f32)
        for p in range(PAIR):
            at = slot_rows(q * PAIR + p)
            da = (dh[64 * p:64 * p + SLOTS] * slope[at, :]).astype(bf)
            da_s[at, :] = da
            zs[lax.rem(i, 2), 64 * p:64 * p + SLOTS, 384 * p:384 * (p + 1)] = da

    def back_x(q, i):
        slot = lax.rem(i, AHEAD)
        fetch_in(q, slot).wait()
        wide = jnp.concatenate([wi[slot, 0], wi[slot, 1]], axis=1)
        both = dot(wide, zs[lax.rem(i, 2)], ((1,), (1,))).astype(bf).T
        for p in range(PAIR):
            sp[0, slot_rows(q * PAIR + p), :] = both[64 * p:64 * p + SLOTS]

    last = n_pairs - 1
    back_h(last, 0)
    fetch_out(last - AHEAD, 0).start()
    for copy in dg_back:
        copy.start()

    def bwd_step(i, _):
        back_x(last + 1 - i, i - 1)
        back_h(last - i, i)

        @pl.when(i < n_pairs - AHEAD)
        def _():
            fetch_out(last - AHEAD - i, lax.rem(i, AHEAD)).start()

        @pl.when(i < n_pairs - AHEAD + 1)
        def _():
            fetch_in(last + 1 - AHEAD - i, lax.rem(i - 1, AHEAD)).start()
        return 0

    lax.fori_loop(1, n_pairs, bwd_step, 0)
    pltpu.make_async_copy(da_s, da_out, out_sem.at[3]).start()
    back_x(0, last)

    def dx_part(n, _):
        lanes = pl.ds(pl.multiple_of(n * 256, 256), 256)
        out = dot(pt[...], sp[0, :, lanes])
        for d in range(4):
            dxp[n, d] = out[128 * d:128 * (d + 1)]

        @pl.when(n > 0)
        def _():
            for k in range(2):
                to_sib(dxp, dxr, dd_s, dd_r, n - 1, k).start()
        return 0

    lax.fori_loop(0, 4, dx_part, 0)
    y_cross.wait()
    for k in range(2):
        to_sib(dxp, dxr, dd_s, dd_r, 3, k).start()
    for n in range(4):
        lanes = slice(256 * n, 256 * (n + 1))
        y_out[:, lanes] = (x[:, lanes].astype(f32) + (yp[n, me] + yr[n, 0] + ygot[n])).astype(bf)
    for copy in dg_back:
        copy.wait()
    dg_out[...] = dgp[me] + (dgr[0] + (dgr[1] + dgr[2]))
    for n in range(4):
        lanes = slice(256 * n, 256 * (n + 1))
        for k in range(2):
            to_sib(dxp, dxr, dd_s, dd_r, n, k).wait()
        dx_own[:, lanes] = dxp[n, me] + dxr[n, 0]
        dx_far[:, lanes] = dxp[n, cross] + dxr[n, 1]
    for copy in small + over + near + far:
        copy.wait_send()
    for k, (src, dst) in enumerate(((b_s, b_out), (h_s, h_out), (g_s, g_out), (da_s, da_out))):
        pltpu.make_async_copy(src, dst, out_sem.at[k]).wait()


def experts(x, dy, idx_t, gate_t, w_in, w_out):
    n_e, d_model, d_ff = w_in.shape
    slots = n_e * SLOTS
    bf, f32 = jnp.bfloat16, jnp.float32
    vmem, hbm = pl.BlockSpec(memory_space=pltpu.VMEM), pl.BlockSpec(memory_space=pl.ANY)
    shape, buf, dma = jax.ShapeDtypeStruct, pltpu.VMEM, pltpu.SemaphoreType.DMA
    return pl.pallas_call(
        expert_kernel,
        out_shape=[shape((128, d_model), bf), shape((8, 128), f32), shape((128, d_model), f32), shape((128, d_model), f32),
                   shape((slots, d_model), bf), shape((slots, d_ff), bf), shape((slots, d_model), bf), shape((slots, d_ff), bf)],
        in_specs=[vmem] * 4 + [hbm] * 2,
        out_specs=[vmem] * 4 + [hbm] * 4,
        scratch_shapes=[
            buf((4, 128, d_model), bf), buf((4, 128, d_model), bf), buf((4, 8, 128), jnp.int32), buf((4, 8, 128), f32),
            buf((8, 4, n_e, 128), f32), buf((4, n_e, 128), f32), buf((4, n_e, 128), f32),
            buf((slots, 512), bf), buf((512, slots), bf), buf((slots, 1), f32),
            buf((slots, d_model), bf), buf((slots, d_model), bf), buf((slots, d_ff), bf), buf((slots, d_ff), bf),
            buf((slots, d_model), bf), buf((slots, d_ff), f32), buf((3, slots, d_model), bf), buf((2, 128, PAIR * d_ff), bf),
            buf((n_e, 128), f32), buf((4, 8, 128), f32), buf((3, 8, 128), f32),
            buf((AHEAD, PAIR, d_model, d_ff), bf), buf((AHEAD, PAIR, d_ff, d_model), bf),
            buf((4, 4, 128, 256), f32), buf((4, 2, 128, 256), f32), buf((4, 128, 256), f32), buf((4, 128, 256), f32),
            buf((4, 4, 128, 256), f32), buf((4, 2, 128, 256), f32),
            dma((AHEAD,)), dma((AHEAD,)), dma((4,)), dma((6,)), dma((6,)), dma((2,)), dma((2,)), dma((4,)), dma((4,)),
            dma((4,)), dma((4,)), dma((4, 2)), dma((4, 2)), dma(()), dma(()), dma((4, 2)), dma((4, 2)), dma((3,)), dma((3,))],
        compiler_params=pltpu.CompilerParams(collective_id=0, has_side_effects=True, vmem_limit_bytes=63 * 1024 * 1024),
        cost_estimate=pl.CostEstimate(flops=8 * slots * d_model * d_ff, bytes_accessed=8 * n_e * d_model * d_ff, transcendentals=0),
    )(x, dy, idx_t, gate_t, w_in, w_out)


def weight_kernel(b, h, g, da, dw_in, dw_out):
    for p in range(PAIR):
        at = slice(p * SLOTS, (p + 1) * SLOTS)
        dw_in[p] = dot(b[at, :], da[at, :], ((0,), (0,))).astype(jnp.bfloat16)
        dw_out[p] = dot(h[at, :], g[at, :], ((0,), (0,))).astype(jnp.bfloat16)


def weight_grads(b, h, g, da, n_e):
    d_model, d_ff = b.shape[1], h.shape[1]
    rows = PAIR * SLOTS
    return pl.pallas_call(
        weight_kernel,
        grid=(n_e // PAIR,),
        out_shape=[jax.ShapeDtypeStruct((n_e, d_model, d_ff), jnp.bfloat16), jax.ShapeDtypeStruct((n_e, d_ff, d_model), jnp.bfloat16)],
        in_specs=[pl.BlockSpec((rows, d_model), lambda i: (i, 0)), pl.BlockSpec((rows, d_ff), lambda i: (i, 0)),
                  pl.BlockSpec((rows, d_model), lambda i: (i, 0)), pl.BlockSpec((rows, d_ff), lambda i: (i, 0))],
        out_specs=[pl.BlockSpec((PAIR, d_model, d_ff), lambda i: (i, 0, 0)), pl.BlockSpec((PAIR, d_ff, d_model), lambda i: (i, 0, 0))],
        compiler_params=pltpu.CompilerParams(vmem_limit_bytes=48 * 1024 * 1024),
        cost_estimate=pl.CostEstimate(flops=4 * n_e * SLOTS * d_model * d_ff, bytes_accessed=4 * n_e * d_model * d_ff, transcendentals=0),
    )(b, h, g, da)


def solution(mesh):
    tok_spec = P(('data', 'expert'), None)
    weight_spec = P('expert', None, None)
    grad_spec = P(('data', 'expert'), None, None)
    to_cross = [(i, i ^ 2) for i in range(4)]

    def device_pass(x_in, expert_idx, gate_weight, grad_y, w_in, w_out):
        y_out, dg, dx_own, dx_far, b, h, g, da = experts(x_in, grad_y, expert_idx.T, gate_weight.T, w_in, w_out)
        dx_got = lax.ppermute(dx_far, 'expert', to_cross)
        grad_w_in, grad_w_out = weight_grads(b, h, g, da, w_in.shape[0])
        grad_x = (grad_y.astype(jnp.float32) + (dx_own + dx_got)).astype(jnp.bfloat16)
        return y_out, grad_x, dg.T, grad_w_in, grad_w_out

    return jax.shard_map(device_pass, mesh=mesh,
                         in_specs=(tok_spec, tok_spec, tok_spec, tok_spec, weight_spec, weight_spec),
                         out_specs=(tok_spec, tok_spec, tok_spec, grad_spec, grad_spec), check_vma=False)
```

```python
import functools

import jax
import jax.numpy as jnp
from jax import lax
from jax.experimental import pallas as pl
from jax.experimental.pallas import tpu as pltpu
from jax.sharding import PartitionSpec as P

MESH = pl.DeviceIdType.MESH
CAP = 40
SLOTS = 48
PAIR = 2
AHEAD = 4
PICK = 384
C0 = 0.7978845608028654
C1 = 0.044715


def dot(a, b, dims=((1,), (0,))):
    return lax.dot_general(a, b, (dims, ((), ())), preferred_element_type=jnp.float32)


def tables(ids_all, first, rj, r0s, r1s):
    eid = lax.broadcasted_iota(jnp.int32, (32, 128), 0) + first
    earlier = (lax.broadcasted_iota(jnp.int32, (128, 128), 0) < lax.broadcasted_iota(jnp.int32, (128, 128), 1)).astype(jnp.bfloat16)
    offset = jnp.zeros((32, 1), jnp.float32)
    for d in range(4):
        ids = ids_all[d]
        hits = [(ids[j:j + 1, :] == eid).astype(jnp.float32) for j in range(8)]
        count = sum(hits[1:], hits[0])
        rank = dot(count.astype(jnp.bfloat16), earlier) + offset
        r0s[d] = rank
        for j in range(8):
            rj[j, d] = jnp.where((hits[j] > 0.0) & (rank < CAP), rank, -1.0)
            rank = rank + hits[j]
        r1s[d] = jnp.minimum(rank, CAP)
        offset = offset + jnp.sum(count, axis=1, keepdims=True)


def slot_rows(e):
    return pl.ds(pl.multiple_of(e * SLOTS, SLOTS), SLOTS)


def expert_kernel(x, dy, idx, gate, w_in, w_out, y_out, dg_out, dx_own, dx_far, b_out, h_out, g_out, da_out,
                  xa, dya, ida, ga, rj, r0s, r1s, pm, pt, gs, b_s, g_s, h_s, da_s, o_s, slope, sp, zs, dg_tab, dgp, dgr,
                  wi, wo, yp, yr, yfar, ygot, dxp, dxr,
                  wi_sem, wo_sem, out_sem, small_s, small_r, sib_s, sib_r, cross_s, cross_r, fwd_s, fwd_r,
                  yd_s, yd_r, yx_s, yx_r, dd_s, dd_r, dg_s, dg_r):
    me = lax.axis_index("expert")
    sib, cross = me + 1 - 2 * lax.rem(me, 2), lax.rem(me + 2, 4)
    diag = lax.rem(sib + 2, 4)
    n_pairs = w_in.shape[0] // PAIR
    slots = 32 * SLOTS
    bf, f32 = jnp.bfloat16, jnp.float32

    def fetch_in(q, slot):
        return pltpu.make_async_copy(w_in.at[pl.ds(PAIR * q, PAIR)], wi.at[slot], wi_sem.at[slot])

    def fetch_out(q, slot):
        return pltpu.make_async_copy(w_out.at[pl.ds(PAIR * q, PAIR)], wo.at[slot], wo_sem.at[slot])

    def remote(src, dst, s, r, peer):
        return pltpu.make_async_remote_copy(src_ref=src, dst_ref=dst, send_sem=s, recv_sem=r,
                                            device_id={"expert": peer}, device_id_type=MESH)

    for q in range(AHEAD):
        fetch_in(q, q).start()
        fetch_out(q, q).start()

    barrier = pltpu.get_barrier_semaphore()
    for peer in (sib, cross, diag):
        pl.semaphore_signal(barrier, inc=1, device_id={"expert": peer}, device_id_type=MESH)
    pl.semaphore_wait(barrier, 3)

    small, over, near, far = [], [], [], []
    for k, peer in enumerate((cross, diag, sib)):
        small.append(remote(idx, ida.at[me], small_s.at[2 * k], small_r.at[2 * k], peer))
        small.append(remote(gate, ga.at[me], small_s.at[2 * k + 1], small_r.at[2 * k + 1], peer))
    for a, (src, dst) in enumerate(((x, xa), (dy, dya))):
        for c in range(2):
            rows = pl.ds(64 * c, 64)
            n = 2 * a + c
            over.append(remote(src.at[rows], dst.at[me, rows], cross_s.at[n], cross_r.at[n], cross))
            far.append(remote(dst.at[cross, rows], dst.at[cross, rows], fwd_s.at[n], fwd_r.at[n], sib))
        near.append(remote(src, dst.at[me], sib_s.at[a], sib_r.at[a], sib))
    for copy in small + over[:2] + near[:1] + over[2:] + near[1:]:
        copy.start()
    xa[me] = x[...]
    dya[me] = dy[...]
    ida[me] = idx[...]
    ga[me] = gate[...]
    zs[...] = jnp.zeros_like(zs)

    def forward(n):
        over[n].wait_recv()
        far[n].start()

    for copy in small:
        copy.wait_recv()
    tables(ida, me * 32, rj, r0s, r1s)
    slot_id = lax.broadcasted_iota(jnp.int32, (SLOTS, 128), 0).astype(f32)

    def one(e, _):
        total = jnp.zeros((SLOTS, 128), f32)
        for d in range(4):
            lanes = slice(128 * d, 128 * (d + 1))
            inside = (slot_id >= r0s[d, pl.ds(e, 1), :]) & (slot_id < r1s[d, pl.ds(e, 1), :])
            pm[slot_rows(e), lanes] = jnp.where(inside, 1.0, 0.0).astype(bf)
            for j in range(8):
                total = jnp.where(slot_id == rj[j, d, pl.ds(e, 1), :], ga[d, j:j + 1, :], total)
        gs[slot_rows(e), :] = jnp.sum(total, axis=1, keepdims=True)
        return 0

    lax.fori_loop(0, 32, one, 0)
    forward(0)

    def turn(c, _):
        at = pl.ds(pl.multiple_of(c * 128, 128), 128)
        pt[:, at] = pm[at, :].astype(f32).T.astype(bf)
        return 0

    lax.fori_loop(0, slots // 128, turn, 0)
    forward(1)
    near[0].wait_recv()
    far[0].wait_recv()
    far[1].wait_recv()

    def pick_x(c, _):
        at = pl.ds(pl.multiple_of(c * PICK, PICK), PICK)
        b_s[at, :] = dot(pm[at, :], xa[...].reshape(512, xa.shape[2])).astype(bf)
        return 0

    lax.fori_loop(0, slots // PICK, pick_x, 0)
    pltpu.make_async_copy(b_s, b_out, out_sem.at[0]).start()

    def fwd_step(i, _):
        slot = lax.rem(i, AHEAD)
        fetch_in(i, slot).wait()
        fetch_out(i, slot).wait()
        for p in range(PAIR):
            at = slot_rows(i * PAIR + p)
            a = dot(b_s[at, :], wi[slot, p])
            th = jnp.tanh(C0 * (a + C1 * (a * a * a)))
            cdf = 0.5 * (1.0 + th)
            slope[at, :] = cdf + 0.5 * a * (1.0 - th * th) * (C0 * (1.0 + 3.0 * C1 * (a * a)))
            h = (a * cdf).astype(bf)
            h_s[at, :] = h
            o = dot(h, wo[slot, p]).astype(bf)
            o_s[at, :] = o
            s = o.astype(f32) * gs[at, :]
            s1 = s.astype(bf)
            s = s - s1.astype(f32)
            s2 = s.astype(bf)
            s = s - s2.astype(f32)
            sp[0, at, :] = s1
            sp[1, at, :] = s2
            sp[2, at, :] = s.astype(bf)

        @pl.when(i < n_pairs - AHEAD)
        def _():
            fetch_in(i + AHEAD, slot).start()
            fetch_out(i + AHEAD, slot).start()

        @pl.when(i >= n_pairs - AHEAD)
        def _():
            fetch_in(2 * n_pairs - 1 - AHEAD - i, slot).start()
            fetch_out(2 * n_pairs - 1 - AHEAD - i, slot).start()

        for n, when in ((2, 1), (3, 4)):
            @pl.when(i == when)
            def _(n=n):
                forward(n)
        return 0

    lax.fori_loop(0, n_pairs, fwd_step, 0)
    pltpu.make_async_copy(h_s, h_out, out_sem.at[1]).start()

    def to_sib(part, got, s, r, n, k):
        return remote(part.at[n, sib if k == 0 else diag], got.at[n, k], s.at[n, k], r.at[n, k], sib)

    def y_part(n, _):
        lanes = pl.ds(pl.multiple_of(n * 256, 256), 256)
        out = dot(pt[...], sp[0, :, lanes]) + dot(pt[...], sp[1, :, lanes]) + dot(pt[...], sp[2, :, lanes])
        for d in range(4):
            yp[n, d] = out[128 * d:128 * (d + 1)]

        @pl.when(n > 0)
        def _():
            for k in range(2):
                to_sib(yp, yr, yd_s, yd_r, n - 1, k).start()
        return 0

    lax.fori_loop(0, 4, y_part, 0)
    near[1].wait_recv()
    far[2].wait_recv()
    far[3].wait_recv()
    for k in range(2):
        to_sib(yp, yr, yd_s, yd_r, 3, k).start()

    def pick_dy(c, _):
        at = pl.ds(pl.multiple_of(c * PICK, PICK), PICK)
        rows = dot(pm[at, :], dya[...].reshape(512, dya.shape[2]))
        g_s[at, :] = (rows * gs[at, :]).astype(bf)
        prod = rows * o_s[at, :].astype(f32)
        part = sum((prod[:, 128 * k:128 * (k + 1)] for k in range(1, 8)), prod[:, :128])
        for k in range(PICK // SLOTS):
            dg_tab[pl.ds(c * (PICK // SLOTS) + k, 1), :SLOTS] = jnp.sum(part[SLOTS * k:SLOTS * (k + 1)].T, axis=0, keepdims=True)
        return 0

    lax.fori_loop(0, slots // PICK, pick_dy, 0)
    pltpu.make_async_copy(g_s, g_out, out_sem.at[2]).start()
    for n in range(4):
        for k in range(2):
            to_sib(yp, yr, yd_s, yd_r, n, k).wait()
        yfar[n] = yp[n, cross] + yr[n, 1]
    for d in range(4):
        for j in range(8):
            at = rj[j, d].astype(jnp.int32)
            got = jnp.take_along_axis(dg_tab[...], jnp.maximum(at, 0), axis=1)
            dgp[d, j:j + 1, :] = jnp.sum(jnp.where(at >= 0, got, 0.0), axis=0, keepdims=True)
    y_cross = remote(yfar, ygot, yx_s, yx_r, cross)
    y_cross.start()
    dg_back = [remote(dgp.at[peer], dgr.at[k], dg_s.at[k], dg_r.at[k], peer) for k, peer in enumerate((cross, diag, sib))]

    def zero(n, like):
        return jnp.zeros((n, like.shape[1]), bf)

    def back_h(q, i):
        slot = lax.rem(i, AHEAD)
        g0, g1 = g_s[slot_rows(q * PAIR), :], g_s[slot_rows(q * PAIR + 1), :]
        both = dot(wo[slot, 0], jnp.concatenate([g0, zero(80, g0)], axis=0), ((1,), (1,)))
        both = both + dot(wo[slot, 1], jnp.concatenate([zero(64, g1), g1, zero(16, g1)], axis=0), ((1,), (1,)))
        dh = both.astype(bf).T.astype(f32)
        for p in range(PAIR):
            at = slot_rows(q * PAIR + p)
            da = (dh[64 * p:64 * p + SLOTS] * slope[at, :]).astype(bf)
            da_s[at, :] = da
            zs[lax.rem(i, 2), 64 * p:64 * p + SLOTS, 384 * p:384 * (p + 1)] = da

    def back_x(q, i):
        slot = lax.rem(i, AHEAD)
        wide = jnp.concatenate([wi[slot, 0], wi[slot, 1]], axis=1)
        both = dot(wide, zs[lax.rem(i, 2)], ((1,), (1,))).astype(bf).T
        for p in range(PAIR):
            sp[0, slot_rows(q * PAIR + p), :] = both[64 * p:64 * p + SLOTS]

    last = n_pairs - 1
    fetch_out(last, 0).wait()
    back_h(last, 0)
    fetch_out(last - AHEAD, 0).start()
    for copy in dg_back:
        copy.start()

    def bwd_step(i, _):
        fetch_in(last + 1 - i, lax.rem(i - 1, AHEAD)).wait()
        fetch_out(last - i, lax.rem(i, AHEAD)).wait()
        back_x(last + 1 - i, i - 1)
        back_h(last - i, i)

        @pl.when(i < n_pairs - AHEAD)
        def _():
            fetch_out(last - AHEAD - i, lax.rem(i, AHEAD)).start()

        @pl.when(i < n_pairs - AHEAD + 1)
        def _():
            fetch_in(last + 1 - AHEAD - i, lax.rem(i - 1, AHEAD)).start()
        return 0

    lax.fori_loop(1, n_pairs, bwd_step, 0)
    pltpu.make_async_copy(da_s, da_out, out_sem.at[3]).start()
    fetch_in(0, lax.rem(last, AHEAD)).wait()
    back_x(0, last)

    def dx_part(n, _):
        lanes = pl.ds(pl.multiple_of(n * 256, 256), 256)
        out = dot(pt[...], sp[0, :, lanes])
        for d in range(4):
            dxp[n, d] = out[128 * d:128 * (d + 1)]

        @pl.when(n > 0)
        def _():
            for k in range(2):
                to_sib(dxp, dxr, dd_s, dd_r, n - 1, k).start()
        return 0

    lax.fori_loop(0, 4, dx_part, 0)
    y_cross.wait()
    for k in range(2):
        to_sib(dxp, dxr, dd_s, dd_r, 3, k).start()
    for n in range(4):
        lanes = slice(256 * n, 256 * (n + 1))
        y_out[:, lanes] = (x[:, lanes].astype(f32) + (yp[n, me] + yr[n, 0] + ygot[n])).astype(bf)
    for copy in dg_back:
        copy.wait()
    dg_out[...] = dgp[me] + (dgr[0] + (dgr[1] + dgr[2]))
    for n in range(4):
        lanes = slice(256 * n, 256 * (n + 1))
        for k in range(2):
            to_sib(dxp, dxr, dd_s, dd_r, n, k).wait()
        dx_own[:, lanes] = dxp[n, me] + dxr[n, 0]
        dx_far[:, lanes] = dxp[n, cross] + dxr[n, 1]
    for copy in small + over + near + far:
        copy.wait_send()
    for k, (src, dst) in enumerate(((b_s, b_out), (h_s, h_out), (g_s, g_out), (da_s, da_out))):
        pltpu.make_async_copy(src, dst, out_sem.at[k]).wait()


def experts(x, dy, idx_t, gate_t, w_in, w_out):
    n_e, d_model, d_ff = w_in.shape
    slots = n_e * SLOTS
    bf, f32 = jnp.bfloat16, jnp.float32
    vmem, hbm = pl.BlockSpec(memory_space=pltpu.VMEM), pl.BlockSpec(memory_space=pl.ANY)
    shape, buf, dma = jax.ShapeDtypeStruct, pltpu.VMEM, pltpu.SemaphoreType.DMA
    return pl.pallas_call(
        expert_kernel,
        out_shape=[shape((128, d_model), bf), shape((8, 128), f32), shape((128, d_model), f32), shape((128, d_model), f32),
                   shape((slots, d_model), bf), shape((slots, d_ff), bf), shape((slots, d_model), bf), shape((slots, d_ff), bf)],
        in_specs=[vmem] * 4 + [hbm] * 2,
        out_specs=[vmem] * 4 + [hbm] * 4,
        scratch_shapes=[
            buf((4, 128, d_model), bf), buf((4, 128, d_model), bf), buf((4, 8, 128), jnp.int32), buf((4, 8, 128), f32),
            buf((8, 4, n_e, 128), f32), buf((4, n_e, 128), f32), buf((4, n_e, 128), f32),
            buf((slots, 512), bf), buf((512, slots), bf), buf((slots, 1), f32),
            buf((slots, d_model), bf), buf((slots, d_model), bf), buf((slots, d_ff), bf), buf((slots, d_ff), bf),
            buf((slots, d_model), bf), buf((slots, d_ff), f32), buf((3, slots, d_model), bf), buf((2, 128, PAIR * d_ff), bf),
            buf((n_e, 128), f32), buf((4, 8, 128), f32), buf((3, 8, 128), f32),
            buf((AHEAD, PAIR, d_model, d_ff), bf), buf((AHEAD, PAIR, d_ff, d_model), bf),
            buf((4, 4, 128, 256), f32), buf((4, 2, 128, 256), f32), buf((4, 128, 256), f32), buf((4, 128, 256), f32),
            buf((4, 4, 128, 256), f32), buf((4, 2, 128, 256), f32),
            dma((AHEAD,)), dma((AHEAD,)), dma((4,)), dma((6,)), dma((6,)), dma((2,)), dma((2,)), dma((4,)), dma((4,)),
            dma((4,)), dma((4,)), dma((4, 2)), dma((4, 2)), dma(()), dma(()), dma((4, 2)), dma((4, 2)), dma((3,)), dma((3,))],
        compiler_params=pltpu.CompilerParams(collective_id=0, has_side_effects=True, vmem_limit_bytes=63 * 1024 * 1024),
        cost_estimate=pl.CostEstimate(flops=8 * slots * d_model * d_ff, bytes_accessed=8 * n_e * d_model * d_ff, transcendentals=0),
    )(x, dy, idx_t, gate_t, w_in, w_out)


def weight_kernel(b, h, g, da, y, dg, dw_in, dw_out, y_out, dg_out):
    for p in range(PAIR):
        at = slice(p * SLOTS, (p + 1) * SLOTS)
        dw_in[p] = dot(b[at, :], da[at, :], ((0,), (0,))).astype(jnp.bfloat16)
        dw_out[p] = dot(h[at, :], g[at, :], ((0,), (0,))).astype(jnp.bfloat16)

    @pl.when(pl.program_id(0) == 0)
    def _():
        y_out[...] = y[...]
        dg_out[...] = dg[...]


def weight_grads(b, h, g, da, y, dg, n_e):
    d_model, d_ff = b.shape[1], h.shape[1]
    rows = PAIR * SLOTS
    whole = [pl.BlockSpec(y.shape, lambda i: (0, 0)), pl.BlockSpec(dg.shape, lambda i: (0, 0))]
    return pl.pallas_call(
        weight_kernel,
        grid=(n_e // PAIR,),
        out_shape=[jax.ShapeDtypeStruct((n_e, d_model, d_ff), jnp.bfloat16), jax.ShapeDtypeStruct((n_e, d_ff, d_model), jnp.bfloat16),
                   jax.ShapeDtypeStruct(y.shape, y.dtype), jax.ShapeDtypeStruct(dg.shape, dg.dtype)],
        in_specs=[pl.BlockSpec((rows, d_model), lambda i: (i, 0)), pl.BlockSpec((rows, d_ff), lambda i: (i, 0)),
                  pl.BlockSpec((rows, d_model), lambda i: (i, 0)), pl.BlockSpec((rows, d_ff), lambda i: (i, 0))] + whole,
        out_specs=[pl.BlockSpec((PAIR, d_model, d_ff), lambda i: (i, 0, 0)), pl.BlockSpec((PAIR, d_ff, d_model), lambda i: (i, 0, 0))] + whole,
        compiler_params=pltpu.CompilerParams(vmem_limit_bytes=62 * 1024 * 1024),
        cost_estimate=pl.CostEstimate(flops=4 * n_e * SLOTS * d_model * d_ff, bytes_accessed=4 * n_e * d_model * d_ff, transcendentals=0),
    )(b, h, g, da, y, dg)


def solution(mesh):
    tok_spec = P(('data', 'expert'), None)
    weight_spec = P('expert', None, None)
    grad_spec = P(('data', 'expert'), None, None)
    to_cross = [(i, i ^ 2) for i in range(4)]

    def device_pass(x_in, expert_idx, gate_weight, grad_y, w_in, w_out):
        y_mid, dg, dx_own, dx_far, b, h, g, da = experts(x_in, grad_y, expert_idx.T, gate_weight.T, w_in, w_out)
        dx_got = lax.ppermute(dx_far, 'expert', to_cross)
        grad_w_in, grad_w_out, y_out, dg = weight_grads(b, h, g, da, y_mid, dg, w_in.shape[0])
        grad_x = (grad_y.astype(jnp.float32) + (dx_own + dx_got)).astype(jnp.bfloat16)
        return y_out, grad_x, dg.T, grad_w_in, grad_w_out

    return jax.shard_map(device_pass, mesh=mesh,
                         in_specs=(tok_spec, tok_spec, tok_spec, tok_spec, weight_spec, weight_spec),
                         out_specs=(tok_spec, tok_spec, tok_spec, grad_spec, grad_spec), check_vma=False)
```

```python
import functools

import jax
import jax.numpy as jnp
from jax import lax
from jax.experimental import pallas as pl
from jax.experimental.pallas import tpu as pltpu
from jax.sharding import PartitionSpec as P

MESH = pl.DeviceIdType.MESH
CAP = 40
SLOTS = 48
PAIR = 2
AHEAD = 4
PICK = 384
C0 = 0.7978845608028654
C1 = 0.044715


def dot(a, b, dims=((1,), (0,))):
    return lax.dot_general(a, b, (dims, ((), ())), preferred_element_type=jnp.float32)


def tables(ids_all, first, rj, r0s, r1s):
    eid = lax.broadcasted_iota(jnp.int32, (32, 128), 0) + first
    earlier = (lax.broadcasted_iota(jnp.int32, (128, 128), 0) < lax.broadcasted_iota(jnp.int32, (128, 128), 1)).astype(jnp.bfloat16)
    offset = jnp.zeros((32, 1), jnp.float32)
    for d in range(4):
        ids = ids_all[d]
        hits = [(ids[j:j + 1, :] == eid).astype(jnp.float32) for j in range(8)]
        count = sum(hits[1:], hits[0])
        rank = dot(count.astype(jnp.bfloat16), earlier) + offset
        r0s[d] = rank
        for j in range(8):
            rj[j, d] = jnp.where((hits[j] > 0.0) & (rank < CAP), rank, -1.0)
            rank = rank + hits[j]
        r1s[d] = jnp.minimum(rank, CAP)
        offset = offset + jnp.sum(count, axis=1, keepdims=True)


def slot_rows(e):
    return pl.ds(pl.multiple_of(e * SLOTS, SLOTS), SLOTS)


def expert_kernel(x, dy, idx, gate, w_in, w_out, y_out, dg_out, dx_own, dx_far, b_s, h_s, g_s, da_s,
                  xa, dya, ida, ga, rj, r0s, r1s, pm, pt, gs, o_s, slope, sp, zs, dg_tab, dgp, dgr,
                  wi, wo, yp, yr, yfar, ygot, dxp, dxr,
                  wi_sem, wo_sem, small_s, small_r, sib_s, sib_r, cross_s, cross_r, fwd_s, fwd_r,
                  yd_s, yd_r, yx_s, yx_r, dd_s, dd_r, dg_s, dg_r):
    me = lax.axis_index("expert")
    sib, cross = me + 1 - 2 * lax.rem(me, 2), lax.rem(me + 2, 4)
    diag = lax.rem(sib + 2, 4)
    n_pairs = w_in.shape[0] // PAIR
    slots = 32 * SLOTS
    bf, f32 = jnp.bfloat16, jnp.float32

    def fetch_in(q, slot):
        return pltpu.make_async_copy(w_in.at[pl.ds(PAIR * q, PAIR)], wi.at[slot], wi_sem.at[slot])

    def fetch_out(q, slot):
        return pltpu.make_async_copy(w_out.at[pl.ds(PAIR * q, PAIR)], wo.at[slot], wo_sem.at[slot])

    def remote(src, dst, s, r, peer):
        return pltpu.make_async_remote_copy(src_ref=src, dst_ref=dst, send_sem=s, recv_sem=r,
                                            device_id={"expert": peer}, device_id_type=MESH)

    for q in range(AHEAD):
        fetch_in(q, q).start()
        fetch_out(q, q).start()

    barrier = pltpu.get_barrier_semaphore()
    for peer in (sib, cross, diag):
        pl.semaphore_signal(barrier, inc=1, device_id={"expert": peer}, device_id_type=MESH)
    pl.semaphore_wait(barrier, 3)

    small, over, near, far = [], [], [], []
    for k, peer in enumerate((cross, diag, sib)):
        small.append(remote(idx, ida.at[me], small_s.at[2 * k], small_r.at[2 * k], peer))
        small.append(remote(gate, ga.at[me], small_s.at[2 * k + 1], small_r.at[2 * k + 1], peer))
    for a, (src, dst) in enumerate(((x, xa), (dy, dya))):
        for c in range(2):
            rows = pl.ds(64 * c, 64)
            n = 2 * a + c
            over.append(remote(src.at[rows], dst.at[me, rows], cross_s.at[n], cross_r.at[n], cross))
            far.append(remote(dst.at[cross, rows], dst.at[cross, rows], fwd_s.at[n], fwd_r.at[n], sib))
        near.append(remote(src, dst.at[me], sib_s.at[a], sib_r.at[a], sib))
    for copy in small + over[:2] + near[:1] + over[2:] + near[1:]:
        copy.start()
    xa[me] = x[...]
    dya[me] = dy[...]
    ida[me] = idx[...]
    ga[me] = gate[...]
    zs[...] = jnp.zeros_like(zs)

    def forward(n):
        over[n].wait_recv()
        far[n].start()

    for copy in small:
        copy.wait_recv()
    tables(ida, me * 32, rj, r0s, r1s)
    slot_id = lax.broadcasted_iota(jnp.int32, (SLOTS, 128), 0).astype(f32)

    def one(e, _):
        total = jnp.zeros((SLOTS, 128), f32)
        for d in range(4):
            lanes = slice(128 * d, 128 * (d + 1))
            inside = (slot_id >= r0s[d, pl.ds(e, 1), :]) & (slot_id < r1s[d, pl.ds(e, 1), :])
            pm[slot_rows(e), lanes] = jnp.where(inside, 1.0, 0.0).astype(bf)
            for j in range(8):
                total = jnp.where(slot_id == rj[j, d, pl.ds(e, 1), :], ga[d, j:j + 1, :], total)
        gs[slot_rows(e), :] = jnp.sum(total, axis=1, keepdims=True)
        return 0

    lax.fori_loop(0, 32, one, 0)
    forward(0)

    def turn(c, _):
        at = pl.ds(pl.multiple_of(c * 128, 128), 128)
        pt[:, at] = pm[at, :].astype(f32).T.astype(bf)
        return 0

    lax.fori_loop(0, slots // 128, turn, 0)
    forward(1)
    near[0].wait_recv()
    far[0].wait_recv()
    far[1].wait_recv()

    def pick_x(c, _):
        at = pl.ds(pl.multiple_of(c * PICK, PICK), PICK)
        b_s[at, :] = dot(pm[at, :], xa[...].reshape(512, xa.shape[2])).astype(bf)
        return 0

    lax.fori_loop(0, slots // PICK, pick_x, 0)

    def fwd_step(i, _):
        slot = lax.rem(i, AHEAD)
        fetch_in(i, slot).wait()
        fetch_out(i, slot).wait()
        for p in range(PAIR):
            at = slot_rows(i * PAIR + p)
            a = dot(b_s[at, :], wi[slot, p])
            th = jnp.tanh(C0 * (a + C1 * (a * a * a)))
            cdf = 0.5 * (1.0 + th)
            slope[at, :] = cdf + 0.5 * a * (1.0 - th * th) * (C0 * (1.0 + 3.0 * C1 * (a * a)))
            h = (a * cdf).astype(bf)
            h_s[at, :] = h
            o = dot(h, wo[slot, p]).astype(bf)
            o_s[at, :] = o
            s = o.astype(f32) * gs[at, :]
            s1 = s.astype(bf)
            s = s - s1.astype(f32)
            s2 = s.astype(bf)
            s = s - s2.astype(f32)
            sp[0, at, :] = s1
            sp[1, at, :] = s2
            sp[2, at, :] = s.astype(bf)

        @pl.when(i < n_pairs - AHEAD)
        def _():
            fetch_in(i + AHEAD, slot).start()
            fetch_out(i + AHEAD, slot).start()

        @pl.when(i >= n_pairs - AHEAD)
        def _():
            fetch_in(2 * n_pairs - 1 - AHEAD - i, slot).start()
            fetch_out(2 * n_pairs - 1 - AHEAD - i, slot).start()

        for n, when in ((2, 1), (3, 4)):
            @pl.when(i == when)
            def _(n=n):
                forward(n)
        return 0

    lax.fori_loop(0, n_pairs, fwd_step, 0)

    def to_sib(part, got, s, r, n, k):
        return remote(part.at[n, sib if k == 0 else diag], got.at[n, k], s.at[n, k], r.at[n, k], sib)

    def y_part(n, _):
        lanes = pl.ds(pl.multiple_of(n * 256, 256), 256)
        out = dot(pt[...], sp[0, :, lanes]) + dot(pt[...], sp[1, :, lanes]) + dot(pt[...], sp[2, :, lanes])
        for d in range(4):
            yp[n, d] = out[128 * d:128 * (d + 1)]

        @pl.when(n > 0)
        def _():
            for k in range(2):
                to_sib(yp, yr, yd_s, yd_r, n - 1, k).start()
        return 0

    lax.fori_loop(0, 4, y_part, 0)
    near[1].wait_recv()
    far[2].wait_recv()
    far[3].wait_recv()
    for k in range(2):
        to_sib(yp, yr, yd_s, yd_r, 3, k).start()

    def pick_dy(c, _):
        at = pl.ds(pl.multiple_of(c * PICK, PICK), PICK)
        rows = dot(pm[at, :], dya[...].reshape(512, dya.shape[2]))
        g_s[at, :] = (rows * gs[at, :]).astype(bf)
        prod = rows * o_s[at, :].astype(f32)
        part = sum((prod[:, 128 * k:128 * (k + 1)] for k in range(1, 8)), prod[:, :128])
        for k in range(PICK // SLOTS):
            dg_tab[pl.ds(c * (PICK // SLOTS) + k, 1), :SLOTS] = jnp.sum(part[SLOTS * k:SLOTS * (k + 1)].T, axis=0, keepdims=True)
        return 0

    lax.fori_loop(0, slots // PICK, pick_dy, 0)
    for n in range(4):
        for k in range(2):
            to_sib(yp, yr, yd_s, yd_r, n, k).wait()
        yfar[n] = yp[n, cross] + yr[n, 1]
    for d in range(4):
        for j in range(8):
            at = rj[j, d].astype(jnp.int32)
            got = jnp.take_along_axis(dg_tab[...], jnp.maximum(at, 0), axis=1)
            dgp[d, j:j + 1, :] = jnp.sum(jnp.where(at >= 0, got, 0.0), axis=0, keepdims=True)
    y_cross = remote(yfar, ygot, yx_s, yx_r, cross)
    y_cross.start()
    dg_back = [remote(dgp.at[peer], dgr.at[k], dg_s.at[k], dg_r.at[k], peer) for k, peer in enumerate((cross, diag, sib))]

    def zero(n, like):
        return jnp.zeros((n, like.shape[1]), bf)

    def back_h(q, i):
        slot = lax.rem(i, AHEAD)
        g0, g1 = g_s[slot_rows(q * PAIR), :], g_s[slot_rows(q * PAIR + 1), :]
        both = dot(wo[slot, 0], jnp.concatenate([g0, zero(80, g0)], axis=0), ((1,), (1,)))
        both = both + dot(wo[slot, 1], jnp.concatenate([zero(64, g1), g1, zero(16, g1)], axis=0), ((1,), (1,)))
        dh = both.astype(bf).T.astype(f32)
        for p in range(PAIR):
            at = slot_rows(q * PAIR + p)
            da = (dh[64 * p:64 * p + SLOTS] * slope[at, :]).astype(bf)
            da_s[at, :] = da
            zs[lax.rem(i, 2), 64 * p:64 * p + SLOTS, 384 * p:384 * (p + 1)] = da

    def back_x(q, i):
        slot = lax.rem(i, AHEAD)
        wide = jnp.concatenate([wi[slot, 0], wi[slot, 1]], axis=1)
        both = dot(wide, zs[lax.rem(i, 2)], ((1,), (1,))).astype(bf).T
        for p in range(PAIR):
            sp[0, slot_rows(q * PAIR + p), :] = both[64 * p:64 * p + SLOTS]

    last = n_pairs - 1
    fetch_out(last, 0).wait()
    back_h(last, 0)
    fetch_out(last - AHEAD, 0).start()
    for copy in dg_back:
        copy.start()

    def bwd_step(i, _):
        fetch_in(last + 1 - i, lax.rem(i - 1, AHEAD)).wait()
        fetch_out(last - i, lax.rem(i, AHEAD)).wait()
        back_x(last + 1 - i, i - 1)
        back_h(last - i, i)

        @pl.when(i < n_pairs - AHEAD)
        def _():
            fetch_out(last - AHEAD - i, lax.rem(i, AHEAD)).start()

        @pl.when(i < n_pairs - AHEAD + 1)
        def _():
            fetch_in(last + 1 - AHEAD - i, lax.rem(i - 1, AHEAD)).start()
        return 0

    lax.fori_loop(1, n_pairs, bwd_step, 0)
    fetch_in(0, lax.rem(last, AHEAD)).wait()
    back_x(0, last)

    def dx_part(n, _):
        lanes = pl.ds(pl.multiple_of(n * 256, 256), 256)
        out = dot(pt[...], sp[0, :, lanes])
        for d in range(4):
            dxp[n, d] = out[128 * d:128 * (d + 1)]

        @pl.when(n > 0)
        def _():
            for k in range(2):
                to_sib(dxp, dxr, dd_s, dd_r, n - 1, k).start()
        return 0

    lax.fori_loop(0, 4, dx_part, 0)
    y_cross.wait()
    for k in range(2):
        to_sib(dxp, dxr, dd_s, dd_r, 3, k).start()
    for n in range(4):
        lanes = slice(256 * n, 256 * (n + 1))
        y_out[:, lanes] = (x[:, lanes].astype(f32) + (yp[n, me] + yr[n, 0] + ygot[n])).astype(bf)
    for copy in dg_back:
        copy.wait()
    dg_out[...] = dgp[me] + (dgr[0] + (dgr[1] + dgr[2]))
    for n in range(4):
        lanes = slice(256 * n, 256 * (n + 1))
        for k in range(2):
            to_sib(dxp, dxr, dd_s, dd_r, n, k).wait()
        dx_own[:, lanes] = dxp[n, me] + dxr[n, 0]
        dx_far[:, lanes] = dxp[n, cross] + dxr[n, 1]
    for copy in small + over + near + far:
        copy.wait_send()


def experts(x, dy, idx_t, gate_t, w_in, w_out):
    n_e, d_model, d_ff = w_in.shape
    slots = n_e * SLOTS
    bf, f32 = jnp.bfloat16, jnp.float32
    vmem, hbm = pl.BlockSpec(memory_space=pltpu.VMEM), pl.BlockSpec(memory_space=pl.ANY)
    buf, dma = pltpu.VMEM, pltpu.SemaphoreType.DMA
    return pl.pallas_call(
        expert_kernel,
        out_shape=[buf((128, d_model), bf), buf((8, 128), f32), buf((128, d_model), f32), buf((128, d_model), f32),
                   buf((slots, d_model), bf), buf((slots, d_ff), bf), buf((slots, d_model), bf), buf((slots, d_ff), bf)],
        in_specs=[vmem] * 4 + [hbm] * 2,
        out_specs=[vmem] * 8,
        scratch_shapes=[
            buf((4, 128, d_model), bf), buf((4, 128, d_model), bf), buf((4, 8, 128), jnp.int32), buf((4, 8, 128), f32),
            buf((8, 4, n_e, 128), f32), buf((4, n_e, 128), f32), buf((4, n_e, 128), f32),
            buf((slots, 512), bf), buf((512, slots), bf), buf((slots, 1), f32),
            buf((slots, d_model), bf), buf((slots, d_ff), f32), buf((3, slots, d_model), bf), buf((2, 128, PAIR * d_ff), bf),
            buf((n_e, 128), f32), buf((4, 8, 128), f32), buf((3, 8, 128), f32),
            buf((AHEAD, PAIR, d_model, d_ff), bf), buf((AHEAD, PAIR, d_ff, d_model), bf),
            buf((4, 4, 128, 256), f32), buf((4, 2, 128, 256), f32), buf((4, 128, 256), f32), buf((4, 128, 256), f32),
            buf((4, 4, 128, 256), f32), buf((4, 2, 128, 256), f32),
            dma((AHEAD,)), dma((AHEAD,)), dma((6,)), dma((6,)), dma((2,)), dma((2,)), dma((4,)), dma((4,)),
            dma((4,)), dma((4,)), dma((4, 2)), dma((4, 2)), dma(()), dma(()), dma((4, 2)), dma((4, 2)), dma((3,)), dma((3,))],
        compiler_params=pltpu.CompilerParams(collective_id=0, has_side_effects=True, vmem_limit_bytes=53 * 1024 * 1024),
        cost_estimate=pl.CostEstimate(flops=8 * slots * d_model * d_ff, bytes_accessed=8 * n_e * d_model * d_ff, transcendentals=0),
    )(x, dy, idx_t, gate_t, w_in, w_out)


def weight_kernel(b, h, g, da, y, dg, dw_in, dw_out, y_out, dg_out):
    for p in range(PAIR):
        at = slot_rows(pl.program_id(0) * PAIR + p)
        dw_in[p] = dot(b[at, :], da[at, :], ((0,), (0,))).astype(jnp.bfloat16)
        dw_out[p] = dot(h[at, :], g[at, :], ((0,), (0,))).astype(jnp.bfloat16)

    @pl.when(pl.program_id(0) == 0)
    def _():
        y_out[...] = y[...]
        dg_out[...] = dg[...]


def weight_grads(b, h, g, da, y, dg, n_e):
    d_model, d_ff = b.shape[1], h.shape[1]
    whole = [pl.BlockSpec(y.shape, lambda i: (0, 0)), pl.BlockSpec(dg.shape, lambda i: (0, 0))]
    return pl.pallas_call(
        weight_kernel,
        grid=(n_e // PAIR,),
        out_shape=[jax.ShapeDtypeStruct((n_e, d_model, d_ff), jnp.bfloat16), jax.ShapeDtypeStruct((n_e, d_ff, d_model), jnp.bfloat16),
                   jax.ShapeDtypeStruct(y.shape, y.dtype), jax.ShapeDtypeStruct(dg.shape, dg.dtype)],
        in_specs=[pl.BlockSpec(memory_space=pltpu.VMEM)] * 6,
        out_specs=[pl.BlockSpec((PAIR, d_model, d_ff), lambda i: (i, 0, 0)), pl.BlockSpec((PAIR, d_ff, d_model), lambda i: (i, 0, 0))] + whole,
        compiler_params=pltpu.CompilerParams(vmem_limit_bytes=40 * 1024 * 1024),
        cost_estimate=pl.CostEstimate(flops=4 * n_e * SLOTS * d_model * d_ff, bytes_accessed=4 * n_e * d_model * d_ff, transcendentals=0),
    )(b, h, g, da, y, dg)


def solution(mesh):
    tok_spec = P(('data', 'expert'), None)
    weight_spec = P('expert', None, None)
    grad_spec = P(('data', 'expert'), None, None)
    to_cross = [(i, i ^ 2) for i in range(4)]

    def device_pass(x_in, expert_idx, gate_weight, grad_y, w_in, w_out):
        y_mid, dg, dx_own, dx_far, b, h, g, da = experts(x_in, grad_y, expert_idx.T, gate_weight.T, w_in, w_out)
        dx_got = lax.ppermute(dx_far, 'expert', to_cross)
        grad_w_in, grad_w_out, y_out, dg = weight_grads(b, h, g, da, y_mid, dg, w_in.shape[0])
        grad_x = (grad_y.astype(jnp.float32) + (dx_own + dx_got)).astype(jnp.bfloat16)
        return y_out, grad_x, dg.T, grad_w_in, grad_w_out

    return jax.shard_map(device_pass, mesh=mesh,
                         in_specs=(tok_spec, tok_spec, tok_spec, tok_spec, weight_spec, weight_spec),
                         out_specs=(tok_spec, tok_spec, tok_spec, grad_spec, grad_spec), check_vma=False)
```

```python
import functools

import jax
import jax.numpy as jnp
from jax import lax
from jax.experimental import pallas as pl
from jax.experimental.pallas import tpu as pltpu
from jax.sharding import PartitionSpec as P

MESH = pl.DeviceIdType.MESH
CAP = 40
SLOTS = 48
PAIR = 2
RING = 4
AHEAD = 4
PICK = 384
C0 = 0.7978845608028654
C1 = 0.044715


def dot(a, b, dims=((1,), (0,))):
    return lax.dot_general(a, b, (dims, ((), ())), preferred_element_type=jnp.float32)


def tables(ids_all, first, rj, r0s, r1s):
    eid = lax.broadcasted_iota(jnp.int32, (32, 128), 0) + first
    earlier = (lax.broadcasted_iota(jnp.int32, (128, 128), 0) < lax.broadcasted_iota(jnp.int32, (128, 128), 1)).astype(jnp.bfloat16)
    offset = jnp.zeros((32, 1), jnp.float32)
    for d in range(4):
        ids = ids_all[d]
        hits = [(ids[j:j + 1, :] == eid).astype(jnp.float32) for j in range(8)]
        count = sum(hits[1:], hits[0])
        rank = dot(count.astype(jnp.bfloat16), earlier) + offset
        r0s[d] = rank
        for j in range(8):
            rj[j, d] = jnp.where((hits[j] > 0.0) & (rank < CAP), rank, -1.0)
            rank = rank + hits[j]
        r1s[d] = jnp.minimum(rank, CAP)
        offset = offset + jnp.sum(count, axis=1, keepdims=True)


def slot_rows(e):
    return pl.ds(pl.multiple_of(e * SLOTS, SLOTS), SLOTS)


def expert_kernel(x_hbm, dy_hbm, idx_hbm, gate_hbm, w_in, w_out, y_out, dg_out, dx_own, dx_far, b_s, h_s, g_s, da_s,
                  x, dy, idx, gate, xa, dya, ida, ga, rj, r0s, r1s, pm, pt, gs, o_s, slope, sp, zs, dg_tab, dgp, dgr,
                  wi, wo, yp, yr, yfar, ygot, dxp, dxr,
                  arg_sem, wi_sem, wo_sem, small_s, small_r, sib_s, sib_r, cross_s, cross_r, fwd_s, fwd_r,
                  yd_s, yd_r, yx_s, yx_r, dd_s, dd_r, dg_s, dg_r):
    me = lax.axis_index("expert")
    sib, cross = me + 1 - 2 * lax.rem(me, 2), lax.rem(me + 2, 4)
    diag = lax.rem(sib + 2, 4)
    n_pairs = w_in.shape[0] // PAIR
    slots = 32 * SLOTS
    bf, f32 = jnp.bfloat16, jnp.float32

    def fetch_in(q, slot):
        return pltpu.make_async_copy(w_in.at[pl.ds(PAIR * q, PAIR)], wi.at[slot], wi_sem.at[slot])

    def fetch_out(q, slot):
        return pltpu.make_async_copy(w_out.at[pl.ds(PAIR * q, PAIR)], wo.at[slot], wo_sem.at[slot])

    def remote(src, dst, s, r, peer):
        return pltpu.make_async_remote_copy(src_ref=src, dst_ref=dst, send_sem=s, recv_sem=r,
                                            device_id={"expert": peer}, device_id_type=MESH)

    barrier = pltpu.get_barrier_semaphore()
    for peer in (sib, cross, diag):
        pl.semaphore_signal(barrier, inc=1, device_id={"expert": peer}, device_id_type=MESH)
    args = [pltpu.make_async_copy(src, dst, arg_sem.at[k])
            for k, (src, dst) in enumerate(((idx_hbm, idx), (gate_hbm, gate), (x_hbm, x), (dy_hbm, dy)))]
    for copy in args:
        copy.start()
    for q in range(AHEAD):
        fetch_in(q, q).start()
        fetch_out(q, q).start()
    zs[...] = jnp.zeros_like(zs)
    for copy in args:
        copy.wait()
    pl.semaphore_wait(barrier, 3)

    small, over, near, far = [], [], [], []
    for k, peer in enumerate((cross, diag, sib)):
        small.append(remote(idx, ida.at[me], small_s.at[2 * k], small_r.at[2 * k], peer))
        small.append(remote(gate, ga.at[me], small_s.at[2 * k + 1], small_r.at[2 * k + 1], peer))
    for a, (src, dst) in enumerate(((x, xa), (dy, dya))):
        for c in range(2):
            rows = pl.ds(64 * c, 64)
            n = 2 * a + c
            over.append(remote(src.at[rows], dst.at[me, rows], cross_s.at[n], cross_r.at[n], cross))
            far.append(remote(dst.at[cross, rows], dst.at[cross, rows], fwd_s.at[n], fwd_r.at[n], sib))
        near.append(remote(src, dst.at[me], sib_s.at[a], sib_r.at[a], sib))
    for copy in small + over[:2] + near[:1] + over[2:] + near[1:]:
        copy.start()
    xa[me] = x[...]
    dya[me] = dy[...]
    ida[me] = idx[...]
    ga[me] = gate[...]

    def forward(n):
        over[n].wait_recv()
        far[n].start()

    for copy in small:
        copy.wait_recv()
    tables(ida, me * 32, rj, r0s, r1s)
    slot_id = lax.broadcasted_iota(jnp.int32, (SLOTS, 128), 0).astype(f32)

    def one(e, _):
        total = jnp.zeros((SLOTS, 128), f32)
        for d in range(4):
            lanes = slice(128 * d, 128 * (d + 1))
            inside = (slot_id >= r0s[d, pl.ds(e, 1), :]) & (slot_id < r1s[d, pl.ds(e, 1), :])
            pm[slot_rows(e), lanes] = jnp.where(inside, 1.0, 0.0).astype(bf)
            for j in range(8):
                total = jnp.where(slot_id == rj[j, d, pl.ds(e, 1), :], ga[d, j:j + 1, :], total)
        gs[slot_rows(e), :] = jnp.sum(total, axis=1, keepdims=True)
        return 0

    lax.fori_loop(0, 32, one, 0)
    forward(0)

    def turn(c, _):
        at = pl.ds(pl.multiple_of(c * 128, 128), 128)
        pt[:, at] = pm[at, :].astype(f32).T.astype(bf)
        return 0

    lax.fori_loop(0, slots // 128, turn, 0)
    forward(1)
    near[0].wait_recv()
    far[0].wait_recv()
    far[1].wait_recv()

    def pick_x(c, _):
        at = pl.ds(pl.multiple_of(c * PICK, PICK), PICK)
        b_s[at, :] = dot(pm[at, :], xa[...].reshape(512, xa.shape[2])).astype(bf)
        return 0

    lax.fori_loop(0, slots // PICK, pick_x, 0)

    def fwd_step(i, _):
        slot = lax.rem(i, AHEAD)
        fetch_in(i, slot).wait()
        fetch_out(i, slot).wait()
        for p in range(PAIR):
            at = slot_rows(i * PAIR + p)
            a = dot(b_s[at, :], wi[slot, p])
            th = jnp.tanh(C0 * (a + C1 * (a * a * a)))
            cdf = 0.5 * (1.0 + th)
            slope[at, :] = cdf + 0.5 * a * (1.0 - th * th) * (C0 * (1.0 + 3.0 * C1 * (a * a)))
            h = (a * cdf).astype(bf)
            h_s[at, :] = h
            o = dot(h, wo[slot, p]).astype(bf)
            o_s[at, :] = o
            s = o.astype(f32) * gs[at, :]
            s1 = s.astype(bf)
            s = s - s1.astype(f32)
            s2 = s.astype(bf)
            s = s - s2.astype(f32)
            sp[0, at, :] = s1
            sp[1, at, :] = s2
            sp[2, at, :] = s.astype(bf)

        @pl.when(i < n_pairs - AHEAD)
        def _():
            fetch_in(i + AHEAD, slot).start()
            fetch_out(i + AHEAD, slot).start()

        @pl.when(i >= n_pairs - AHEAD)
        def _():
            fetch_in(2 * n_pairs - 1 - AHEAD - i, slot).start()
            fetch_out(2 * n_pairs - 1 - AHEAD - i, slot).start()

        for n, when in ((2, 1), (3, 4)):
            @pl.when(i == when)
            def _(n=n):
                forward(n)
        return 0

    lax.fori_loop(0, n_pairs, fwd_step, 0)

    def to_sib(part, got, s, r, n, k):
        return remote(part.at[n, sib if k == 0 else diag], got.at[n, k], s.at[n, k], r.at[n, k], sib)

    def y_part(n, _):
        lanes = pl.ds(pl.multiple_of(n * 256, 256), 256)
        out = dot(pt[...], sp[0, :, lanes]) + dot(pt[...], sp[1, :, lanes]) + dot(pt[...], sp[2, :, lanes])
        for d in range(4):
            yp[n, d] = out[128 * d:128 * (d + 1)]

        @pl.when(n > 0)
        def _():
            for k in range(2):
                to_sib(yp, yr, yd_s, yd_r, n - 1, k).start()
        return 0

    lax.fori_loop(0, 4, y_part, 0)
    near[1].wait_recv()
    far[2].wait_recv()
    far[3].wait_recv()
    for k in range(2):
        to_sib(yp, yr, yd_s, yd_r, 3, k).start()

    def pick_dy(c, _):
        at = pl.ds(pl.multiple_of(c * PICK, PICK), PICK)
        rows = dot(pm[at, :], dya[...].reshape(512, dya.shape[2]))
        g_s[at, :] = (rows * gs[at, :]).astype(bf)
        prod = rows * o_s[at, :].astype(f32)
        part = sum((prod[:, 128 * k:128 * (k + 1)] for k in range(1, 8)), prod[:, :128])
        for k in range(PICK // SLOTS):
            dg_tab[pl.ds(c * (PICK // SLOTS) + k, 1), :SLOTS] = jnp.sum(part[SLOTS * k:SLOTS * (k + 1)].T, axis=0, keepdims=True)
        return 0

    lax.fori_loop(0, slots // PICK, pick_dy, 0)
    for n in range(4):
        for k in range(2):
            to_sib(yp, yr, yd_s, yd_r, n, k).wait()
        yfar[n] = yp[n, cross] + yr[n, 1]
    for d in range(4):
        for j in range(8):
            at = rj[j, d].astype(jnp.int32)
            got = jnp.take_along_axis(dg_tab[...], jnp.maximum(at, 0), axis=1)
            dgp[d, j:j + 1, :] = jnp.sum(jnp.where(at >= 0, got, 0.0), axis=0, keepdims=True)
    y_cross = remote(yfar, ygot, yx_s, yx_r, cross)
    y_cross.start()
    dg_back = [remote(dgp.at[peer], dgr.at[k], dg_s.at[k], dg_r.at[k], peer) for k, peer in enumerate((cross, diag, sib))]

    def zero(n, like):
        return jnp.zeros((n, like.shape[1]), bf)

    def back_h(q, i):
        slot = lax.rem(i, AHEAD)
        g0, g1 = g_s[slot_rows(q * PAIR), :], g_s[slot_rows(q * PAIR + 1), :]
        both = dot(wo[slot, 0], jnp.concatenate([g0, zero(80, g0)], axis=0), ((1,), (1,)))
        both = both + dot(wo[slot, 1], jnp.concatenate([zero(64, g1), g1, zero(16, g1)], axis=0), ((1,), (1,)))
        dh = both.astype(bf).T.astype(f32)
        for p in range(PAIR):
            at = slot_rows(q * PAIR + p)
            da = (dh[64 * p:64 * p + SLOTS] * slope[at, :]).astype(bf)
            da_s[at, :] = da
            zs[lax.rem(i, 2), 64 * p:64 * p + SLOTS, 384 * p:384 * (p + 1)] = da

    def back_x(q, i):
        slot = lax.rem(i, AHEAD)
        wide = jnp.concatenate([wi[slot, 0], wi[slot, 1]], axis=1)
        both = dot(wide, zs[lax.rem(i, 2)], ((1,), (1,))).astype(bf).T
        for p in range(PAIR):
            sp[0, slot_rows(q * PAIR + p), :] = both[64 * p:64 * p + SLOTS]

    last = n_pairs - 1
    fetch_out(last, 0).wait()
    back_h(last, 0)
    fetch_out(last - AHEAD, 0).start()
    for copy in dg_back:
        copy.start()

    def bwd_step(i, _):
        fetch_in(last + 1 - i, lax.rem(i - 1, AHEAD)).wait()
        fetch_out(last - i, lax.rem(i, AHEAD)).wait()
        back_x(last + 1 - i, i - 1)
        back_h(last - i, i)

        @pl.when(i < n_pairs - AHEAD)
        def _():
            fetch_out(last - AHEAD - i, lax.rem(i, AHEAD)).start()

        @pl.when(i < n_pairs - AHEAD + 1)
        def _():
            fetch_in(last + 1 - AHEAD - i, lax.rem(i - 1, AHEAD)).start()
        return 0

    lax.fori_loop(1, n_pairs, bwd_step, 0)
    fetch_in(0, lax.rem(last, AHEAD)).wait()
    back_x(0, last)

    def dx_part(n, _):
        lanes = pl.ds(pl.multiple_of(n * 256, 256), 256)
        out = dot(pt[...], sp[0, :, lanes])
        for d in range(4):
            dxp[n, d] = out[128 * d:128 * (d + 1)]

        @pl.when(n > 0)
        def _():
            for k in range(2):
                to_sib(dxp, dxr, dd_s, dd_r, n - 1, k).start()
        return 0

    lax.fori_loop(0, 4, dx_part, 0)
    y_cross.wait()
    for k in range(2):
        to_sib(dxp, dxr, dd_s, dd_r, 3, k).start()
    for n in range(4):
        lanes = slice(256 * n, 256 * (n + 1))
        y_out[:, lanes] = (x[:, lanes].astype(f32) + (yp[n, me] + yr[n, 0] + ygot[n])).astype(bf)
    for copy in dg_back:
        copy.wait()
    dg_out[...] = dgp[me] + (dgr[0] + (dgr[1] + dgr[2]))
    for n in range(4):
        lanes = slice(256 * n, 256 * (n + 1))
        for k in range(2):
            to_sib(dxp, dxr, dd_s, dd_r, n, k).wait()
        dx_own[:, lanes] = dxp[n, me] + dxr[n, 0]
        dx_far[:, lanes] = dxp[n, cross] + dxr[n, 1]
    for copy in small + over + near + far:
        copy.wait_send()


def experts(x, dy, idx_t, gate_t, w_in, w_out):
    n_e, d_model, d_ff = w_in.shape
    slots = n_e * SLOTS
    bf, f32 = jnp.bfloat16, jnp.float32
    vmem, hbm = pl.BlockSpec(memory_space=pltpu.VMEM), pl.BlockSpec(memory_space=pl.ANY)
    buf, dma = pltpu.VMEM, pltpu.SemaphoreType.DMA
    return pl.pallas_call(
        expert_kernel,
        out_shape=[buf((128, d_model), bf), buf((8, 128), f32), buf((128, d_model), f32), buf((128, d_model), f32),
                   buf((slots, d_model), bf), buf((slots, d_ff), bf), buf((slots, d_model), bf), buf((slots, d_ff), bf)],
        in_specs=[hbm] * 6,
        out_specs=[vmem] * 8,
        scratch_shapes=[
            buf((128, d_model), bf), buf((128, d_model), bf), buf((8, 128), jnp.int32), buf((8, 128), f32),
            buf((4, 128, d_model), bf), buf((4, 128, d_model), bf), buf((4, 8, 128), jnp.int32), buf((4, 8, 128), f32),
            buf((8, 4, n_e, 128), f32), buf((4, n_e, 128), f32), buf((4, n_e, 128), f32),
            buf((slots, 512), bf), buf((512, slots), bf), buf((slots, 1), f32),
            buf((slots, d_model), bf), buf((slots, d_ff), f32), buf((3, slots, d_model), bf), buf((2, 128, PAIR * d_ff), bf),
            buf((n_e, 128), f32), buf((4, 8, 128), f32), buf((3, 8, 128), f32),
            buf((AHEAD, PAIR, d_model, d_ff), bf), buf((AHEAD, PAIR, d_ff, d_model), bf),
            buf((4, 4, 128, 256), f32), buf((4, 2, 128, 256), f32), buf((4, 128, 256), f32), buf((4, 128, 256), f32),
            buf((4, 4, 128, 256), f32), buf((4, 2, 128, 256), f32),
            dma((4,)), dma((AHEAD,)), dma((AHEAD,)), dma((6,)), dma((6,)), dma((2,)), dma((2,)), dma((4,)), dma((4,)),
            dma((4,)), dma((4,)), dma((4, 2)), dma((4, 2)), dma(()), dma(()), dma((4, 2)), dma((4, 2)), dma((3,)), dma((3,))],
        compiler_params=pltpu.CompilerParams(collective_id=0, has_side_effects=True, vmem_limit_bytes=53 * 1024 * 1024),
        cost_estimate=pl.CostEstimate(flops=8 * slots * d_model * d_ff, bytes_accessed=8 * n_e * d_model * d_ff, transcendentals=0),
    )(x, dy, idx_t, gate_t, w_in, w_out)


def weight_kernel(b, h, g, da, y, dg, dw_in, dw_out, y_out, dg_out, ring_in, ring_out, sem_in, sem_out, sem):
    n_steps = dw_in.shape[0] // PAIR
    passed = [pltpu.make_async_copy(y, y_out, sem.at[0]), pltpu.make_async_copy(dg, dg_out, sem.at[1])]
    for copy in passed:
        copy.start()

    def copies(i):
        slot = lax.rem(i, RING)
        return [pltpu.make_async_copy(ring.at[slot, p], out.at[i * PAIR + p], sems.at[slot, p])
                for p in range(PAIR) for ring, out, sems in ((ring_in, dw_in, sem_in), (ring_out, dw_out, sem_out))]

    def step(i, _):
        slot = lax.rem(i, RING)

        @pl.when(i >= RING)
        def _():
            for copy in copies(i - RING):
                copy.wait()

        for p in range(PAIR):
            at = slot_rows(i * PAIR + p)
            ring_in[slot, p] = dot(b[at, :], da[at, :], ((0,), (0,))).astype(jnp.bfloat16)
            ring_out[slot, p] = dot(h[at, :], g[at, :], ((0,), (0,))).astype(jnp.bfloat16)
        for copy in copies(i):
            copy.start()
        return 0

    lax.fori_loop(0, n_steps, step, 0)
    for i in range(n_steps - RING, n_steps):
        for copy in copies(i):
            copy.wait()
    for copy in passed:
        copy.wait()


def weight_grads(b, h, g, da, y, dg, n_e):
    d_model, d_ff = b.shape[1], h.shape[1]
    bf, shape, dma = jnp.bfloat16, jax.ShapeDtypeStruct, pltpu.SemaphoreType.DMA
    return pl.pallas_call(
        weight_kernel,
        out_shape=[shape((n_e, d_model, d_ff), bf), shape((n_e, d_ff, d_model), bf), shape(y.shape, y.dtype), shape(dg.shape, dg.dtype)],
        in_specs=[pl.BlockSpec(memory_space=pltpu.VMEM)] * 6,
        out_specs=[pl.BlockSpec(memory_space=pl.ANY)] * 4,
        scratch_shapes=[pltpu.VMEM((RING, PAIR, d_model, d_ff), bf), pltpu.VMEM((RING, PAIR, d_ff, d_model), bf),
                        dma((RING, PAIR)), dma((RING, PAIR)), dma((2,))],
        compiler_params=pltpu.CompilerParams(vmem_limit_bytes=40 * 1024 * 1024),
        cost_estimate=pl.CostEstimate(flops=4 * n_e * SLOTS * d_model * d_ff, bytes_accessed=4 * n_e * d_model * d_ff, transcendentals=0),
    )(b, h, g, da, y, dg)


def solution(mesh):
    tok_spec = P(('data', 'expert'), None)
    weight_spec = P('expert', None, None)
    grad_spec = P(('data', 'expert'), None, None)
    to_cross = [(i, i ^ 2) for i in range(4)]

    def device_pass(x_in, expert_idx, gate_weight, grad_y, w_in, w_out):
        y_mid, dg, dx_own, dx_far, b, h, g, da = experts(x_in, grad_y, expert_idx.T, gate_weight.T, w_in, w_out)
        dx_got = lax.ppermute(dx_far, 'expert', to_cross)
        grad_w_in, grad_w_out, y_out, dg = weight_grads(b, h, g, da, y_mid, dg, w_in.shape[0])
        grad_x = (grad_y.astype(jnp.float32) + (dx_own + dx_got)).astype(jnp.bfloat16)
        return y_out, grad_x, dg.T, grad_w_in, grad_w_out

    return jax.shard_map(device_pass, mesh=mesh,
                         in_specs=(tok_spec, tok_spec, tok_spec, tok_spec, weight_spec, weight_spec),
                         out_specs=(tok_spec, tok_spec, tok_spec, grad_spec, grad_spec), check_vma=False)
```

```python
import functools

import jax
import jax.numpy as jnp
from jax import lax
from jax.experimental import pallas as pl
from jax.experimental.pallas import tpu as pltpu
from jax.sharding import PartitionSpec as P

MESH = pl.DeviceIdType.MESH
CAP = 40
PAIR = 2
RING = 4
AHEAD = 4
PICK = 640
C0 = 0.7978845608028654
C1 = 0.044715


def dot(a, b, dims=((1,), (0,))):
    return lax.dot_general(a, b, (dims, ((), ())), preferred_element_type=jnp.float32)


def tables(ids_all, first, rj, r0s, r1s):
    eid = lax.broadcasted_iota(jnp.int32, (32, 128), 0) + first
    earlier = (lax.broadcasted_iota(jnp.int32, (128, 128), 0) < lax.broadcasted_iota(jnp.int32, (128, 128), 1)).astype(jnp.bfloat16)
    offset = jnp.zeros((32, 1), jnp.float32)
    for d in range(4):
        ids = ids_all[d]
        hits = [(ids[j:j + 1, :] == eid).astype(jnp.float32) for j in range(8)]
        count = sum(hits[1:], hits[0])
        rank = dot(count.astype(jnp.bfloat16), earlier) + offset
        r0s[d] = rank
        for j in range(8):
            rj[j, d] = jnp.where((hits[j] > 0.0) & (rank < CAP), rank, -1.0)
            rank = rank + hits[j]
        r1s[d] = jnp.minimum(rank, CAP)
        offset = offset + jnp.sum(count, axis=1, keepdims=True)


def pair_rows(q):
    return pl.ds(pl.multiple_of(q * PAIR * CAP, 16), PAIR * CAP)


def expert_kernel(x_hbm, dy_hbm, idx_hbm, gate_hbm, w_in, w_out, y_out, dg_out, dx_own, dx_far, b_s, h_s, g_s, da_s,
                  x, dy, idx, gate, xa, dya, ida, ga, rj, r0s, r1s, pm, pt, gs, o_s, slope, sp, dg_tab, dgp, dgr,
                  wi, wo, yp, yr, yfar, ygot, dxp, dxr,
                  arg_sem, wi_sem, wo_sem, small_s, small_r, sib_s, sib_r, cross_s, cross_r, fwd_s, fwd_r,
                  yd_s, yd_r, yx_s, yx_r, dd_s, dd_r, dg_s, dg_r):
    me = lax.axis_index("expert")
    sib, cross = me + 1 - 2 * lax.rem(me, 2), lax.rem(me + 2, 4)
    diag = lax.rem(sib + 2, 4)
    n_pairs = w_in.shape[0] // PAIR
    slots = 32 * CAP
    bf, f32 = jnp.bfloat16, jnp.float32
    d_ff = w_in.shape[2]

    def fetch_in(q, slot):
        return pltpu.make_async_copy(w_in.at[pl.ds(PAIR * q, PAIR)], wi.at[slot], wi_sem.at[slot])

    def fetch_out(q, slot):
        return pltpu.make_async_copy(w_out.at[pl.ds(PAIR * q, PAIR)], wo.at[slot], wo_sem.at[slot])

    def remote(src, dst, s, r, peer):
        return pltpu.make_async_remote_copy(src_ref=src, dst_ref=dst, send_sem=s, recv_sem=r,
                                            device_id={"expert": peer}, device_id_type=MESH)

    barrier = pltpu.get_barrier_semaphore()
    for peer in (sib, cross, diag):
        pl.semaphore_signal(barrier, inc=1, device_id={"expert": peer}, device_id_type=MESH)
    args = [pltpu.make_async_copy(src, dst, arg_sem.at[k])
            for k, (src, dst) in enumerate(((idx_hbm, idx), (gate_hbm, gate), (x_hbm, x), (dy_hbm, dy)))]
    for copy in args:
        copy.start()
    for q in range(AHEAD):
        fetch_in(q, q).start()
        fetch_out(q, q).start()
    for copy in args:
        copy.wait()
    pl.semaphore_wait(barrier, 3)

    small, over, near, far = [], [], [], []
    for k, peer in enumerate((cross, diag, sib)):
        small.append(remote(idx, ida.at[me], small_s.at[2 * k], small_r.at[2 * k], peer))
        small.append(remote(gate, ga.at[me], small_s.at[2 * k + 1], small_r.at[2 * k + 1], peer))
    for a, (src, dst) in enumerate(((x, xa), (dy, dya))):
        for c in range(2):
            rows = pl.ds(64 * c, 64)
            n = 2 * a + c
            over.append(remote(src.at[rows], dst.at[me, rows], cross_s.at[n], cross_r.at[n], cross))
            far.append(remote(dst.at[cross, rows], dst.at[cross, rows], fwd_s.at[n], fwd_r.at[n], sib))
        near.append(remote(src, dst.at[me], sib_s.at[a], sib_r.at[a], sib))
    for copy in small + over[:2] + near[:1] + over[2:] + near[1:]:
        copy.start()
    xa[me] = x[...]
    dya[me] = dy[...]
    ida[me] = idx[...]
    ga[me] = gate[...]

    def forward(n):
        over[n].wait_recv()
        far[n].start()

    for copy in small:
        copy.wait_recv()
    tables(ida, me * 32, rj, r0s, r1s)
    slot_id = lax.broadcasted_iota(jnp.int32, (CAP, 128), 0).astype(f32)

    def one(q, _):
        inside, total = [], [jnp.zeros((CAP, 128), f32) for _ in range(PAIR)]
        for d in range(4):
            for p in range(PAIR):
                e = pl.ds(q * PAIR + p, 1)
                inside.append(jnp.where((slot_id >= r0s[d, e, :]) & (slot_id < r1s[d, e, :]), 1.0, 0.0))
                for j in range(8):
                    total[p] = jnp.where(slot_id == rj[j, d, e, :], ga[d, j:j + 1, :], total[p])
            pm[pair_rows(q), 128 * d:128 * (d + 1)] = jnp.concatenate(inside[-PAIR:], axis=0).astype(bf)
        gs[pair_rows(q), :] = jnp.sum(jnp.concatenate(total, axis=0), axis=1, keepdims=True)
        return 0

    lax.fori_loop(0, n_pairs, one, 0)
    forward(0)
    forward(1)
    near[0].wait_recv()
    far[0].wait_recv()
    far[1].wait_recv()

    def pick_x(c, _):
        at = pl.ds(pl.multiple_of(c * PICK, PICK), PICK)
        b_s[at, :] = dot(pm[at, :], xa[...].reshape(512, xa.shape[2])).astype(bf)
        return 0

    lax.fori_loop(0, slots // PICK, pick_x, 0)

    first = lax.broadcasted_iota(jnp.int32, (PAIR * CAP, d_ff), 0) < CAP

    def fwd_step(i, _):
        slot = lax.rem(i, AHEAD)
        fetch_in(i, slot).wait()
        fetch_out(i, slot).wait()
        at = pair_rows(i)
        rows = b_s[at, :]
        a = jnp.concatenate([dot(rows, wi[slot, 0])[:CAP], dot(rows, wi[slot, 1])[CAP:]], axis=0)
        th = jnp.tanh(C0 * (a + C1 * (a * a * a)))
        cdf = 0.5 * (1.0 + th)
        slope[at, :] = cdf + 0.5 * a * (1.0 - th * th) * (C0 * (1.0 + 3.0 * C1 * (a * a)))
        h = a * cdf
        h = jnp.concatenate([jnp.where(first, h, 0.0), jnp.where(first, 0.0, h)], axis=1).astype(bf)
        h_s[at, :] = h
        o = dot(h, jnp.concatenate([wo[slot, 0], wo[slot, 1]], axis=0)).astype(bf)
        o_s[at, :] = o
        s = o.astype(f32) * gs[at, :]
        s1 = s.astype(bf)
        s = s - s1.astype(f32)
        s2 = s.astype(bf)
        s = s - s2.astype(f32)
        sp[0, at, :] = s1
        sp[1, at, :] = s2
        sp[2, at, :] = s.astype(bf)
        turned = i * (slots // 128) // n_pairs
        tile = pl.ds(pl.multiple_of(turned * 128, 128), 128)
        pt[:, tile] = pm[tile, :].astype(f32).T.astype(bf)

        @pl.when(i < n_pairs - AHEAD)
        def _():
            fetch_in(i + AHEAD, slot).start()
            fetch_out(i + AHEAD, slot).start()

        @pl.when(i >= n_pairs - AHEAD)
        def _():
            fetch_in(2 * n_pairs - 1 - AHEAD - i, slot).start()
            fetch_out(2 * n_pairs - 1 - AHEAD - i, slot).start()

        for n, when in ((2, 1), (3, 4)):
            @pl.when(i == when)
            def _(n=n):
                forward(n)
        return 0

    lax.fori_loop(0, n_pairs, fwd_step, 0)

    def to_sib(part, got, s, r, n, k):
        return remote(part.at[n, sib if k == 0 else diag], got.at[n, k], s.at[n, k], r.at[n, k], sib)

    def y_part(n, _):
        lanes = pl.ds(pl.multiple_of(n * 256, 256), 256)
        out = dot(pt[...], sp[0, :, lanes]) + dot(pt[...], sp[1, :, lanes]) + dot(pt[...], sp[2, :, lanes])
        for d in range(4):
            yp[n, d] = out[128 * d:128 * (d + 1)]

        @pl.when(n > 0)
        def _():
            for k in range(2):
                to_sib(yp, yr, yd_s, yd_r, n - 1, k).start()
        return 0

    lax.fori_loop(0, 4, y_part, 0)
    near[1].wait_recv()
    far[2].wait_recv()
    far[3].wait_recv()
    for k in range(2):
        to_sib(yp, yr, yd_s, yd_r, 3, k).start()

    def pick_dy(c, _):
        at = pl.ds(pl.multiple_of(c * PICK, PICK), PICK)
        rows = dot(pm[at, :], dya[...].reshape(512, dya.shape[2]))
        g_s[at, :] = (rows * gs[at, :]).astype(bf)
        prod = rows * o_s[at, :].astype(f32)
        part = sum((prod[:, 128 * k:128 * (k + 1)] for k in range(1, 8)), prod[:, :128])
        for k in range(PICK // CAP):
            dg_tab[pl.ds(c * (PICK // CAP) + k, 1), :CAP] = jnp.sum(part[CAP * k:CAP * (k + 1)].T, axis=0, keepdims=True)
        return 0

    lax.fori_loop(0, slots // PICK, pick_dy, 0)
    for n in range(4):
        for k in range(2):
            to_sib(yp, yr, yd_s, yd_r, n, k).wait()
        yfar[n] = yp[n, cross] + yr[n, 1]
    for d in range(4):
        for j in range(8):
            at = rj[j, d].astype(jnp.int32)
            got = jnp.take_along_axis(dg_tab[...], jnp.maximum(at, 0), axis=1)
            dgp[d, j:j + 1, :] = jnp.sum(jnp.where(at >= 0, got, 0.0), axis=0, keepdims=True)
    y_cross = remote(yfar, ygot, yx_s, yx_r, cross)
    y_cross.start()
    dg_back = [remote(dgp.at[peer], dgr.at[k], dg_s.at[k], dg_r.at[k], peer) for k, peer in enumerate((cross, diag, sib))]

    mine = lax.broadcasted_iota(jnp.int32, (d_ff, PAIR * CAP), 1) < CAP
    last = n_pairs - 1

    def back_h(i):
        slot, at = lax.rem(i, AHEAD), pair_rows(last - i)
        g = g_s[at, :]
        dh = jnp.where(mine, dot(wo[slot, 0], g, ((1,), (1,))), dot(wo[slot, 1], g, ((1,), (1,))))
        da = dh.astype(bf).T.astype(f32) * slope[at, :]
        da_s[at, :] = jnp.concatenate([jnp.where(first, da, 0.0), jnp.where(first, 0.0, da)], axis=1).astype(bf)

    def back_x(i):
        slot, at = lax.rem(i, AHEAD), pair_rows(last - i)
        wide = jnp.concatenate([wi[slot, 0], wi[slot, 1]], axis=1)
        sp[0, at, :] = dot(wide, da_s[at, :], ((1,), (1,))).astype(bf).T

    def wait_in(i):
        fetch_in(last - i, lax.rem(i, AHEAD)).wait()

    def wait_out(i):
        fetch_out(last - i, lax.rem(i, AHEAD)).wait()

    wait_out(0)
    wait_out(1)
    back_h(0)
    back_h(1)
    for copy in dg_back:
        copy.start()
    for i in range(2):
        fetch_out(last - AHEAD - i, i).start()

    def bwd_step(j, _):
        i = 2 * j
        for k in range(2):
            wait_in(i - 2 + k)
            wait_out(i + k)
        back_x(i - 2)
        back_x(i - 1)
        back_h(i)
        back_h(i + 1)

        @pl.when(i < n_pairs - AHEAD)
        def _():
            for k in range(2):
                fetch_out(last - AHEAD - i - k, lax.rem(i + k, AHEAD)).start()

        @pl.when(i < n_pairs - AHEAD + 2)
        def _():
            for k in range(2):
                fetch_in(last + 2 - AHEAD - i - k, lax.rem(i - 2 + k, AHEAD)).start()
        return 0

    lax.fori_loop(1, n_pairs // 2, bwd_step, 0)
    y_cross.wait()
    for copy in dg_back:
        copy.wait()
    for i in range(last - 1, last + 1):
        wait_in(i)
    dg_out[...] = dgp[me] + (dgr[0] + (dgr[1] + dgr[2]))
    for n in range(4):
        lanes = slice(256 * n, 256 * (n + 1))
        y_out[:, lanes] = (x[:, lanes].astype(f32) + (yp[n, me] + yr[n, 0] + ygot[n])).astype(bf)
    back_x(last - 1)
    back_x(last)

    def dx_part(n, _):
        lanes = pl.ds(pl.multiple_of(n * 256, 256), 256)
        out = dot(pt[...], sp[0, :, lanes])
        for d in range(4):
            dxp[n, d] = out[128 * d:128 * (d + 1)]

        @pl.when(n > 0)
        def _():
            for k in range(2):
                to_sib(dxp, dxr, dd_s, dd_r, n - 1, k).start()
        return 0

    lax.fori_loop(0, 4, dx_part, 0)
    for k in range(2):
        to_sib(dxp, dxr, dd_s, dd_r, 3, k).start()
    for n in range(4):
        lanes = slice(256 * n, 256 * (n + 1))
        for k in range(2):
            to_sib(dxp, dxr, dd_s, dd_r, n, k).wait()
        dx_own[:, lanes] = dxp[n, me] + dxr[n, 0]
        dx_far[:, lanes] = dxp[n, cross] + dxr[n, 1]
    for copy in small + over + near + far:
        copy.wait_send()


def experts(x, dy, idx_t, gate_t, w_in, w_out):
    n_e, d_model, d_ff = w_in.shape
    slots = n_e * CAP
    bf, f32 = jnp.bfloat16, jnp.float32
    vmem, hbm = pl.BlockSpec(memory_space=pltpu.VMEM), pl.BlockSpec(memory_space=pl.ANY)
    buf, dma = pltpu.VMEM, pltpu.SemaphoreType.DMA
    return pl.pallas_call(
        expert_kernel,
        out_shape=[buf((128, d_model), bf), buf((8, 128), f32), buf((128, d_model), f32), buf((128, d_model), f32),
                   buf((slots, d_model), bf), buf((slots, PAIR * d_ff), bf), buf((slots, d_model), bf), buf((slots, PAIR * d_ff), bf)],
        in_specs=[hbm] * 6,
        out_specs=[vmem] * 8,
        scratch_shapes=[
            buf((128, d_model), bf), buf((128, d_model), bf), buf((8, 128), jnp.int32), buf((8, 128), f32),
            buf((4, 128, d_model), bf), buf((4, 128, d_model), bf), buf((4, 8, 128), jnp.int32), buf((4, 8, 128), f32),
            buf((8, 4, n_e, 128), f32), buf((4, n_e, 128), f32), buf((4, n_e, 128), f32),
            buf((slots, 512), bf), buf((512, slots), bf), buf((slots, 1), f32),
            buf((slots, d_model), bf), buf((slots, d_ff), f32), buf((3, slots, d_model), bf),
            buf((n_e, 128), f32), buf((4, 8, 128), f32), buf((3, 8, 128), f32),
            buf((AHEAD, PAIR, d_model, d_ff), bf), buf((AHEAD, PAIR, d_ff, d_model), bf),
            buf((4, 4, 128, 256), f32), buf((4, 2, 128, 256), f32), buf((4, 128, 256), f32), buf((4, 128, 256), f32),
            buf((4, 4, 128, 256), f32), buf((4, 2, 128, 256), f32),
            dma((4,)), dma((AHEAD,)), dma((AHEAD,)), dma((6,)), dma((6,)), dma((2,)), dma((2,)), dma((4,)), dma((4,)),
            dma((4,)), dma((4,)), dma((4, 2)), dma((4, 2)), dma(()), dma(()), dma((4, 2)), dma((4, 2)), dma((3,)), dma((3,))],
        compiler_params=pltpu.CompilerParams(collective_id=0, has_side_effects=True, vmem_limit_bytes=53 * 1024 * 1024),
        cost_estimate=pl.CostEstimate(flops=8 * slots * d_model * d_ff, bytes_accessed=8 * n_e * d_model * d_ff, transcendentals=0),
    )(x, dy, idx_t, gate_t, w_in, w_out)


def weight_kernel(b, h, g, da, y, dg, dw_in, dw_out, y_out, dg_out, ring_in, ring_out, sem_in, sem_out, sem):
    n_steps, d_ff = dw_in.shape[0] // PAIR, dw_in.shape[2]
    passed = [pltpu.make_async_copy(y, y_out, sem.at[0]), pltpu.make_async_copy(dg, dg_out, sem.at[1])]
    for copy in passed:
        copy.start()

    def copies(i):
        slot = lax.rem(i, RING)
        return [pltpu.make_async_copy(ring.at[slot, p], out.at[i * PAIR + p], sems.at[slot, p])
                for p in range(PAIR) for ring, out, sems in ((ring_in, dw_in, sem_in), (ring_out, dw_out, sem_out))]

    def step(i, _):
        slot = lax.rem(i, RING)

        @pl.when(i >= RING)
        def _():
            for copy in copies(i - RING):
                copy.wait()

        at = pair_rows(i)
        for p in range(PAIR):
            own = slice(d_ff * p, d_ff * (p + 1))
            ring_in[slot, p] = dot(b[at, :], da[at, own], ((0,), (0,))).astype(jnp.bfloat16)
            ring_out[slot, p] = dot(h[at, own], g[at, :], ((0,), (0,))).astype(jnp.bfloat16)
        for copy in copies(i):
            copy.start()
        return 0

    lax.fori_loop(0, n_steps, step, 0)
    for i in range(n_steps - RING, n_steps):
        for copy in copies(i):
            copy.wait()
    for copy in passed:
        copy.wait()


def weight_grads(b, h, g, da, y, dg, n_e):
    d_model, d_ff = b.shape[1], h.shape[1] // PAIR
    bf, shape, dma = jnp.bfloat16, jax.ShapeDtypeStruct, pltpu.SemaphoreType.DMA
    return pl.pallas_call(
        weight_kernel,
        out_shape=[shape((n_e, d_model, d_ff), bf), shape((n_e, d_ff, d_model), bf), shape(y.shape, y.dtype), shape(dg.shape, dg.dtype)],
        in_specs=[pl.BlockSpec(memory_space=pltpu.VMEM)] * 6,
        out_specs=[pl.BlockSpec(memory_space=pl.ANY)] * 4,
        scratch_shapes=[pltpu.VMEM((RING, PAIR, d_model, d_ff), bf), pltpu.VMEM((RING, PAIR, d_ff, d_model), bf),
                        dma((RING, PAIR)), dma((RING, PAIR)), dma((2,))],
        compiler_params=pltpu.CompilerParams(vmem_limit_bytes=40 * 1024 * 1024),
        cost_estimate=pl.CostEstimate(flops=4 * n_e * CAP * d_model * d_ff, bytes_accessed=4 * n_e * d_model * d_ff, transcendentals=0),
    )(b, h, g, da, y, dg)


def solution(mesh):
    tok_spec = P(('data', 'expert'), None)
    weight_spec = P('expert', None, None)
    grad_spec = P(('data', 'expert'), None, None)
    to_cross = [(i, i ^ 2) for i in range(4)]

    def device_pass(x_in, expert_idx, gate_weight, grad_y, w_in, w_out):
        y_mid, dg, dx_own, dx_far, b, h, g, da = experts(x_in, grad_y, expert_idx.T, gate_weight.T, w_in, w_out)
        dx_got = lax.ppermute(dx_far, 'expert', to_cross)
        grad_w_in, grad_w_out, y_out, dg = weight_grads(b, h, g, da, y_mid, dg, w_in.shape[0])
        grad_x = (grad_y.astype(jnp.float32) + (dx_own + dx_got)).astype(jnp.bfloat16)
        return y_out, grad_x, dg.T, grad_w_in, grad_w_out

    return jax.shard_map(device_pass, mesh=mesh,
                         in_specs=(tok_spec, tok_spec, tok_spec, tok_spec, weight_spec, weight_spec),
                         out_specs=(tok_spec, tok_spec, tok_spec, grad_spec, grad_spec), check_vma=False)
```

```python
import functools

import jax
import jax.numpy as jnp
from jax import lax
from jax.experimental import pallas as pl
from jax.experimental.pallas import tpu as pltpu
from jax.sharding import PartitionSpec as P

MESH = pl.DeviceIdType.MESH
CAP = 40
PAIR = 2
RING = 4
AHEAD = 8
PICK = 640
C0 = 0.7978845608028654
C1 = 0.044715


def dot(a, b, dims=((1,), (0,))):
    return lax.dot_general(a, b, (dims, ((), ())), preferred_element_type=jnp.float32)


def tables(ids_all, first, rj, r0s, r1s):
    eid = lax.broadcasted_iota(jnp.int32, (32, 128), 0) + first
    earlier = (lax.broadcasted_iota(jnp.int32, (128, 128), 0) < lax.broadcasted_iota(jnp.int32, (128, 128), 1)).astype(jnp.bfloat16)
    offset = jnp.zeros((32, 1), jnp.float32)
    for d in range(4):
        ids = ids_all[d]
        hits = [(ids[j:j + 1, :] == eid).astype(jnp.float32) for j in range(8)]
        count = sum(hits[1:], hits[0])
        rank = dot(count.astype(jnp.bfloat16), earlier) + offset
        r0s[d] = rank
        for j in range(8):
            rj[j, d] = jnp.where((hits[j] > 0.0) & (rank < CAP), rank, -1.0)
            rank = rank + hits[j]
        r1s[d] = jnp.minimum(rank, CAP)
        offset = offset + jnp.sum(count, axis=1, keepdims=True)


def pair_rows(q):
    return pl.ds(pl.multiple_of(q * PAIR * CAP, 16), PAIR * CAP)


def expert_kernel(x_hbm, dy_hbm, idx_hbm, gate_hbm, w_in, w_out, y_out, dg_out, dx_own, dx_far, b_s, h_s, g_s, da_s,
                  x, dy, idx, gate, xa, dya, ida, ga, rj, r0s, r1s, pm, pt, gs, o_s, slope, sp, dg_tab, dgp, dgr,
                  wi, wo, yp, yr, yfar, ygot, dxp, dxr,
                  arg_sem, wi_sem, wo_sem, small_s, small_r, sib_s, sib_r, cross_s, cross_r, fwd_s, fwd_r,
                  yd_s, yd_r, yx_s, yx_r, dd_s, dd_r, dg_s, dg_r):
    me = lax.axis_index("expert")
    sib, cross = me + 1 - 2 * lax.rem(me, 2), lax.rem(me + 2, 4)
    diag = lax.rem(sib + 2, 4)
    n_pairs = w_in.shape[0] // PAIR
    slots = 32 * CAP
    bf, f32 = jnp.bfloat16, jnp.float32
    d_ff = w_in.shape[2]

    def fetch_in(q):
        slot = lax.rem(q, AHEAD)
        return pltpu.make_async_copy(w_in.at[pl.ds(PAIR * q, PAIR)], wi.at[slot], wi_sem.at[slot])

    def fetch_out(q):
        slot = lax.rem(q, AHEAD)
        return pltpu.make_async_copy(w_out.at[pl.ds(PAIR * q, PAIR)], wo.at[slot], wo_sem.at[slot])

    def remote(src, dst, s, r, peer):
        return pltpu.make_async_remote_copy(src_ref=src, dst_ref=dst, send_sem=s, recv_sem=r,
                                            device_id={"expert": peer}, device_id_type=MESH)

    barrier = pltpu.get_barrier_semaphore()
    for peer in (sib, cross, diag):
        pl.semaphore_signal(barrier, inc=1, device_id={"expert": peer}, device_id_type=MESH)
    args = [pltpu.make_async_copy(src, dst, arg_sem.at[k])
            for k, (src, dst) in enumerate(((idx_hbm, idx), (gate_hbm, gate), (x_hbm, x), (dy_hbm, dy)))]
    for copy in args:
        copy.start()
    for q in range(AHEAD):
        fetch_in(q).start()
        fetch_out(q).start()
    for copy in args:
        copy.wait()
    pl.semaphore_wait(barrier, 3)

    small, over, near, far = [], [], [], []
    for k, peer in enumerate((cross, diag, sib)):
        small.append(remote(idx, ida.at[me], small_s.at[2 * k], small_r.at[2 * k], peer))
        small.append(remote(gate, ga.at[me], small_s.at[2 * k + 1], small_r.at[2 * k + 1], peer))
    for a, (src, dst) in enumerate(((x, xa), (dy, dya))):
        for c in range(2):
            rows = pl.ds(64 * c, 64)
            n = 2 * a + c
            over.append(remote(src.at[rows], dst.at[me, rows], cross_s.at[n], cross_r.at[n], cross))
            far.append(remote(dst.at[cross, rows], dst.at[cross, rows], fwd_s.at[n], fwd_r.at[n], sib))
        near.append(remote(src, dst.at[me], sib_s.at[a], sib_r.at[a], sib))
    for copy in small + over[:2] + near[:1] + over[2:] + near[1:]:
        copy.start()
    xa[me] = x[...]
    dya[me] = dy[...]
    ida[me] = idx[...]
    ga[me] = gate[...]

    def forward(n):
        over[n].wait_recv()
        far[n].start()

    for copy in small:
        copy.wait_recv()
    tables(ida, me * 32, rj, r0s, r1s)
    slot_id = lax.broadcasted_iota(jnp.int32, (CAP, 128), 0).astype(f32)

    def one(q, _):
        inside, total = [], [jnp.zeros((CAP, 128), f32) for _ in range(PAIR)]
        for d in range(4):
            for p in range(PAIR):
                e = pl.ds(q * PAIR + p, 1)
                inside.append(jnp.where((slot_id >= r0s[d, e, :]) & (slot_id < r1s[d, e, :]), 1.0, 0.0))
                for j in range(8):
                    total[p] = jnp.where(slot_id == rj[j, d, e, :], ga[d, j:j + 1, :], total[p])
            pm[pair_rows(q), 128 * d:128 * (d + 1)] = jnp.concatenate(inside[-PAIR:], axis=0).astype(bf)
        gs[pair_rows(q), :] = jnp.sum(jnp.concatenate(total, axis=0), axis=1, keepdims=True)
        return 0

    lax.fori_loop(0, n_pairs, one, 0)
    forward(0)
    forward(1)
    near[0].wait_recv()
    far[0].wait_recv()
    far[1].wait_recv()

    def pick_x(c, _):
        at = pl.ds(pl.multiple_of(c * PICK, PICK), PICK)
        b_s[at, :] = dot(pm[at, :], xa[...].reshape(512, xa.shape[2])).astype(bf)
        return 0

    lax.fori_loop(0, slots // PICK, pick_x, 0)

    first = lax.broadcasted_iota(jnp.int32, (PAIR * CAP, d_ff), 0) < CAP

    def fwd_step(i, _):
        slot = lax.rem(i, AHEAD)
        fetch_in(i).wait()
        fetch_out(i).wait()
        at = pair_rows(i)
        rows = b_s[at, :]
        a = jnp.concatenate([dot(rows, wi[slot, 0])[:CAP], dot(rows, wi[slot, 1])[CAP:]], axis=0)
        th = jnp.tanh(C0 * (a + C1 * (a * a * a)))
        cdf = 0.5 * (1.0 + th)
        slope[at, :] = cdf + 0.5 * a * (1.0 - th * th) * (C0 * (1.0 + 3.0 * C1 * (a * a)))
        h = a * cdf
        h = jnp.concatenate([jnp.where(first, h, 0.0), jnp.where(first, 0.0, h)], axis=1).astype(bf)
        h_s[at, :] = h
        o = dot(h, jnp.concatenate([wo[slot, 0], wo[slot, 1]], axis=0)).astype(bf)
        o_s[at, :] = o
        s = o.astype(f32) * gs[at, :]
        s1 = s.astype(bf)
        s = s - s1.astype(f32)
        s2 = s.astype(bf)
        s = s - s2.astype(f32)
        sp[0, at, :] = s1
        sp[1, at, :] = s2
        sp[2, at, :] = s.astype(bf)
        turned = i * (slots // 128) // n_pairs
        tile = pl.ds(pl.multiple_of(turned * 128, 128), 128)
        pt[:, tile] = pm[tile, :].astype(f32).T.astype(bf)

        @pl.when(i < n_pairs - AHEAD)
        def _():
            fetch_in(i + AHEAD).start()
            fetch_out(i + AHEAD).start()

        for n, when in ((2, 1), (3, 4)):
            @pl.when(i == when)
            def _(n=n):
                forward(n)
        return 0

    lax.fori_loop(0, n_pairs, fwd_step, 0)

    def to_sib(part, got, s, r, n, k):
        return remote(part.at[n, sib if k == 0 else diag], got.at[n, k], s.at[n, k], r.at[n, k], sib)

    def y_part(n, _):
        lanes = pl.ds(pl.multiple_of(n * 256, 256), 256)
        out = dot(pt[...], sp[0, :, lanes]) + dot(pt[...], sp[1, :, lanes]) + dot(pt[...], sp[2, :, lanes])
        for d in range(4):
            yp[n, d] = out[128 * d:128 * (d + 1)]

        @pl.when(n > 0)
        def _():
            for k in range(2):
                to_sib(yp, yr, yd_s, yd_r, n - 1, k).start()
        return 0

    lax.fori_loop(0, 4, y_part, 0)
    near[1].wait_recv()
    far[2].wait_recv()
    far[3].wait_recv()
    for k in range(2):
        to_sib(yp, yr, yd_s, yd_r, 3, k).start()

    def pick_dy(c, _):
        at = pl.ds(pl.multiple_of(c * PICK, PICK), PICK)
        rows = dot(pm[at, :], dya[...].reshape(512, dya.shape[2]))
        g_s[at, :] = (rows * gs[at, :]).astype(bf)
        prod = rows * o_s[at, :].astype(f32)
        part = sum((prod[:, 128 * k:128 * (k + 1)] for k in range(1, 8)), prod[:, :128])
        for k in range(PICK // CAP):
            dg_tab[pl.ds(c * (PICK // CAP) + k, 1), :CAP] = jnp.sum(part[CAP * k:CAP * (k + 1)].T, axis=0, keepdims=True)
        return 0

    lax.fori_loop(0, slots // PICK, pick_dy, 0)
    for n in range(4):
        for k in range(2):
            to_sib(yp, yr, yd_s, yd_r, n, k).wait()
        yfar[n] = yp[n, cross] + yr[n, 1]
    for d in range(4):
        for j in range(8):
            at = rj[j, d].astype(jnp.int32)
            got = jnp.take_along_axis(dg_tab[...], jnp.maximum(at, 0), axis=1)
            dgp[d, j:j + 1, :] = jnp.sum(jnp.where(at >= 0, got, 0.0), axis=0, keepdims=True)
    y_cross = remote(yfar, ygot, yx_s, yx_r, cross)
    y_cross.start()
    dg_back = [remote(dgp.at[peer], dgr.at[k], dg_s.at[k], dg_r.at[k], peer) for k, peer in enumerate((cross, diag, sib))]

    mine = lax.broadcasted_iota(jnp.int32, (d_ff, PAIR * CAP), 1) < CAP
    last = n_pairs - 1

    def back_h(i):
        slot, at = lax.rem(last - i, AHEAD), pair_rows(last - i)
        g = g_s[at, :]
        dh = jnp.where(mine, dot(wo[slot, 0], g, ((1,), (1,))), dot(wo[slot, 1], g, ((1,), (1,))))
        da = dh.astype(bf).T.astype(f32) * slope[at, :]
        da_s[at, :] = jnp.concatenate([jnp.where(first, da, 0.0), jnp.where(first, 0.0, da)], axis=1).astype(bf)

    def back_x(i):
        slot, at = lax.rem(last - i, AHEAD), pair_rows(last - i)
        wide = jnp.concatenate([wi[slot, 0], wi[slot, 1]], axis=1)
        sp[0, at, :] = dot(wide, da_s[at, :], ((1,), (1,))).astype(bf).T

    back_h(0)
    back_h(1)
    for copy in dg_back:
        copy.start()
    for i in range(2):
        fetch_out(last - AHEAD - i).start()

    def bwd_step(j, _):
        i = 2 * j

        @pl.when(i - 2 >= n_pairs - AHEAD)
        def _():
            for k in range(2):
                fetch_in(last + 2 - i - k).wait()

        @pl.when(i >= n_pairs - AHEAD)
        def _():
            for k in range(2):
                fetch_out(last - i - k).wait()

        back_x(i - 2)
        back_x(i - 1)
        back_h(i)
        back_h(i + 1)

        @pl.when(i < n_pairs - AHEAD)
        def _():
            for k in range(2):
                fetch_out(last - AHEAD - i - k).start()

        @pl.when(i < n_pairs - AHEAD + 2)
        def _():
            for k in range(2):
                fetch_in(last + 2 - AHEAD - i - k).start()
        return 0

    lax.fori_loop(1, n_pairs // 2, bwd_step, 0)
    y_cross.wait()
    for copy in dg_back:
        copy.wait()
    for i in range(2):
        fetch_in(i).wait()
    dg_out[...] = dgp[me] + (dgr[0] + (dgr[1] + dgr[2]))
    for n in range(4):
        lanes = slice(256 * n, 256 * (n + 1))
        y_out[:, lanes] = (x[:, lanes].astype(f32) + (yp[n, me] + yr[n, 0] + ygot[n])).astype(bf)
    back_x(last - 1)
    back_x(last)

    def dx_part(n, _):
        lanes = pl.ds(pl.multiple_of(n * 256, 256), 256)
        out = dot(pt[...], sp[0, :, lanes])
        for d in range(4):
            dxp[n, d] = out[128 * d:128 * (d + 1)]

        @pl.when(n > 0)
        def _():
            for k in range(2):
                to_sib(dxp, dxr, dd_s, dd_r, n - 1, k).start()
        return 0

    lax.fori_loop(0, 4, dx_part, 0)
    for k in range(2):
        to_sib(dxp, dxr, dd_s, dd_r, 3, k).start()
    for n in range(4):
        lanes = slice(256 * n, 256 * (n + 1))
        for k in range(2):
            to_sib(dxp, dxr, dd_s, dd_r, n, k).wait()
        dx_own[:, lanes] = dxp[n, me] + dxr[n, 0]
        dx_far[:, lanes] = dxp[n, cross] + dxr[n, 1]
    for copy in small + over + near + far:
        copy.wait_send()


def experts(x, dy, idx_t, gate_t, w_in, w_out):
    n_e, d_model, d_ff = w_in.shape
    slots = n_e * CAP
    bf, f32 = jnp.bfloat16, jnp.float32
    vmem, hbm = pl.BlockSpec(memory_space=pltpu.VMEM), pl.BlockSpec(memory_space=pl.ANY)
    buf, dma = pltpu.VMEM, pltpu.SemaphoreType.DMA
    return pl.pallas_call(
        expert_kernel,
        out_shape=[buf((128, d_model), bf), buf((8, 128), f32), buf((128, d_model), f32), buf((128, d_model), f32),
                   buf((slots, d_model), bf), buf((slots, PAIR * d_ff), bf), buf((slots, d_model), bf), buf((slots, PAIR * d_ff), bf)],
        in_specs=[hbm] * 6,
        out_specs=[vmem] * 8,
        scratch_shapes=[
            buf((128, d_model), bf), buf((128, d_model), bf), buf((8, 128), jnp.int32), buf((8, 128), f32),
            buf((4, 128, d_model), bf), buf((4, 128, d_model), bf), buf((4, 8, 128), jnp.int32), buf((4, 8, 128), f32),
            buf((8, 4, n_e, 128), f32), buf((4, n_e, 128), f32), buf((4, n_e, 128), f32),
            buf((slots, 512), bf), buf((512, slots), bf), buf((slots, 1), f32),
            buf((slots, d_model), bf), buf((slots, d_ff), f32), buf((3, slots, d_model), bf),
            buf((n_e, 128), f32), buf((4, 8, 128), f32), buf((3, 8, 128), f32),
            buf((AHEAD, PAIR, d_model, d_ff), bf), buf((AHEAD, PAIR, d_ff, d_model), bf),
            buf((4, 4, 128, 256), f32), buf((4, 2, 128, 256), f32), buf((4, 128, 256), f32), buf((4, 128, 256), f32),
            buf((4, 4, 128, 256), f32), buf((4, 2, 128, 256), f32),
            dma((4,)), dma((AHEAD,)), dma((AHEAD,)), dma((6,)), dma((6,)), dma((2,)), dma((2,)), dma((4,)), dma((4,)),
            dma((4,)), dma((4,)), dma((4, 2)), dma((4, 2)), dma(()), dma(()), dma((4, 2)), dma((4, 2)), dma((3,)), dma((3,))],
        compiler_params=pltpu.CompilerParams(collective_id=0, has_side_effects=True, vmem_limit_bytes=53 * 1024 * 1024),
        cost_estimate=pl.CostEstimate(flops=8 * slots * d_model * d_ff, bytes_accessed=8 * n_e * d_model * d_ff, transcendentals=0),
    )(x, dy, idx_t, gate_t, w_in, w_out)


def weight_kernel(b, h, g, da, y, dg, dw_in, dw_out, y_out, dg_out, ring_in, ring_out, sem_in, sem_out, sem):
    n_steps, d_ff = dw_in.shape[0] // PAIR, dw_in.shape[2]
    passed = [pltpu.make_async_copy(y, y_out, sem.at[0]), pltpu.make_async_copy(dg, dg_out, sem.at[1])]
    for copy in passed:
        copy.start()

    def copies(i):
        slot = lax.rem(i, RING)
        return [pltpu.make_async_copy(ring.at[slot, p], out.at[i * PAIR + p], sems.at[slot, p])
                for p in range(PAIR) for ring, out, sems in ((ring_in, dw_in, sem_in), (ring_out, dw_out, sem_out))]

    def step(i, _):
        slot = lax.rem(i, RING)

        @pl.when(i >= RING)
        def _():
            for copy in copies(i - RING):
                copy.wait()

        at = pair_rows(i)
        for p in range(PAIR):
            own = slice(d_ff * p, d_ff * (p + 1))
            ring_in[slot, p] = dot(b[at, :], da[at, own], ((0,), (0,))).astype(jnp.bfloat16)
            ring_out[slot, p] = dot(h[at, own], g[at, :], ((0,), (0,))).astype(jnp.bfloat16)
        for copy in copies(i):
            copy.start()
        return 0

    lax.fori_loop(0, n_steps, step, 0)
    for i in range(n_steps - RING, n_steps):
        for copy in copies(i):
            copy.wait()
    for copy in passed:
        copy.wait()


def weight_grads(b, h, g, da, y, dg, n_e):
    d_model, d_ff = b.shape[1], h.shape[1] // PAIR
    bf, shape, dma = jnp.bfloat16, jax.ShapeDtypeStruct, pltpu.SemaphoreType.DMA
    return pl.pallas_call(
        weight_kernel,
        out_shape=[shape((n_e, d_model, d_ff), bf), shape((n_e, d_ff, d_model), bf), shape(y.shape, y.dtype), shape(dg.shape, dg.dtype)],
        in_specs=[pl.BlockSpec(memory_space=pltpu.VMEM)] * 6,
        out_specs=[pl.BlockSpec(memory_space=pl.ANY)] * 4,
        scratch_shapes=[pltpu.VMEM((RING, PAIR, d_model, d_ff), bf), pltpu.VMEM((RING, PAIR, d_ff, d_model), bf),
                        dma((RING, PAIR)), dma((RING, PAIR)), dma((2,))],
        compiler_params=pltpu.CompilerParams(vmem_limit_bytes=40 * 1024 * 1024),
        cost_estimate=pl.CostEstimate(flops=4 * n_e * CAP * d_model * d_ff, bytes_accessed=4 * n_e * d_model * d_ff, transcendentals=0),
    )(b, h, g, da, y, dg)


def solution(mesh):
    tok_spec = P(('data', 'expert'), None)
    weight_spec = P('expert', None, None)
    grad_spec = P(('data', 'expert'), None, None)
    to_cross = [(i, i ^ 2) for i in range(4)]

    def device_pass(x_in, expert_idx, gate_weight, grad_y, w_in, w_out):
        y_mid, dg, dx_own, dx_far, b, h, g, da = experts(x_in, grad_y, expert_idx.T, gate_weight.T, w_in, w_out)
        dx_got = lax.ppermute(dx_far, 'expert', to_cross)
        grad_w_in, grad_w_out, y_out, dg = weight_grads(b, h, g, da, y_mid, dg, w_in.shape[0])
        grad_x = (grad_y.astype(jnp.float32) + (dx_own + dx_got)).astype(jnp.bfloat16)
        return y_out, grad_x, dg.T, grad_w_in, grad_w_out

    return jax.shard_map(device_pass, mesh=mesh,
                         in_specs=(tok_spec, tok_spec, tok_spec, tok_spec, weight_spec, weight_spec),
                         out_specs=(tok_spec, tok_spec, tok_spec, grad_spec, grad_spec), check_vma=False)
```

```python
import functools

import jax
import jax.numpy as jnp
from jax import lax
from jax.experimental import pallas as pl
from jax.experimental.pallas import tpu as pltpu
from jax.sharding import PartitionSpec as P

MESH = pl.DeviceIdType.MESH
CAP = 40
PAIR = 2
RING = 4
AHEAD = 8
PICK = 640
C0 = 0.7978845608028654
C1 = 0.044715


def dot(a, b, dims=((1,), (0,))):
    return lax.dot_general(a, b, (dims, ((), ())), preferred_element_type=jnp.float32)


def tables(ids_all, first, rj, r0s, r1s):
    eid = lax.broadcasted_iota(jnp.int32, (32, 128), 0) + first
    earlier = (lax.broadcasted_iota(jnp.int32, (128, 128), 0) < lax.broadcasted_iota(jnp.int32, (128, 128), 1)).astype(jnp.bfloat16)
    offset = jnp.zeros((32, 1), jnp.float32)
    for d in range(4):
        ids = ids_all[d]
        hits = [(ids[j:j + 1, :] == eid).astype(jnp.float32) for j in range(8)]
        count = sum(hits[1:], hits[0])
        rank = dot(count.astype(jnp.bfloat16), earlier) + offset
        r0s[d] = rank
        for j in range(8):
            rj[j, d] = jnp.where((hits[j] > 0.0) & (rank < CAP), rank, -1.0)
            rank = rank + hits[j]
        r1s[d] = jnp.minimum(rank, CAP)
        offset = offset + jnp.sum(count, axis=1, keepdims=True)


def pair_rows(q):
    return pl.ds(pl.multiple_of(q * PAIR * CAP, 16), PAIR * CAP)


def expert_kernel(x_hbm, dy_hbm, idx_hbm, gate_hbm, w_in, w_out, y_out, dg_out, dx_own, dx_far, b_s, h_s, g_s, da_s,
                  x, dy, idx, gate, xa, dya, ida, ga, rj, r0s, r1s, pm, pt, gs, o_s, slope, sp, dg_tab, dgp, dgr,
                  wi, wo, yp, yr, yfar, ygot, dxp, dxr,
                  arg_sem, wi_sem, wo_sem, small_s, small_r, sib_s, sib_r, cross_s, cross_r, fwd_s, fwd_r,
                  yd_s, yd_r, yx_s, yx_r, dd_s, dd_r, dg_s, dg_r):
    me = lax.axis_index("expert")
    sib, cross = me + 1 - 2 * lax.rem(me, 2), lax.rem(me + 2, 4)
    diag, chip = lax.rem(sib + 2, 4), me // 2
    n_pairs = w_in.shape[0] // PAIR
    slots = 32 * CAP
    bf, f32 = jnp.bfloat16, jnp.float32
    d_ff = w_in.shape[2]

    def fetch_in(q):
        slot = lax.rem(q, AHEAD)
        return pltpu.make_async_copy(w_in.at[pl.ds(PAIR * q, PAIR)], wi.at[slot], wi_sem.at[slot])

    def fetch_out(q):
        slot = lax.rem(q, AHEAD)
        return pltpu.make_async_copy(w_out.at[pl.ds(PAIR * q, PAIR)], wo.at[slot], wo_sem.at[slot])

    def remote(src, dst, s, r, peer):
        return pltpu.make_async_remote_copy(src_ref=src, dst_ref=dst, send_sem=s, recv_sem=r,
                                            device_id={"expert": peer}, device_id_type=MESH)

    barrier = pltpu.get_barrier_semaphore()
    for peer in (sib, cross, diag):
        pl.semaphore_signal(barrier, inc=1, device_id={"expert": peer}, device_id_type=MESH)
    args = [pltpu.make_async_copy(src, dst, arg_sem.at[k])
            for k, (src, dst) in enumerate(((idx_hbm, idx), (gate_hbm, gate), (x_hbm, x), (dy_hbm, dy)))]
    for copy in args:
        copy.start()
    for copy in args:
        copy.wait()
    pl.semaphore_wait(barrier, 3)

    small, over, near, far = [], [], [], []
    for k, peer in enumerate((cross, diag, sib)):
        small.append(remote(idx, ida.at[me], small_s.at[2 * k], small_r.at[2 * k], peer))
        small.append(remote(gate, ga.at[me], small_s.at[2 * k + 1], small_r.at[2 * k + 1], peer))
    for a, (src, dst) in enumerate(((x, xa), (dy, dya))):
        for c in range(2):
            rows = pl.ds(64 * c, 64)
            n = 2 * a + c
            over.append(remote(src.at[rows], dst.at[me, rows], cross_s.at[n], cross_r.at[n], cross))
            far.append(remote(dst.at[cross, rows], dst.at[cross, rows], fwd_s.at[n], fwd_r.at[n], sib))
        near.append(remote(src, dst.at[me], sib_s.at[a], sib_r.at[a], sib))
    for copy in small + over[:2] + near[:1] + over[2:] + near[1:]:
        copy.start()
    for q in range(AHEAD):
        fetch_in(q).start()
        fetch_out(q).start()
    xa[me] = x[...]
    dya[me] = dy[...]
    ida[me] = idx[...]
    ga[me] = gate[...]

    def forward(n):
        over[n].wait_recv()
        far[n].start()

    for copy in small:
        copy.wait_recv()
    tables(ida, me * 32, rj, r0s, r1s)
    slot_id = lax.broadcasted_iota(jnp.int32, (CAP, 128), 0).astype(f32)

    def one(q, _):
        inside, total = [], [jnp.zeros((CAP, 128), f32) for _ in range(PAIR)]
        for d in range(4):
            for p in range(PAIR):
                e = pl.ds(q * PAIR + p, 1)
                inside.append(jnp.where((slot_id >= r0s[d, e, :]) & (slot_id < r1s[d, e, :]), 1.0, 0.0))
                for j in range(8):
                    total[p] = jnp.where(slot_id == rj[j, d, e, :], ga[d, j:j + 1, :], total[p])
            pm[pair_rows(q), 128 * d:128 * (d + 1)] = jnp.concatenate(inside[-PAIR:], axis=0).astype(bf)
        gs[pair_rows(q), :] = jnp.sum(jnp.concatenate(total, axis=0), axis=1, keepdims=True)
        return 0

    lax.fori_loop(0, n_pairs, one, 0)
    forward(0)
    near[0].wait_recv()

    def half(devices):
        return pl.ds(pl.multiple_of(devices * 256, 256), 256)

    def pick_near(c, _):
        at = pl.ds(pl.multiple_of(c * PICK, PICK), PICK)
        rows = jnp.concatenate([xa[2 * chip], xa[2 * chip + 1]], axis=0)
        b_s[at, :] = dot(pm[at, half(chip)], rows).astype(bf)
        return 0

    lax.fori_loop(0, slots // PICK, pick_near, 0)
    forward(1)
    far[0].wait_recv()
    far[1].wait_recv()

    def pick_far(c, _):
        at = pl.ds(pl.multiple_of(c * PICK, PICK), PICK)
        rows = jnp.concatenate([xa[2 - 2 * chip], xa[3 - 2 * chip]], axis=0)
        b_s[at, :] += dot(pm[at, half(1 - chip)], rows).astype(bf)
        return 0

    lax.fori_loop(0, slots // PICK, pick_far, 0)

    first = lax.broadcasted_iota(jnp.int32, (PAIR * CAP, d_ff), 0) < CAP

    def fwd_step(i, _):
        slot = lax.rem(i, AHEAD)
        fetch_in(i).wait()
        fetch_out(i).wait()
        at = pair_rows(i)
        rows = b_s[at, :]
        a = jnp.concatenate([dot(rows, wi[slot, 0])[:CAP], dot(rows, wi[slot, 1])[CAP:]], axis=0)
        th = jnp.tanh(C0 * (a + C1 * (a * a * a)))
        cdf = 0.5 * (1.0 + th)
        slope[at, :] = cdf + 0.5 * a * (1.0 - th * th) * (C0 * (1.0 + 3.0 * C1 * (a * a)))
        h = a * cdf
        h = jnp.concatenate([jnp.where(first, h, 0.0), jnp.where(first, 0.0, h)], axis=1).astype(bf)
        h_s[at, :] = h
        o = dot(h, jnp.concatenate([wo[slot, 0], wo[slot, 1]], axis=0)).astype(bf)
        o_s[at, :] = o
        s = o.astype(f32) * gs[at, :]
        s1 = s.astype(bf)
        s = s - s1.astype(f32)
        s2 = s.astype(bf)
        s = s - s2.astype(f32)
        sp[0, at, :] = s1
        sp[1, at, :] = s2
        sp[2, at, :] = s.astype(bf)
        turned = i * (slots // 128) // n_pairs
        tile = pl.ds(pl.multiple_of(turned * 128, 128), 128)
        pt[:, tile] = pm[tile, :].astype(f32).T.astype(bf)

        @pl.when(i < n_pairs - AHEAD)
        def _():
            fetch_in(i + AHEAD).start()
            fetch_out(i + AHEAD).start()

        for n, when in ((2, 1), (3, 4)):
            @pl.when(i == when)
            def _(n=n):
                forward(n)
        return 0

    lax.fori_loop(0, n_pairs, fwd_step, 0)

    def to_sib(part, got, s, r, n, k):
        return remote(part.at[n, sib if k == 0 else diag], got.at[n, k], s.at[n, k], r.at[n, k], sib)

    def y_part(n, _):
        lanes = pl.ds(pl.multiple_of(n * 256, 256), 256)
        out = dot(pt[...], sp[0, :, lanes]) + dot(pt[...], sp[1, :, lanes]) + dot(pt[...], sp[2, :, lanes])
        for d in range(4):
            yp[n, d] = out[128 * d:128 * (d + 1)]

        @pl.when(n > 0)
        def _():
            for k in range(2):
                to_sib(yp, yr, yd_s, yd_r, n - 1, k).start()
        return 0

    lax.fori_loop(0, 4, y_part, 0)
    near[1].wait_recv()
    far[2].wait_recv()
    far[3].wait_recv()
    for k in range(2):
        to_sib(yp, yr, yd_s, yd_r, 3, k).start()

    def pick_dy(c, _):
        at = pl.ds(pl.multiple_of(c * PICK, PICK), PICK)
        rows = dot(pm[at, :], dya[...].reshape(512, dya.shape[2]))
        g_s[at, :] = (rows * gs[at, :]).astype(bf)
        prod = rows * o_s[at, :].astype(f32)
        part = sum((prod[:, 128 * k:128 * (k + 1)] for k in range(1, 8)), prod[:, :128])
        for k in range(PICK // CAP):
            dg_tab[pl.ds(c * (PICK // CAP) + k, 1), :CAP] = jnp.sum(part[CAP * k:CAP * (k + 1)].T, axis=0, keepdims=True)
        return 0

    lax.fori_loop(0, slots // PICK, pick_dy, 0)
    for n in range(4):
        for k in range(2):
            to_sib(yp, yr, yd_s, yd_r, n, k).wait()
        yfar[n] = yp[n, cross] + yr[n, 1]
    for d in range(4):
        for j in range(8):
            at = rj[j, d].astype(jnp.int32)
            got = jnp.take_along_axis(dg_tab[...], jnp.maximum(at, 0), axis=1)
            dgp[d, j:j + 1, :] = jnp.sum(jnp.where(at >= 0, got, 0.0), axis=0, keepdims=True)
    y_cross = remote(yfar, ygot, yx_s, yx_r, cross)
    y_cross.start()
    dg_back = [remote(dgp.at[peer], dgr.at[k], dg_s.at[k], dg_r.at[k], peer) for k, peer in enumerate((cross, diag, sib))]

    mine = lax.broadcasted_iota(jnp.int32, (d_ff, PAIR * CAP), 1) < CAP
    last = n_pairs - 1

    def back_h(i):
        slot, at = lax.rem(last - i, AHEAD), pair_rows(last - i)
        g = g_s[at, :]
        dh = jnp.where(mine, dot(wo[slot, 0], g, ((1,), (1,))), dot(wo[slot, 1], g, ((1,), (1,))))
        da = dh.astype(bf).T.astype(f32) * slope[at, :]
        da_s[at, :] = jnp.concatenate([jnp.where(first, da, 0.0), jnp.where(first, 0.0, da)], axis=1).astype(bf)

    def back_x(i):
        slot, at = lax.rem(last - i, AHEAD), pair_rows(last - i)
        wide = jnp.concatenate([wi[slot, 0], wi[slot, 1]], axis=1)
        sp[0, at, :] = dot(wide, da_s[at, :], ((1,), (1,))).astype(bf).T

    back_h(0)
    back_h(1)
    for copy in dg_back:
        copy.start()
    for i in range(2):
        fetch_out(last - AHEAD - i).start()

    def bwd_step(j, _):
        i = 2 * j

        @pl.when(i - 2 >= n_pairs - AHEAD)
        def _():
            for k in range(2):
                fetch_in(last + 2 - i - k).wait()

        @pl.when(i >= n_pairs - AHEAD)
        def _():
            for k in range(2):
                fetch_out(last - i - k).wait()

        back_x(i - 2)
        back_x(i - 1)
        back_h(i)
        back_h(i + 1)

        @pl.when(i < n_pairs - AHEAD)
        def _():
            for k in range(2):
                fetch_out(last - AHEAD - i - k).start()

        @pl.when(i < n_pairs - AHEAD + 2)
        def _():
            for k in range(2):
                fetch_in(last + 2 - AHEAD - i - k).start()
        return 0

    lax.fori_loop(1, n_pairs // 2, bwd_step, 0)
    y_cross.wait()
    for copy in dg_back:
        copy.wait()
    for i in range(2):
        fetch_in(i).wait()
    dg_out[...] = dgp[me] + (dgr[0] + (dgr[1] + dgr[2]))
    for n in range(4):
        lanes = slice(256 * n, 256 * (n + 1))
        y_out[:, lanes] = (x[:, lanes].astype(f32) + (yp[n, me] + yr[n, 0] + ygot[n])).astype(bf)
    back_x(last - 1)
    back_x(last)

    def dx_part(n, _):
        lanes = pl.ds(pl.multiple_of(n * 256, 256), 256)
        out = dot(pt[...], sp[0, :, lanes])
        for d in range(4):
            dxp[n, d] = out[128 * d:128 * (d + 1)]

        @pl.when(n > 0)
        def _():
            for k in range(2):
                to_sib(dxp, dxr, dd_s, dd_r, n - 1, k).start()
        return 0

    lax.fori_loop(0, 4, dx_part, 0)
    for k in range(2):
        to_sib(dxp, dxr, dd_s, dd_r, 3, k).start()
    for n in range(4):
        lanes = slice(256 * n, 256 * (n + 1))
        for k in range(2):
            to_sib(dxp, dxr, dd_s, dd_r, n, k).wait()
        dx_own[:, lanes] = dxp[n, me] + dxr[n, 0]
        dx_far[:, lanes] = dxp[n, cross] + dxr[n, 1]
    for copy in small + over + near + far:
        copy.wait_send()


def experts(x, dy, idx_t, gate_t, w_in, w_out):
    n_e, d_model, d_ff = w_in.shape
    slots = n_e * CAP
    bf, f32 = jnp.bfloat16, jnp.float32
    vmem, hbm = pl.BlockSpec(memory_space=pltpu.VMEM), pl.BlockSpec(memory_space=pl.ANY)
    buf, dma = pltpu.VMEM, pltpu.SemaphoreType.DMA
    return pl.pallas_call(
        expert_kernel,
        out_shape=[buf((128, d_model), bf), buf((8, 128), f32), buf((128, d_model), f32), buf((128, d_model), f32),
                   buf((slots, d_model), bf), buf((slots, PAIR * d_ff), bf), buf((slots, d_model), bf), buf((slots, PAIR * d_ff), bf)],
        in_specs=[hbm] * 6,
        out_specs=[vmem] * 8,
        scratch_shapes=[
            buf((128, d_model), bf), buf((128, d_model), bf), buf((8, 128), jnp.int32), buf((8, 128), f32),
            buf((4, 128, d_model), bf), buf((4, 128, d_model), bf), buf((4, 8, 128), jnp.int32), buf((4, 8, 128), f32),
            buf((8, 4, n_e, 128), f32), buf((4, n_e, 128), f32), buf((4, n_e, 128), f32),
            buf((slots, 512), bf), buf((512, slots), bf), buf((slots, 1), f32),
            buf((slots, d_model), bf), buf((slots, d_ff), f32), buf((3, slots, d_model), bf),
            buf((n_e, 128), f32), buf((4, 8, 128), f32), buf((3, 8, 128), f32),
            buf((AHEAD, PAIR, d_model, d_ff), bf), buf((AHEAD, PAIR, d_ff, d_model), bf),
            buf((4, 4, 128, 256), f32), buf((4, 2, 128, 256), f32), buf((4, 128, 256), f32), buf((4, 128, 256), f32),
            buf((4, 4, 128, 256), f32), buf((4, 2, 128, 256), f32),
            dma((4,)), dma((AHEAD,)), dma((AHEAD,)), dma((6,)), dma((6,)), dma((2,)), dma((2,)), dma((4,)), dma((4,)),
            dma((4,)), dma((4,)), dma((4, 2)), dma((4, 2)), dma(()), dma(()), dma((4, 2)), dma((4, 2)), dma((3,)), dma((3,))],
        compiler_params=pltpu.CompilerParams(collective_id=0, has_side_effects=True, vmem_limit_bytes=53 * 1024 * 1024),
        cost_estimate=pl.CostEstimate(flops=8 * slots * d_model * d_ff, bytes_accessed=8 * n_e * d_model * d_ff, transcendentals=0),
    )(x, dy, idx_t, gate_t, w_in, w_out)


def weight_kernel(b, h, g, da, y, dg, dw_in, dw_out, y_out, dg_out, ring_in, ring_out, sem_in, sem_out, sem):
    n_steps, d_ff = dw_in.shape[0] // PAIR, dw_in.shape[2]
    passed = [pltpu.make_async_copy(y, y_out, sem.at[0]), pltpu.make_async_copy(dg, dg_out, sem.at[1])]
    for copy in passed:
        copy.start()

    def copies(i):
        slot = lax.rem(i, RING)
        return [pltpu.make_async_copy(ring.at[slot, p], out.at[i * PAIR + p], sems.at[slot, p])
                for p in range(PAIR) for ring, out, sems in ((ring_in, dw_in, sem_in), (ring_out, dw_out, sem_out))]

    def step(i, _):
        slot = lax.rem(i, RING)

        @pl.when(i >= RING)
        def _():
            for copy in copies(i - RING):
                copy.wait()

        at = pair_rows(i)
        for p in range(PAIR):
            own = slice(d_ff * p, d_ff * (p + 1))
            ring_in[slot, p] = dot(b[at, :], da[at, own], ((0,), (0,))).astype(jnp.bfloat16)
            ring_out[slot, p] = dot(h[at, own], g[at, :], ((0,), (0,))).astype(jnp.bfloat16)
        for copy in copies(i):
            copy.start()
        return 0

    lax.fori_loop(0, n_steps, step, 0)
    for i in range(n_steps - RING, n_steps):
        for copy in copies(i):
            copy.wait()
    for copy in passed:
        copy.wait()


def weight_grads(b, h, g, da, y, dg, n_e):
    d_model, d_ff = b.shape[1], h.shape[1] // PAIR
    bf, shape, dma = jnp.bfloat16, jax.ShapeDtypeStruct, pltpu.SemaphoreType.DMA
    return pl.pallas_call(
        weight_kernel,
        out_shape=[shape((n_e, d_model, d_ff), bf), shape((n_e, d_ff, d_model), bf), shape(y.shape, y.dtype), shape(dg.shape, dg.dtype)],
        in_specs=[pl.BlockSpec(memory_space=pltpu.VMEM)] * 6,
        out_specs=[pl.BlockSpec(memory_space=pl.ANY)] * 4,
        scratch_shapes=[pltpu.VMEM((RING, PAIR, d_model, d_ff), bf), pltpu.VMEM((RING, PAIR, d_ff, d_model), bf),
                        dma((RING, PAIR)), dma((RING, PAIR)), dma((2,))],
        compiler_params=pltpu.CompilerParams(vmem_limit_bytes=40 * 1024 * 1024),
        cost_estimate=pl.CostEstimate(flops=4 * n_e * CAP * d_model * d_ff, bytes_accessed=4 * n_e * d_model * d_ff, transcendentals=0),
    )(b, h, g, da, y, dg)


def solution(mesh):
    tok_spec = P(('data', 'expert'), None)
    weight_spec = P('expert', None, None)
    grad_spec = P(('data', 'expert'), None, None)
    to_cross = [(i, i ^ 2) for i in range(4)]

    def device_pass(x_in, expert_idx, gate_weight, grad_y, w_in, w_out):
        y_mid, dg, dx_own, dx_far, b, h, g, da = experts(x_in, grad_y, expert_idx.T, gate_weight.T, w_in, w_out)
        dx_got = lax.ppermute(dx_far, 'expert', to_cross)
        grad_w_in, grad_w_out, y_out, dg = weight_grads(b, h, g, da, y_mid, dg, w_in.shape[0])
        grad_x = (grad_y.astype(jnp.float32) + (dx_own + dx_got)).astype(jnp.bfloat16)
        return y_out, grad_x, dg.T, grad_w_in, grad_w_out

    return jax.shard_map(device_pass, mesh=mesh,
                         in_specs=(tok_spec, tok_spec, tok_spec, tok_spec, weight_spec, weight_spec),
                         out_specs=(tok_spec, tok_spec, tok_spec, grad_spec, grad_spec), check_vma=False)
```

```python
import functools

import jax
import jax.numpy as jnp
from jax import lax
from jax.experimental import pallas as pl
from jax.experimental.pallas import tpu as pltpu
from jax.sharding import PartitionSpec as P

MESH = pl.DeviceIdType.MESH
CAP = 40
PAIR = 2
RING = 4
AHEAD = 8
PICK, PICK_DY = 640, 640
C0 = 0.7978845608028654
C1 = 0.044715


def dot(a, b, dims=((1,), (0,))):
    return lax.dot_general(a, b, (dims, ((), ())), preferred_element_type=jnp.float32)


def tables(ids_all, first, rj, r0s, r1s):
    eid = lax.broadcasted_iota(jnp.int32, (32, 128), 0) + first
    earlier = (lax.broadcasted_iota(jnp.int32, (128, 128), 0) < lax.broadcasted_iota(jnp.int32, (128, 128), 1)).astype(jnp.bfloat16)
    offset = jnp.zeros((32, 1), jnp.float32)
    for d in range(4):
        ids = ids_all[d]
        hits = [(ids[j:j + 1, :] == eid).astype(jnp.float32) for j in range(8)]
        count = sum(hits[1:], hits[0])
        rank = dot(count.astype(jnp.bfloat16), earlier) + offset
        r0s[d] = rank
        for j in range(8):
            rj[j, d] = jnp.where((hits[j] > 0.0) & (rank < CAP), rank, -1.0)
            rank = rank + hits[j]
        r1s[d] = jnp.minimum(rank, CAP)
        offset = offset + jnp.sum(count, axis=1, keepdims=True)


def pair_rows(q):
    return pl.ds(pl.multiple_of(q * PAIR * CAP, 16), PAIR * CAP)


def expert_kernel(x_hbm, dy_hbm, idx_hbm, gate_hbm, w_in, w_out, y_out, dg_out, dx_own, dx_far, b_s, h_s, g_s, da_s,
                  x, dy, idx, gate, xa, dya, ida, ga, rj, r0s, r1s, pm, pt, gs, o_s, slope, sp, dg_tab, dgp, dgr,
                  wi, wo, yp, yr, yfar, ygot, dxs, dxm, dxr,
                  arg_sem, wi_sem, wo_sem, small_s, small_r, sib_s, sib_r, cross_s, cross_r, fwd_s, fwd_r,
                  yd_s, yd_r, yx_s, yx_r, dd_s, dd_r, dg_s, dg_r):
    me = lax.axis_index("expert")
    sib, cross = me + 1 - 2 * lax.rem(me, 2), lax.rem(me + 2, 4)
    diag, chip = lax.rem(sib + 2, 4), me // 2
    n_pairs = w_in.shape[0] // PAIR
    slots = 32 * CAP
    bf, f32 = jnp.bfloat16, jnp.float32
    d_ff = w_in.shape[2]

    def fetch_in(q):
        slot = lax.rem(q, AHEAD)
        return pltpu.make_async_copy(w_in.at[pl.ds(PAIR * q, PAIR)], wi.at[slot], wi_sem.at[slot])

    def fetch_out(q):
        slot = lax.rem(q, AHEAD)
        return pltpu.make_async_copy(w_out.at[pl.ds(PAIR * q, PAIR)], wo.at[slot], wo_sem.at[slot])

    def remote(src, dst, s, r, peer):
        return pltpu.make_async_remote_copy(src_ref=src, dst_ref=dst, send_sem=s, recv_sem=r,
                                            device_id={"expert": peer}, device_id_type=MESH)

    barrier = pltpu.get_barrier_semaphore()
    for peer in (sib, cross, diag):
        pl.semaphore_signal(barrier, inc=1, device_id={"expert": peer}, device_id_type=MESH)
    args = [pltpu.make_async_copy(src, dst, arg_sem.at[k])
            for k, (src, dst) in enumerate(((idx_hbm, idx), (gate_hbm, gate), (x_hbm, x), (dy_hbm, dy)))]
    for copy in args:
        copy.start()
    for copy in args:
        copy.wait()
    pl.semaphore_wait(barrier, 3)

    small, over, near, far = [], [], [], []
    for k, peer in enumerate((cross, diag, sib)):
        small.append(remote(idx, ida.at[me], small_s.at[2 * k], small_r.at[2 * k], peer))
        small.append(remote(gate, ga.at[me], small_s.at[2 * k + 1], small_r.at[2 * k + 1], peer))
    for a, (src, dst) in enumerate(((x, xa), (dy, dya))):
        for c in range(2):
            rows = pl.ds(64 * c, 64)
            n = 2 * a + c
            over.append(remote(src.at[rows], dst.at[me, rows], cross_s.at[n], cross_r.at[n], cross))
            far.append(remote(dst.at[cross, rows], dst.at[cross, rows], fwd_s.at[n], fwd_r.at[n], sib))
        near.append(remote(src, dst.at[me], sib_s.at[a], sib_r.at[a], sib))
    for copy in small + over[:2] + near[:1] + over[2:] + near[1:]:
        copy.start()
    for q in range(AHEAD):
        fetch_in(q).start()
        fetch_out(q).start()
    xa[me] = x[...]
    dya[me] = dy[...]
    ida[me] = idx[...]
    ga[me] = gate[...]

    def forward(n):
        over[n].wait_recv()
        far[n].start()

    for copy in small:
        copy.wait_recv()
    tables(ida, me * 32, rj, r0s, r1s)
    slot_id = lax.broadcasted_iota(jnp.int32, (CAP, 128), 0).astype(f32)

    def one(q, _):
        inside, total = [], [jnp.zeros((CAP, 128), f32) for _ in range(PAIR)]
        for d in range(4):
            for p in range(PAIR):
                e = pl.ds(q * PAIR + p, 1)
                inside.append(jnp.where((slot_id >= r0s[d, e, :]) & (slot_id < r1s[d, e, :]), 1.0, 0.0))
                for j in range(8):
                    total[p] = jnp.where(slot_id == rj[j, d, e, :], ga[d, j:j + 1, :], total[p])
            pm[pair_rows(q), 128 * d:128 * (d + 1)] = jnp.concatenate(inside[-PAIR:], axis=0).astype(bf)
        gs[pair_rows(q), :] = jnp.sum(jnp.concatenate(total, axis=0), axis=1, keepdims=True)
        return 0

    lax.fori_loop(0, n_pairs, one, 0)
    forward(0)
    near[0].wait_recv()

    def half(devices):
        return pl.ds(pl.multiple_of(devices * 256, 256), 256)

    def pick_near(c, _):
        at = pl.ds(pl.multiple_of(c * PICK, PICK), PICK)
        rows = jnp.concatenate([xa[2 * chip], xa[2 * chip + 1]], axis=0)
        b_s[at, :] = dot(pm[at, half(chip)], rows).astype(bf)
        return 0

    lax.fori_loop(0, slots // PICK, pick_near, 0)
    forward(1)
    far[0].wait_recv()
    far[1].wait_recv()

    def pick_far(c, _):
        at = pl.ds(pl.multiple_of(c * PICK, PICK), PICK)
        rows = jnp.concatenate([xa[2 - 2 * chip], xa[3 - 2 * chip]], axis=0)
        b_s[at, :] += dot(pm[at, half(1 - chip)], rows).astype(bf)
        return 0

    lax.fori_loop(0, slots // PICK, pick_far, 0)

    first = lax.broadcasted_iota(jnp.int32, (PAIR * CAP, d_ff), 0) < CAP

    def fwd_h(i):
        slot, at = lax.rem(i, AHEAD), pair_rows(i)
        rows = b_s[at, :]
        a = jnp.concatenate([dot(rows, wi[slot, 0])[:CAP], dot(rows, wi[slot, 1])[CAP:]], axis=0)
        th = jnp.tanh(C0 * (a + C1 * (a * a * a)))
        cdf = 0.5 * (1.0 + th)
        slope[at, :] = cdf + 0.5 * a * (1.0 - th * th) * (C0 * (1.0 + 3.0 * C1 * (a * a)))
        h = a * cdf
        h_s[at, :] = jnp.concatenate([jnp.where(first, h, 0.0), jnp.where(first, 0.0, h)], axis=1).astype(bf)

    def fwd_o(i):
        slot, at = lax.rem(i, AHEAD), pair_rows(i)
        o = dot(h_s[at, :], jnp.concatenate([wo[slot, 0], wo[slot, 1]], axis=0)).astype(bf)
        o_s[at, :] = o
        s = o.astype(f32) * gs[at, :]
        s1 = s.astype(bf)
        s = s - s1.astype(f32)
        s2 = s.astype(bf)
        s = s - s2.astype(f32)
        sp[0, at, :] = s1
        sp[1, at, :] = s2
        sp[2, at, :] = s.astype(bf)

    for i in range(2):
        fetch_in(i).wait()
    fwd_h(0)
    fwd_h(1)
    for i in range(2):
        fetch_in(AHEAD + i).start()

    def fwd_step(j, _):
        i = 2 * j
        for k in range(2):
            fetch_in(i + k).wait()
            fetch_out(i - 2 + k).wait()
        fwd_o(i - 2)
        fwd_o(i - 1)
        fwd_h(i)
        fwd_h(i + 1)
        for k in range(2):
            tile = pl.ds(pl.multiple_of(lax.rem(i - 2 + k, slots // 128) * 128, 128), 128)
            pt[:, tile] = pm[tile, :].astype(f32).T.astype(bf)

        @pl.when(i < n_pairs - AHEAD)
        def _():
            for k in range(2):
                fetch_in(i + AHEAD + k).start()

        @pl.when(i < n_pairs - AHEAD + 2)
        def _():
            for k in range(2):
                fetch_out(i - 2 + AHEAD + k).start()

        for n, when in ((2, 2), (3, 4)):
            @pl.when(j == when)
            def _(n=n):
                forward(n)
        return 0

    lax.fori_loop(1, n_pairs // 2, fwd_step, 0)
    for i in range(n_pairs - 2, n_pairs):
        fetch_out(i).wait()
    fwd_o(n_pairs - 2)
    fwd_o(n_pairs - 1)

    def to_sib(part, got, s, r, n, k):
        return remote(part.at[n, sib if k == 0 else diag], got.at[n, k], s.at[n, k], r.at[n, k], sib)

    def y_part(n, _):
        lanes = pl.ds(pl.multiple_of(n * 256, 256), 256)
        out = dot(pt[...], sp[0, :, lanes]) + dot(pt[...], sp[1, :, lanes]) + dot(pt[...], sp[2, :, lanes])
        for d in range(4):
            yp[n, d] = out[128 * d:128 * (d + 1)]

        @pl.when(n > 0)
        def _():
            for k in range(2):
                to_sib(yp, yr, yd_s, yd_r, n - 1, k).start()
        return 0

    lax.fori_loop(0, 4, y_part, 0)
    near[1].wait_recv()
    far[2].wait_recv()
    far[3].wait_recv()
    for k in range(2):
        to_sib(yp, yr, yd_s, yd_r, 3, k).start()

    def pick_dy(c, _):
        at = pl.ds(pl.multiple_of(c * PICK_DY, PICK_DY), PICK_DY)
        rows = dot(pm[at, :], dya[...].reshape(512, dya.shape[2]))
        g_s[at, :] = (rows * gs[at, :]).astype(bf)
        prod = rows * o_s[at, :].astype(f32)
        part = sum((prod[:, 128 * k:128 * (k + 1)] for k in range(1, 8)), prod[:, :128])
        for k in range(PICK_DY // CAP):
            dg_tab[pl.ds(c * (PICK_DY // CAP) + k, 1), :CAP] = jnp.sum(part[CAP * k:CAP * (k + 1)].T, axis=0, keepdims=True)
        return 0

    lax.fori_loop(0, slots // PICK_DY, pick_dy, 0)
    for n in range(4):
        for k in range(2):
            to_sib(yp, yr, yd_s, yd_r, n, k).wait()
        yfar[n] = yp[n, cross] + yr[n, 1]
    for d in range(4):
        for j in range(8):
            at = rj[j, d].astype(jnp.int32)
            got = jnp.take_along_axis(dg_tab[...], jnp.maximum(at, 0), axis=1)
            dgp[d, j:j + 1, :] = jnp.sum(jnp.where(at >= 0, got, 0.0), axis=0, keepdims=True)
    y_cross = remote(yfar, ygot, yx_s, yx_r, cross)
    y_cross.start()
    dg_back = [remote(dgp.at[peer], dgr.at[k], dg_s.at[k], dg_r.at[k], peer) for k, peer in enumerate((cross, diag, sib))]

    mine = lax.broadcasted_iota(jnp.int32, (d_ff, PAIR * CAP), 1) < CAP
    last = n_pairs - 1

    def back_h(i):
        slot, at = lax.rem(last - i, AHEAD), pair_rows(last - i)
        g = g_s[at, :]
        dh = jnp.where(mine, dot(wo[slot, 0], g, ((1,), (1,))), dot(wo[slot, 1], g, ((1,), (1,))))
        da = dh.astype(bf).T.astype(f32) * slope[at, :]
        da_s[at, :] = jnp.concatenate([jnp.where(first, da, 0.0), jnp.where(first, 0.0, da)], axis=1).astype(bf)

    def back_x(i):
        slot, at = lax.rem(last - i, AHEAD), pair_rows(last - i)
        wide = jnp.concatenate([wi[slot, 0], wi[slot, 1]], axis=1)
        sp[0, at, :] = dot(wide, da_s[at, :], ((1,), (1,))).astype(bf).T

    back_h(0)
    back_h(1)
    for copy in dg_back:
        copy.start()
    for i in range(2):
        fetch_out(last - AHEAD - i).start()

    def bwd_step(j, _):
        i = 2 * j

        @pl.when(i - 2 >= n_pairs - AHEAD)
        def _():
            for k in range(2):
                fetch_in(last + 2 - i - k).wait()

        @pl.when(i >= n_pairs - AHEAD)
        def _():
            for k in range(2):
                fetch_out(last - i - k).wait()

        back_x(i - 2)
        back_x(i - 1)
        back_h(i)
        back_h(i + 1)

        @pl.when(i < n_pairs - AHEAD)
        def _():
            for k in range(2):
                fetch_out(last - AHEAD - i - k).start()

        @pl.when(i < n_pairs - AHEAD + 2)
        def _():
            for k in range(2):
                fetch_in(last + 2 - AHEAD - i - k).start()
        return 0

    lax.fori_loop(1, n_pairs // 2, bwd_step, 0)
    y_cross.wait()
    for copy in dg_back:
        copy.wait()
    for i in range(2):
        fetch_in(i).wait()
    dg_out[...] = dgp[me] + (dgr[0] + (dgr[1] + dgr[2]))
    for n in range(4):
        lanes = slice(256 * n, 256 * (n + 1))
        y_out[:, lanes] = (x[:, lanes].astype(f32) + (yp[n, me] + yr[n, 0] + ygot[n])).astype(bf)
    back_x(last - 1)
    back_x(last)

    def dx_send(n, k):
        return remote(dxs.at[n, k], dxr.at[n, k], dd_s.at[n, k], dd_r.at[n, k], sib)

    def dx_rows(n, into, d0, d1):
        lanes = pl.ds(pl.multiple_of(n * 256, 256), 256)
        chosen = jnp.concatenate([pt[pl.ds(pl.multiple_of(d * 128, 128), 128), :] for d in (d0, d1)], axis=0)
        out = dot(chosen, sp[0, :, lanes])
        into[n, 0] = out[:128]
        into[n, 1] = out[128:]

    def dx_theirs(n, _):
        dx_rows(n, dxs, sib, diag)

        @pl.when(n > 0)
        def _():
            for k in range(2):
                dx_send(n - 1, k).start()
        return 0

    def dx_ours(n, _):
        dx_rows(n, dxm, me, cross)

        @pl.when(n == 0)
        def _():
            for k in range(2):
                dx_send(3, k).start()
        return 0

    lax.fori_loop(0, 4, dx_theirs, 0)
    lax.fori_loop(0, 4, dx_ours, 0)
    for n in range(4):
        for k in range(2):
            dx_send(n, k).wait()
    for n in range(4):
        lanes = slice(256 * n, 256 * (n + 1))
        dx_own[:, lanes] = dxm[n, 0] + dxr[n, 0]
        dx_far[:, lanes] = dxm[n, 1] + dxr[n, 1]
    for copy in small + over + near + far:
        copy.wait_send()


def experts(x, dy, idx_t, gate_t, w_in, w_out):
    n_e, d_model, d_ff = w_in.shape
    slots = n_e * CAP
    bf, f32 = jnp.bfloat16, jnp.float32
    vmem, hbm = pl.BlockSpec(memory_space=pltpu.VMEM), pl.BlockSpec(memory_space=pl.ANY)
    buf, dma = pltpu.VMEM, pltpu.SemaphoreType.DMA
    return pl.pallas_call(
        expert_kernel,
        out_shape=[buf((128, d_model), bf), buf((8, 128), f32), buf((128, d_model), f32), buf((128, d_model), f32),
                   buf((slots, d_model), bf), buf((slots, PAIR * d_ff), bf), buf((slots, d_model), bf), buf((slots, PAIR * d_ff), bf)],
        in_specs=[hbm] * 6,
        out_specs=[vmem] * 8,
        scratch_shapes=[
            buf((128, d_model), bf), buf((128, d_model), bf), buf((8, 128), jnp.int32), buf((8, 128), f32),
            buf((4, 128, d_model), bf), buf((4, 128, d_model), bf), buf((4, 8, 128), jnp.int32), buf((4, 8, 128), f32),
            buf((8, 4, n_e, 128), f32), buf((4, n_e, 128), f32), buf((4, n_e, 128), f32),
            buf((slots, 512), bf), buf((512, slots), bf), buf((slots, 1), f32),
            buf((slots, d_model), bf), buf((slots, d_ff), f32), buf((3, slots, d_model), bf),
            buf((n_e, 128), f32), buf((4, 8, 128), f32), buf((3, 8, 128), f32),
            buf((AHEAD, PAIR, d_model, d_ff), bf), buf((AHEAD, PAIR, d_ff, d_model), bf),
            buf((4, 4, 128, 256), f32), buf((4, 2, 128, 256), f32), buf((4, 128, 256), f32), buf((4, 128, 256), f32),
            buf((4, 2, 128, 256), f32), buf((4, 2, 128, 256), f32), buf((4, 2, 128, 256), f32),
            dma((4,)), dma((AHEAD,)), dma((AHEAD,)), dma((6,)), dma((6,)), dma((2,)), dma((2,)), dma((4,)), dma((4,)),
            dma((4,)), dma((4,)), dma((4, 2)), dma((4, 2)), dma(()), dma(()), dma((4, 2)), dma((4, 2)), dma((3,)), dma((3,))],
        compiler_params=pltpu.CompilerParams(collective_id=0, has_side_effects=True, vmem_limit_bytes=53 * 1024 * 1024),
        cost_estimate=pl.CostEstimate(flops=8 * slots * d_model * d_ff, bytes_accessed=8 * n_e * d_model * d_ff, transcendentals=0),
    )(x, dy, idx_t, gate_t, w_in, w_out)


def weight_kernel(b, h, g, da, y, dg, dw_in, dw_out, y_out, dg_out, ring_in, ring_out, sem_in, sem_out, sem):
    n_steps, d_ff = dw_in.shape[0] // PAIR, dw_in.shape[2]
    passed = [pltpu.make_async_copy(y, y_out, sem.at[0]), pltpu.make_async_copy(dg, dg_out, sem.at[1])]
    for copy in passed:
        copy.start()

    def copy_in(i, p):
        slot = lax.rem(i, RING)
        return pltpu.make_async_copy(ring_in.at[slot, p], dw_in.at[i * PAIR + p], sem_in.at[slot, p])

    def copy_out(i, p):
        slot = lax.rem(i, RING)
        return pltpu.make_async_copy(ring_out.at[slot, p], dw_out.at[i * PAIR + p], sem_out.at[slot, p])

    def step(j, _):
        @pl.when(2 * j >= RING)
        def _():
            for k in range(2):
                for p in range(PAIR):
                    copy_in(2 * j + k - RING, p).wait()
                    copy_out(2 * j + k - RING, p).wait()

        for k in range(2):
            i = 2 * j + k
            slot, at = lax.rem(i, RING), pair_rows(i)
            for p in range(PAIR):
                own = slice(d_ff * p, d_ff * (p + 1))
                ring_in[slot, p] = dot(b[at, :], da[at, own], ((0,), (0,))).astype(jnp.bfloat16)
                copy_in(i, p).start()
                ring_out[slot, p] = dot(h[at, own], g[at, :], ((0,), (0,))).astype(jnp.bfloat16)
                copy_out(i, p).start()
        return 0

    lax.fori_loop(0, n_steps // 2, step, 0)
    for i in range(n_steps - RING, n_steps):
        for p in range(PAIR):
            copy_in(i, p).wait()
            copy_out(i, p).wait()
    for copy in passed:
        copy.wait()


def weight_grads(b, h, g, da, y, dg, n_e):
    d_model, d_ff = b.shape[1], h.shape[1] // PAIR
    bf, shape, dma = jnp.bfloat16, jax.ShapeDtypeStruct, pltpu.SemaphoreType.DMA
    return pl.pallas_call(
        weight_kernel,
        out_shape=[shape((n_e, d_model, d_ff), bf), shape((n_e, d_ff, d_model), bf), shape(y.shape, y.dtype), shape(dg.shape, dg.dtype)],
        in_specs=[pl.BlockSpec(memory_space=pltpu.VMEM)] * 6,
        out_specs=[pl.BlockSpec(memory_space=pl.ANY)] * 4,
        scratch_shapes=[pltpu.VMEM((RING, PAIR, d_model, d_ff), bf), pltpu.VMEM((RING, PAIR, d_ff, d_model), bf),
                        dma((RING, PAIR)), dma((RING, PAIR)), dma((2,))],
        compiler_params=pltpu.CompilerParams(vmem_limit_bytes=40 * 1024 * 1024),
        cost_estimate=pl.CostEstimate(flops=4 * n_e * CAP * d_model * d_ff, bytes_accessed=4 * n_e * d_model * d_ff, transcendentals=0),
    )(b, h, g, da, y, dg)


def solution(mesh):
    tok_spec = P(('data', 'expert'), None)
    weight_spec = P('expert', None, None)
    grad_spec = P(('data', 'expert'), None, None)
    to_cross = [(i, i ^ 2) for i in range(4)]

    def device_pass(x_in, expert_idx, gate_weight, grad_y, w_in, w_out):
        y_mid, dg, dx_own, dx_far, b, h, g, da = experts(x_in, grad_y, expert_idx.T, gate_weight.T, w_in, w_out)
        dx_got = lax.ppermute(dx_far, 'expert', to_cross)
        grad_w_in, grad_w_out, y_out, dg = weight_grads(b, h, g, da, y_mid, dg, w_in.shape[0])
        grad_x = (grad_y.astype(jnp.float32) + (dx_own + dx_got)).astype(jnp.bfloat16)
        return y_out, grad_x, dg.T, grad_w_in, grad_w_out

    return jax.shard_map(device_pass, mesh=mesh,
                         in_specs=(tok_spec, tok_spec, tok_spec, tok_spec, weight_spec, weight_spec),
                         out_specs=(tok_spec, tok_spec, tok_spec, grad_spec, grad_spec), check_vma=False)
```

```python
import functools

import jax
import jax.numpy as jnp
from jax import lax
from jax.experimental import pallas as pl
from jax.experimental.pallas import tpu as pltpu
from jax.sharding import PartitionSpec as P

MESH = pl.DeviceIdType.MESH
CAP = 40
PAIR = 2
RING = 4
AHEAD = 8
PICK, PICK_DY = 640, 640
C0 = 0.7978845608028654
C1 = 0.044715


def dot(a, b, dims=((1,), (0,))):
    return lax.dot_general(a, b, (dims, ((), ())), preferred_element_type=jnp.float32)


def tables(ids_all, first, rj, r0s, r1s):
    eid = lax.broadcasted_iota(jnp.int32, (32, 128), 0) + first
    earlier = (lax.broadcasted_iota(jnp.int32, (128, 128), 0) < lax.broadcasted_iota(jnp.int32, (128, 128), 1)).astype(jnp.bfloat16)
    offset = jnp.zeros((32, 1), jnp.float32)
    for d in range(4):
        ids = ids_all[d]
        hits = [(ids[j:j + 1, :] == eid).astype(jnp.float32) for j in range(8)]
        count = sum(hits[1:], hits[0])
        rank = dot(count.astype(jnp.bfloat16), earlier) + offset
        r0s[d] = rank
        for j in range(8):
            rj[j, d] = jnp.where((hits[j] > 0.0) & (rank < CAP), rank, -1.0)
            rank = rank + hits[j]
        r1s[d] = jnp.minimum(rank, CAP)
        offset = offset + jnp.sum(count, axis=1, keepdims=True)


def pair_rows(q):
    return pl.ds(pl.multiple_of(q * PAIR * CAP, 16), PAIR * CAP)


def expert_kernel(x_hbm, dy_hbm, idx_hbm, gate_hbm, w_in, w_out, y_out, dg_out, dx_own, dx_far, b_s, h_s, g_s, da_s,
                  x, dy, idx, gate, xa, dya, ida, ga, rj, r0s, r1s, pm, pt, gs, o_s, slope, sp, dg_tab, dgp, dgr,
                  wi, wo, yp, yr, yfar, ygot, dxs, dxm, dxr,
                  arg_sem, wi_sem, wo_sem, small_s, small_r, sib_s, sib_r, cross_s, cross_r, fwd_s, fwd_r,
                  yd_s, yd_r, yx_s, yx_r, dd_s, dd_r, dg_s, dg_r):
    me = lax.axis_index("expert")
    sib, cross = me + 1 - 2 * lax.rem(me, 2), lax.rem(me + 2, 4)
    diag, chip = lax.rem(sib + 2, 4), me // 2
    n_pairs = w_in.shape[0] // PAIR
    slots = 32 * CAP
    bf, f32 = jnp.bfloat16, jnp.float32
    d_ff = w_in.shape[2]

    def fetch_in(q):
        slot = lax.rem(q, AHEAD)
        return pltpu.make_async_copy(w_in.at[pl.ds(PAIR * q, PAIR)], wi.at[slot], wi_sem.at[slot])

    def fetch_out(q):
        slot = lax.rem(q, AHEAD)
        return pltpu.make_async_copy(w_out.at[pl.ds(PAIR * q, PAIR)], wo.at[slot], wo_sem.at[slot])

    def remote(src, dst, s, r, peer):
        return pltpu.make_async_remote_copy(src_ref=src, dst_ref=dst, send_sem=s, recv_sem=r,
                                            device_id={"expert": peer}, device_id_type=MESH)

    barrier = pltpu.get_barrier_semaphore()
    for peer in (sib, cross, diag):
        pl.semaphore_signal(barrier, inc=1, device_id={"expert": peer}, device_id_type=MESH)
    args = [pltpu.make_async_copy(src, dst, arg_sem.at[k])
            for k, (src, dst) in enumerate(((idx_hbm, idx), (gate_hbm, gate), (x_hbm, x), (dy_hbm, dy)))]
    for copy in args:
        copy.start()
    for copy in args:
        copy.wait()
    pl.semaphore_wait(barrier, 3)

    small, over, near, far = [], [], [], []
    for k, peer in enumerate((cross, diag, sib)):
        small.append(remote(idx, ida.at[me], small_s.at[2 * k], small_r.at[2 * k], peer))
        small.append(remote(gate, ga.at[me], small_s.at[2 * k + 1], small_r.at[2 * k + 1], peer))
    for a, (src, dst) in enumerate(((x, xa), (dy, dya))):
        for c in range(2):
            rows = pl.ds(64 * c, 64)
            n = 2 * a + c
            over.append(remote(src.at[rows], dst.at[me, rows], cross_s.at[n], cross_r.at[n], cross))
            far.append(remote(dst.at[cross, rows], dst.at[cross, rows], fwd_s.at[n], fwd_r.at[n], sib))
        near.append(remote(src, dst.at[me], sib_s.at[a], sib_r.at[a], sib))
    for copy in small + over[:2] + near[:1] + over[2:] + near[1:]:
        copy.start()
    for q in range(AHEAD):
        fetch_in(q).start()
        fetch_out(q).start()
    xa[me] = x[...]
    dya[me] = dy[...]
    ida[me] = idx[...]
    ga[me] = gate[...]

    def forward(n):
        over[n].wait_recv()
        far[n].start()

    for copy in small:
        copy.wait_recv()
    tables(ida, me * 32, rj, r0s, r1s)
    slot_id = lax.broadcasted_iota(jnp.int32, (CAP, 128), 0).astype(f32)

    def one(q, _):
        inside, total = [], [jnp.zeros((CAP, 128), f32) for _ in range(PAIR)]
        for d in range(4):
            for p in range(PAIR):
                e = pl.ds(q * PAIR + p, 1)
                inside.append(jnp.where((slot_id >= r0s[d, e, :]) & (slot_id < r1s[d, e, :]), 1.0, 0.0))
                for j in range(8):
                    total[p] = jnp.where(slot_id == rj[j, d, e, :], ga[d, j:j + 1, :], total[p])
            pm[pair_rows(q), 128 * d:128 * (d + 1)] = jnp.concatenate(inside[-PAIR:], axis=0).astype(bf)
        gs[pair_rows(q), :] = jnp.broadcast_to(jnp.sum(jnp.concatenate(total, axis=0), axis=1, keepdims=True), (PAIR * CAP, 128))
        return 0

    lax.fori_loop(0, n_pairs, one, 0)
    forward(0)
    near[0].wait_recv()

    def half(devices):
        return pl.ds(pl.multiple_of(devices * 256, 256), 256)

    def pick_near(c, _):
        at = pl.ds(pl.multiple_of(c * PICK, PICK), PICK)
        rows = jnp.concatenate([xa[2 * chip], xa[2 * chip + 1]], axis=0)
        b_s[at, :] = dot(pm[at, half(chip)], rows).astype(bf)
        return 0

    lax.fori_loop(0, slots // PICK, pick_near, 0)
    forward(1)
    far[0].wait_recv()
    far[1].wait_recv()

    def pick_far(c, _):
        at = pl.ds(pl.multiple_of(c * PICK, PICK), PICK)
        rows = jnp.concatenate([xa[2 - 2 * chip], xa[3 - 2 * chip]], axis=0)
        b_s[at, :] += dot(pm[at, half(1 - chip)], rows).astype(bf)
        return 0

    lax.fori_loop(0, slots // PICK, pick_far, 0)

    first = lax.broadcasted_iota(jnp.int32, (PAIR * CAP, d_ff), 0) < CAP

    def fwd_h(i):
        slot, at = lax.rem(i, AHEAD), pair_rows(i)
        rows = b_s[at, :]
        a = jnp.concatenate([dot(rows, wi[slot, 0])[:CAP], dot(rows, wi[slot, 1])[CAP:]], axis=0)
        th = jnp.tanh(C0 * (a + C1 * (a * a * a)))
        cdf = 0.5 * (1.0 + th)
        slope[at, :] = cdf + 0.5 * a * (1.0 - th * th) * (C0 * (1.0 + 3.0 * C1 * (a * a)))
        h = a * cdf
        h_s[at, :] = jnp.concatenate([jnp.where(first, h, 0.0), jnp.where(first, 0.0, h)], axis=1).astype(bf)

    def fwd_o(i):
        slot, at = lax.rem(i, AHEAD), pair_rows(i)
        o = dot(h_s[at, :], jnp.concatenate([wo[slot, 0], wo[slot, 1]], axis=0)).astype(bf)
        o_s[at, :] = o
        s = o.astype(f32) * jnp.concatenate([gs[at, :]] * 8, axis=1)
        s1 = s.astype(bf)
        s = s - s1.astype(f32)
        s2 = s.astype(bf)
        s = s - s2.astype(f32)
        sp[0, at, :] = s1
        sp[1, at, :] = s2
        sp[2, at, :] = s.astype(bf)

    for i in range(2):
        fetch_in(i).wait()
    fwd_h(0)
    fwd_h(1)
    for i in range(2):
        fetch_in(AHEAD + i).start()

    def fwd_step(j, _):
        i = 2 * j
        for k in range(2):
            fetch_in(i + k).wait()
            fetch_out(i - 2 + k).wait()
        fwd_o(i - 2)
        fwd_o(i - 1)
        fwd_h(i)
        fwd_h(i + 1)
        for k in range(2):
            tile = pl.ds(pl.multiple_of(lax.rem(i - 2 + k, slots // 128) * 128, 128), 128)
            pt[:, tile] = pm[tile, :].astype(f32).T.astype(bf)

        @pl.when(i < n_pairs - AHEAD)
        def _():
            for k in range(2):
                fetch_in(i + AHEAD + k).start()

        @pl.when(i < n_pairs - AHEAD + 2)
        def _():
            for k in range(2):
                fetch_out(i - 2 + AHEAD + k).start()

        for n, when in ((2, 2), (3, 4)):
            @pl.when(j == when)
            def _(n=n):
                forward(n)
        return 0

    lax.fori_loop(1, n_pairs // 2, fwd_step, 0)
    for i in range(n_pairs - 2, n_pairs):
        fetch_out(i).wait()
    fwd_o(n_pairs - 2)
    fwd_o(n_pairs - 1)

    def to_sib(part, got, s, r, n, k):
        return remote(part.at[n, sib if k == 0 else diag], got.at[n, k], s.at[n, k], r.at[n, k], sib)

    def y_part(c, _):
        for n in (2 * c, 2 * c + 1):
            lanes = pl.ds(pl.multiple_of(n * 256, 256), 256)
            out = dot(pt[...], sp[0, :, lanes]) + dot(pt[...], sp[1, :, lanes]) + dot(pt[...], sp[2, :, lanes])
            for d in range(4):
                yp[n, d] = out[128 * d:128 * (d + 1)]

        @pl.when(c > 0)
        def _():
            for n in range(2):
                for k in range(2):
                    to_sib(yp, yr, yd_s, yd_r, n, k).start()
        return 0

    lax.fori_loop(0, 2, y_part, 0)
    near[1].wait_recv()
    far[2].wait_recv()
    far[3].wait_recv()
    for n in range(2, 4):
        for k in range(2):
            to_sib(yp, yr, yd_s, yd_r, n, k).start()

    def pick_dy(c, _):
        at = pl.ds(pl.multiple_of(c * PICK_DY, PICK_DY), PICK_DY)
        part = jnp.zeros((PICK_DY, 128), f32)
        for n in range(4):
            lanes = slice(256 * n, 256 * (n + 1))
            rows = dot(pm[at, :], dya[:, :, lanes].reshape(512, 256))
            g_s[at, lanes] = (rows * jnp.concatenate([gs[at, :]] * 2, axis=1)).astype(bf)
            prod = rows * o_s[at, lanes].astype(f32)
            part = part + (prod[:, :128] + prod[:, 128:])
        for k in range(PICK_DY // CAP):
            dg_tab[pl.ds(c * (PICK_DY // CAP) + k, 1), :CAP] = jnp.sum(part[CAP * k:CAP * (k + 1)].T, axis=0, keepdims=True)
        return 0

    lax.fori_loop(0, slots // PICK_DY, pick_dy, 0)
    for n in range(4):
        for k in range(2):
            to_sib(yp, yr, yd_s, yd_r, n, k).wait()
        yfar[n] = yp[n, cross] + yr[n, 1]
    y_cross = remote(yfar, ygot, yx_s, yx_r, cross)
    y_cross.start()
    dg_back = [remote(dgp.at[peer], dgr.at[k], dg_s.at[k], dg_r.at[k], peer) for k, peer in enumerate((cross, diag, sib))]

    mine = lax.broadcasted_iota(jnp.int32, (d_ff, PAIR * CAP), 1) < CAP
    last = n_pairs - 1

    def back_h(i):
        slot, at = lax.rem(last - i, AHEAD), pair_rows(last - i)
        g = g_s[at, :]
        dh = jnp.where(mine, dot(wo[slot, 0], g, ((1,), (1,))), dot(wo[slot, 1], g, ((1,), (1,))))
        da = dh.astype(bf).T.astype(f32) * slope[at, :]
        da_s[at, :] = jnp.concatenate([jnp.where(first, da, 0.0), jnp.where(first, 0.0, da)], axis=1).astype(bf)

    def back_x(i):
        slot, at = lax.rem(last - i, AHEAD), pair_rows(last - i)
        wide = jnp.concatenate([wi[slot, 0], wi[slot, 1]], axis=1)
        sp[0, at, :] = dot(wide, da_s[at, :], ((1,), (1,))).astype(bf).T

    back_h(0)
    back_h(1)
    for i in range(2):
        fetch_out(last - AHEAD - i).start()

    def bwd_step(j, _):
        i = 2 * j

        @pl.when(i - 2 >= n_pairs - AHEAD)
        def _():
            for k in range(2):
                fetch_in(last + 2 - i - k).wait()

        @pl.when(i >= n_pairs - AHEAD)
        def _():
            for k in range(2):
                fetch_out(last - i - k).wait()

        back_x(i - 2)
        back_x(i - 1)
        back_h(i)
        back_h(i + 1)
        for k in range(5):
            row = lax.rem(5 * j - 5 + k, 32)
            d, choice = row // 8, lax.rem(row, 8)
            at = rj[choice, d].astype(jnp.int32)
            got = jnp.take_along_axis(dg_tab[...], jnp.maximum(at, 0), axis=1)
            dgp[d, pl.ds(choice, 1), :] = jnp.sum(jnp.where(at >= 0, got, 0.0), axis=0, keepdims=True)

        @pl.when(i < n_pairs - AHEAD)
        def _():
            for k in range(2):
                fetch_out(last - AHEAD - i - k).start()

        @pl.when(i < n_pairs - AHEAD + 2)
        def _():
            for k in range(2):
                fetch_in(last + 2 - AHEAD - i - k).start()
        return 0

    lax.fori_loop(1, n_pairs // 2, bwd_step, 0)
    for copy in dg_back:
        copy.start()
    y_cross.wait()
    for i in range(2):
        fetch_in(i).wait()
    back_x(last - 1)
    back_x(last)

    def dx_send(n, k):
        return remote(dxs.at[n, k], dxr.at[n, k], dd_s.at[n, k], dd_r.at[n, k], sib)

    def dx_rows(n, into, d0, d1):
        lanes = slice(256 * n, 256 * (n + 1))
        chosen = jnp.concatenate([pt[pl.ds(pl.multiple_of(d * 128, 128), 128), :] for d in (d0, d1)], axis=0)
        out = dot(chosen, sp[0, :, lanes])
        into[n, 0] = out[:128]
        into[n, 1] = out[128:]

    for n in range(4):
        dx_rows(n, dxs, sib, diag)
        lanes = slice(256 * n, 256 * (n + 1))
        y_out[:, lanes] = (x[:, lanes].astype(f32) + (yp[n, me] + yr[n, 0] + ygot[n])).astype(bf)
        for k in range(2):
            if n > 0:
                dx_send(n - 1, k).start()
    for n in range(4):
        dx_rows(n, dxm, me, cross)
        for k in range(2):
            if n == 0:
                dx_send(3, k).start()
    for copy in dg_back:
        copy.wait()
    dg_out[...] = dgp[me] + (dgr[0] + (dgr[1] + dgr[2]))
    for n in range(4):
        for k in range(2):
            dx_send(n, k).wait()
    for n in range(4):
        lanes = slice(256 * n, 256 * (n + 1))
        dx_own[:, lanes] = dxm[n, 0] + dxr[n, 0]
        dx_far[:, lanes] = dxm[n, 1] + dxr[n, 1]
    for copy in small + over + near + far:
        copy.wait_send()


def experts(x, dy, idx_t, gate_t, w_in, w_out):
    n_e, d_model, d_ff = w_in.shape
    slots = n_e * CAP
    bf, f32 = jnp.bfloat16, jnp.float32
    vmem, hbm = pl.BlockSpec(memory_space=pltpu.VMEM), pl.BlockSpec(memory_space=pl.ANY)
    buf, dma = pltpu.VMEM, pltpu.SemaphoreType.DMA
    return pl.pallas_call(
        expert_kernel,
        out_shape=[buf((128, d_model), bf), buf((8, 128), f32), buf((128, d_model), f32), buf((128, d_model), f32),
                   buf((slots, d_model), bf), buf((slots, PAIR * d_ff), bf), buf((slots, d_model), bf), buf((slots, PAIR * d_ff), bf)],
        in_specs=[hbm] * 6,
        out_specs=[vmem] * 8,
        scratch_shapes=[
            buf((128, d_model), bf), buf((128, d_model), bf), buf((8, 128), jnp.int32), buf((8, 128), f32),
            buf((4, 128, d_model), bf), buf((4, 128, d_model), bf), buf((4, 8, 128), jnp.int32), buf((4, 8, 128), f32),
            buf((8, 4, n_e, 128), f32), buf((4, n_e, 128), f32), buf((4, n_e, 128), f32),
            buf((slots, 512), bf), buf((512, slots), bf), buf((slots, 128), f32),
            buf((slots, d_model), bf), buf((slots, d_ff), f32), buf((3, slots, d_model), bf),
            buf((n_e, 128), f32), buf((4, 8, 128), f32), buf((3, 8, 128), f32),
            buf((AHEAD, PAIR, d_model, d_ff), bf), buf((AHEAD, PAIR, d_ff, d_model), bf),
            buf((4, 4, 128, 256), f32), buf((4, 2, 128, 256), f32), buf((4, 128, 256), f32), buf((4, 128, 256), f32),
            buf((4, 2, 128, 256), f32), buf((4, 2, 128, 256), f32), buf((4, 2, 128, 256), f32),
            dma((4,)), dma((AHEAD,)), dma((AHEAD,)), dma((6,)), dma((6,)), dma((2,)), dma((2,)), dma((4,)), dma((4,)),
            dma((4,)), dma((4,)), dma((4, 2)), dma((4, 2)), dma(()), dma(()), dma((4, 2)), dma((4, 2)), dma((3,)), dma((3,))],
        compiler_params=pltpu.CompilerParams(collective_id=0, has_side_effects=True, vmem_limit_bytes=53 * 1024 * 1024),
        cost_estimate=pl.CostEstimate(flops=8 * slots * d_model * d_ff, bytes_accessed=8 * n_e * d_model * d_ff, transcendentals=0),
    )(x, dy, idx_t, gate_t, w_in, w_out)


def weight_kernel(b, h, g, da, y, dg, dw_in, dw_out, y_out, dg_out, ring_in, ring_out, sem_in, sem_out, sem):
    n_steps, d_ff = dw_in.shape[0] // PAIR, dw_in.shape[2]
    passed = [pltpu.make_async_copy(y, y_out, sem.at[0]), pltpu.make_async_copy(dg, dg_out, sem.at[1])]
    for copy in passed:
        copy.start()

    def copy_in(i, p):
        slot = lax.rem(i, RING)
        return pltpu.make_async_copy(ring_in.at[slot, p], dw_in.at[i * PAIR + p], sem_in.at[slot, p])

    def copy_out(i, p):
        slot = lax.rem(i, RING)
        return pltpu.make_async_copy(ring_out.at[slot, p], dw_out.at[i * PAIR + p], sem_out.at[slot, p])

    def step(j, _):
        @pl.when(2 * j >= RING)
        def _():
            for k in range(2):
                for p in range(PAIR):
                    copy_in(2 * j + k - RING, p).wait()
                    copy_out(2 * j + k - RING, p).wait()

        for k in range(2):
            i = 2 * j + k
            slot, at = lax.rem(i, RING), pair_rows(i)
            for p in range(PAIR):
                own = slice(d_ff * p, d_ff * (p + 1))
                ring_in[slot, p] = dot(b[at, :], da[at, own], ((0,), (0,))).astype(jnp.bfloat16)
                copy_in(i, p).start()
                ring_out[slot, p] = dot(h[at, own], g[at, :], ((0,), (0,))).astype(jnp.bfloat16)
                copy_out(i, p).start()
        return 0

    lax.fori_loop(0, n_steps // 2, step, 0)
    for i in range(n_steps - RING, n_steps):
        for p in range(PAIR):
            copy_in(i, p).wait()
            copy_out(i, p).wait()
    for copy in passed:
        copy.wait()


def weight_grads(b, h, g, da, y, dg, n_e):
    d_model, d_ff = b.shape[1], h.shape[1] // PAIR
    bf, shape, dma = jnp.bfloat16, jax.ShapeDtypeStruct, pltpu.SemaphoreType.DMA
    return pl.pallas_call(
        weight_kernel,
        out_shape=[shape((n_e, d_model, d_ff), bf), shape((n_e, d_ff, d_model), bf), shape(y.shape, y.dtype), shape(dg.shape, dg.dtype)],
        in_specs=[pl.BlockSpec(memory_space=pltpu.VMEM)] * 6,
        out_specs=[pl.BlockSpec(memory_space=pl.ANY)] * 4,
        scratch_shapes=[pltpu.VMEM((RING, PAIR, d_model, d_ff), bf), pltpu.VMEM((RING, PAIR, d_ff, d_model), bf),
                        dma((RING, PAIR)), dma((RING, PAIR)), dma((2,))],
        compiler_params=pltpu.CompilerParams(vmem_limit_bytes=40 * 1024 * 1024),
        cost_estimate=pl.CostEstimate(flops=4 * n_e * CAP * d_model * d_ff, bytes_accessed=4 * n_e * d_model * d_ff, transcendentals=0),
    )(b, h, g, da, y, dg)


def solution(mesh):
    tok_spec = P(('data', 'expert'), None)
    weight_spec = P('expert', None, None)
    grad_spec = P(('data', 'expert'), None, None)
    to_cross = [(i, i ^ 2) for i in range(4)]

    def device_pass(x_in, expert_idx, gate_weight, grad_y, w_in, w_out):
        y_mid, dg, dx_own, dx_far, b, h, g, da = experts(x_in, grad_y, expert_idx.T, gate_weight.T, w_in, w_out)
        dx_got = lax.ppermute(dx_far, 'expert', to_cross)
        grad_w_in, grad_w_out, y_out, dg = weight_grads(b, h, g, da, y_mid, dg, w_in.shape[0])
        grad_x = (grad_y.astype(jnp.float32) + (dx_own + dx_got)).astype(jnp.bfloat16)
        return y_out, grad_x, dg.T, grad_w_in, grad_w_out

    return jax.shard_map(device_pass, mesh=mesh,
                         in_specs=(tok_spec, tok_spec, tok_spec, tok_spec, weight_spec, weight_spec),
                         out_specs=(tok_spec, tok_spec, tok_spec, grad_spec, grad_spec), check_vma=False)
```

```python
import functools

import jax
import jax.numpy as jnp
from jax import lax
from jax.experimental import pallas as pl
from jax.experimental.pallas import tpu as pltpu
from jax.sharding import PartitionSpec as P

MESH = pl.DeviceIdType.MESH
CAP = 40
PAIR = 2
RING = 4
AHEAD = 8
PICK, PICK_DY = 640, 640
C0 = 0.7978845608028654
C1 = 0.044715


def dot(a, b, dims=((1,), (0,))):
    return lax.dot_general(a, b, (dims, ((), ())), preferred_element_type=jnp.float32)


def tables(ids_all, first, rj, r0s, r1s):
    eid = lax.broadcasted_iota(jnp.int32, (32, 128), 0) + first
    earlier = (lax.broadcasted_iota(jnp.int32, (128, 128), 0) < lax.broadcasted_iota(jnp.int32, (128, 128), 1)).astype(jnp.bfloat16)
    offset = jnp.zeros((32, 1), jnp.float32)
    for d in range(4):
        ids = ids_all[d]
        hits = [(ids[j:j + 1, :] == eid).astype(jnp.float32) for j in range(8)]
        count = sum(hits[1:], hits[0])
        rank = dot(count.astype(jnp.bfloat16), earlier) + offset
        r0s[d] = rank
        for j in range(8):
            rj[j, d] = jnp.where((hits[j] > 0.0) & (rank < CAP), rank, -1.0)
            rank = rank + hits[j]
        r1s[d] = jnp.minimum(rank, CAP)
        offset = offset + jnp.sum(count, axis=1, keepdims=True)


def pair_rows(q):
    return pl.ds(pl.multiple_of(q * PAIR * CAP, 16), PAIR * CAP)


def expert_kernel(x_hbm, dy_hbm, idx_hbm, gate_hbm, w_in, w_out, y_out, dg_out, dx_own, dx_far, b_s, h_s, g_s, da_s,
                  x, dy, idx, gate, xa, dya, ida, ga, rj, r0s, r1s, pm, pt, gs, o_s, slope, sp, dg_tab, dgp, dgr,
                  wi, wo, yp, yr, yfar, ygot, dxs, dxm, dxr,
                  arg_sem, wi_sem, wo_sem, small_s, small_r, sib_s, sib_r, cross_s, cross_r, fwd_s, fwd_r,
                  yd_s, yd_r, yx_s, yx_r, dd_s, dd_r, dg_s, dg_r):
    me = lax.axis_index("expert")
    sib, cross = me + 1 - 2 * lax.rem(me, 2), lax.rem(me + 2, 4)
    diag, chip = lax.rem(sib + 2, 4), me // 2
    n_pairs = w_in.shape[0] // PAIR
    slots = 32 * CAP
    bf, f32 = jnp.bfloat16, jnp.float32
    d_ff = w_in.shape[2]

    def fetch_in(q):
        slot = lax.rem(q, AHEAD)
        return pltpu.make_async_copy(w_in.at[pl.ds(PAIR * q, PAIR)], wi.at[slot], wi_sem.at[slot])

    def fetch_out(q):
        slot = lax.rem(q, AHEAD)
        return pltpu.make_async_copy(w_out.at[pl.ds(PAIR * q, PAIR)], wo.at[slot], wo_sem.at[slot])

    def remote(src, dst, s, r, peer):
        return pltpu.make_async_remote_copy(src_ref=src, dst_ref=dst, send_sem=s, recv_sem=r,
                                            device_id={"expert": peer}, device_id_type=MESH)

    barrier = pltpu.get_barrier_semaphore()
    for peer in (sib, cross, diag):
        pl.semaphore_signal(barrier, inc=1, device_id={"expert": peer}, device_id_type=MESH)
    args = [pltpu.make_async_copy(src, dst, arg_sem.at[k])
            for k, (src, dst) in enumerate(((idx_hbm, idx), (gate_hbm, gate), (x_hbm, x), (dy_hbm, dy)))]
    for copy in args:
        copy.start()
    for copy in args:
        copy.wait()
    pl.semaphore_wait(barrier, 3)

    small, over, near, far = [], [], [], []
    for k, peer in enumerate((cross, diag, sib)):
        small.append(remote(idx, ida.at[me], small_s.at[2 * k], small_r.at[2 * k], peer))
        small.append(remote(gate, ga.at[me], small_s.at[2 * k + 1], small_r.at[2 * k + 1], peer))
    for a, (src, dst) in enumerate(((x, xa), (dy, dya))):
        for c in range(2):
            rows = pl.ds(64 * c, 64)
            n = 2 * a + c
            over.append(remote(src.at[rows], dst.at[me, rows], cross_s.at[n], cross_r.at[n], cross))
            far.append(remote(dst.at[cross, rows], dst.at[cross, rows], fwd_s.at[n], fwd_r.at[n], sib))
        near.append(remote(src, dst.at[me], sib_s.at[a], sib_r.at[a], sib))
    for copy in small + over[:2] + near[:1] + over[2:] + near[1:]:
        copy.start()
    for q in range(AHEAD):
        fetch_in(q).start()
        fetch_out(q).start()
    xa[me] = x[...]
    dya[me] = dy[...]
    ida[me] = idx[...]
    ga[me] = gate[...]

    def forward(n):
        over[n].wait_recv()
        far[n].start()

    for copy in small:
        copy.wait_recv()
    tables(ida, me * 32, rj, r0s, r1s)
    slot_id = lax.broadcasted_iota(jnp.int32, (CAP, 128), 0).astype(f32)

    def one(q, _):
        inside, total = [], [jnp.zeros((CAP, 128), f32) for _ in range(PAIR)]
        for d in range(4):
            for p in range(PAIR):
                e = pl.ds(q * PAIR + p, 1)
                inside.append(jnp.where((slot_id >= r0s[d, e, :]) & (slot_id < r1s[d, e, :]), 1.0, 0.0))
                for j in range(8):
                    total[p] = jnp.where(slot_id == rj[j, d, e, :], ga[d, j:j + 1, :], total[p])
            pm[pair_rows(q), 128 * d:128 * (d + 1)] = jnp.concatenate(inside[-PAIR:], axis=0).astype(bf)
        gs[pair_rows(q), :] = jnp.broadcast_to(jnp.sum(jnp.concatenate(total, axis=0), axis=1, keepdims=True), (PAIR * CAP, 128))
        return 0

    lax.fori_loop(0, n_pairs, one, 0)
    forward(0)
    near[0].wait_recv()

    def half(devices):
        return pl.ds(pl.multiple_of(devices * 256, 256), 256)

    def pick_near(c, _):
        at = pl.ds(pl.multiple_of(c * PICK, PICK), PICK)
        rows = jnp.concatenate([xa[2 * chip], xa[2 * chip + 1]], axis=0)
        b_s[at, :] = dot(pm[at, half(chip)], rows).astype(bf)
        return 0

    lax.fori_loop(0, slots // PICK, pick_near, 0)
    forward(1)
    far[0].wait_recv()
    far[1].wait_recv()

    for c in range(slots // PICK):
        at = pl.ds(c * PICK, PICK)
        rows = jnp.concatenate([xa[2 - 2 * chip], xa[3 - 2 * chip]], axis=0)
        b_s[at, :] += dot(pm[at, half(1 - chip)], rows).astype(bf)

    first = lax.broadcasted_iota(jnp.int32, (PAIR * CAP, d_ff), 0) < CAP

    def fwd_h(i):
        slot, at = lax.rem(i, AHEAD), pair_rows(i)
        rows = b_s[at, :]
        a = jnp.concatenate([dot(rows, wi[slot, 0])[:CAP], dot(rows, wi[slot, 1])[CAP:]], axis=0)
        th = jnp.tanh(C0 * (a + C1 * (a * a * a)))
        cdf = 0.5 * (1.0 + th)
        slope[at, :] = cdf + 0.5 * a * (1.0 - th * th) * (C0 * (1.0 + 3.0 * C1 * (a * a)))
        h = a * cdf
        h_s[at, :] = jnp.concatenate([jnp.where(first, h, 0.0), jnp.where(first, 0.0, h)], axis=1).astype(bf)

    def fwd_o(i):
        slot, at = lax.rem(i, AHEAD), pair_rows(i)
        o = dot(h_s[at, :], jnp.concatenate([wo[slot, 0], wo[slot, 1]], axis=0)).astype(bf)
        o_s[at, :] = o
        s = o.astype(f32) * jnp.concatenate([gs[at, :]] * 8, axis=1)
        s1 = s.astype(bf)
        s = s - s1.astype(f32)
        s2 = s.astype(bf)
        s = s - s2.astype(f32)
        sp[0, at, :] = s1
        sp[1, at, :] = s2
        sp[2, at, :] = s.astype(bf)

    for i in range(2):
        fetch_in(i).wait()
    fwd_h(0)
    fwd_h(1)
    for i in range(2):
        fetch_in(AHEAD + i).start()

    def fwd_step(j, _):
        i = 2 * j
        for k in range(2):
            fetch_in(i + k).wait()
            fetch_out(i - 2 + k).wait()
        fwd_o(i - 2)
        fwd_o(i - 1)
        fwd_h(i)
        fwd_h(i + 1)
        for k in range(2):
            tile = pl.ds(pl.multiple_of(lax.rem(i - 2 + k, slots // 128) * 128, 128), 128)
            pt[:, tile] = pm[tile, :].astype(f32).T.astype(bf)

        @pl.when(i < n_pairs - AHEAD)
        def _():
            for k in range(2):
                fetch_in(i + AHEAD + k).start()

        @pl.when(i < n_pairs - AHEAD + 2)
        def _():
            for k in range(2):
                fetch_out(i - 2 + AHEAD + k).start()

        for n, when in ((2, 2), (3, 4)):
            @pl.when(j == when)
            def _(n=n):
                forward(n)
        return 0

    lax.fori_loop(1, n_pairs // 2, fwd_step, 0)
    for i in range(n_pairs - 2, n_pairs):
        fetch_out(i).wait()
    fwd_o(n_pairs - 2)
    fwd_o(n_pairs - 1)

    def to_sib(part, got, s, r, n, k):
        return remote(part.at[n, sib if k == 0 else diag], got.at[n, k], s.at[n, k], r.at[n, k], sib)

    def y_part(c, _):
        for n in (2 * c, 2 * c + 1):
            lanes = pl.ds(pl.multiple_of(n * 256, 256), 256)
            out = dot(pt[...], sp[0, :, lanes]) + dot(pt[...], sp[1, :, lanes]) + dot(pt[...], sp[2, :, lanes])
            for d in range(4):
                yp[n, d] = out[128 * d:128 * (d + 1)]

        @pl.when(c > 0)
        def _():
            for n in range(2):
                for k in range(2):
                    to_sib(yp, yr, yd_s, yd_r, n, k).start()
        return 0

    lax.fori_loop(0, 2, y_part, 0)
    near[1].wait_recv()
    far[2].wait_recv()
    far[3].wait_recv()
    for n in range(2, 4):
        for k in range(2):
            to_sib(yp, yr, yd_s, yd_r, n, k).start()

    for c in range(slots // PICK_DY):
        at = pl.ds(c * PICK_DY, PICK_DY)
        part = jnp.zeros((PICK_DY, 128), f32)
        for n in range(4):
            lanes = slice(256 * n, 256 * (n + 1))
            rows = dot(pm[at, :], dya[:, :, lanes].reshape(512, 256))
            g_s[at, lanes] = (rows * jnp.concatenate([gs[at, :]] * 2, axis=1)).astype(bf)
            prod = rows * o_s[at, lanes].astype(f32)
            part = part + (prod[:, :128] + prod[:, 128:])
        for k in range(PICK_DY // CAP):
            dg_tab[pl.ds(c * (PICK_DY // CAP) + k, 1), :CAP] = jnp.sum(part[CAP * k:CAP * (k + 1)].T, axis=0, keepdims=True)

    for n in range(4):
        for k in range(2):
            to_sib(yp, yr, yd_s, yd_r, n, k).wait()
        yfar[n] = yp[n, cross] + yr[n, 1]
    y_cross = remote(yfar, ygot, yx_s, yx_r, cross)
    y_cross.start()
    dg_back = [remote(dgp.at[peer], dgr.at[k], dg_s.at[k], dg_r.at[k], peer) for k, peer in enumerate((cross, diag, sib))]

    mine = lax.broadcasted_iota(jnp.int32, (d_ff, PAIR * CAP), 1) < CAP
    last = n_pairs - 1

    def back_h(i):
        slot, at = lax.rem(last - i, AHEAD), pair_rows(last - i)
        g = g_s[at, :]
        dh = jnp.where(mine, dot(wo[slot, 0], g, ((1,), (1,))), dot(wo[slot, 1], g, ((1,), (1,))))
        da = dh.astype(bf).T.astype(f32) * slope[at, :]
        da_s[at, :] = jnp.concatenate([jnp.where(first, da, 0.0), jnp.where(first, 0.0, da)], axis=1).astype(bf)

    def back_x(i):
        slot, at = lax.rem(last - i, AHEAD), pair_rows(last - i)
        wide = jnp.concatenate([wi[slot, 0], wi[slot, 1]], axis=1)
        sp[0, at, :] = dot(wide, da_s[at, :], ((1,), (1,))).astype(bf).T

    back_h(0)
    back_h(1)
    for i in range(2):
        fetch_out(last - AHEAD - i).start()

    def bwd_step(j, _):
        i = 2 * j

        @pl.when(i - 2 >= n_pairs - AHEAD)
        def _():
            for k in range(2):
                fetch_in(last + 2 - i - k).wait()

        @pl.when(i >= n_pairs - AHEAD)
        def _():
            for k in range(2):
                fetch_out(last - i - k).wait()

        back_x(i - 2)
        back_x(i - 1)
        back_h(i)
        back_h(i + 1)
        for k in range(5):
            row = lax.rem(5 * j - 5 + k, 32)
            d, choice = row // 8, lax.rem(row, 8)
            at = rj[choice, d].astype(jnp.int32)
            got = jnp.take_along_axis(dg_tab[...], jnp.maximum(at, 0), axis=1)
            dgp[d, pl.ds(choice, 1), :] = jnp.sum(jnp.where(at >= 0, got, 0.0), axis=0, keepdims=True)

        @pl.when(i < n_pairs - AHEAD)
        def _():
            for k in range(2):
                fetch_out(last - AHEAD - i - k).start()

        @pl.when(i < n_pairs - AHEAD + 2)
        def _():
            for k in range(2):
                fetch_in(last + 2 - AHEAD - i - k).start()
        return 0

    lax.fori_loop(1, n_pairs // 2, bwd_step, 0)
    for copy in dg_back:
        copy.start()
    y_cross.wait()
    for i in range(2):
        fetch_in(i).wait()
    back_x(last - 1)
    back_x(last)

    def dx_send(n, k):
        return remote(dxs.at[n, k], dxr.at[n, k], dd_s.at[n, k], dd_r.at[n, k], sib)

    def dx_rows(n, into, d0, d1):
        lanes = slice(256 * n, 256 * (n + 1))
        chosen = jnp.concatenate([pt[pl.ds(pl.multiple_of(d * 128, 128), 128), :] for d in (d0, d1)], axis=0)
        out = dot(chosen, sp[0, :, lanes])
        into[n, 0] = out[:128]
        into[n, 1] = out[128:]

    for n in range(4):
        dx_rows(n, dxs, sib, diag)
        lanes = slice(256 * n, 256 * (n + 1))
        y_out[:, lanes] = (x[:, lanes].astype(f32) + (yp[n, me] + yr[n, 0] + ygot[n])).astype(bf)
    for n in range(4):
        for k in range(2):
            dx_send(n, k).start()
    for n in range(4):
        dx_rows(n, dxm, me, cross)
    for copy in dg_back:
        copy.wait()
    dg_out[...] = dgp[me] + (dgr[0] + (dgr[1] + dgr[2]))
    for n in range(4):
        for k in range(2):
            dx_send(n, k).wait()
    for n in range(4):
        lanes = slice(256 * n, 256 * (n + 1))
        dx_own[:, lanes] = dxm[n, 0] + dxr[n, 0]
        dx_far[:, lanes] = dxm[n, 1] + dxr[n, 1]
    for copy in small + over + near + far:
        copy.wait_send()


def experts(x, dy, idx_t, gate_t, w_in, w_out):
    n_e, d_model, d_ff = w_in.shape
    slots = n_e * CAP
    bf, f32 = jnp.bfloat16, jnp.float32
    vmem, hbm = pl.BlockSpec(memory_space=pltpu.VMEM), pl.BlockSpec(memory_space=pl.ANY)
    buf, dma = pltpu.VMEM, pltpu.SemaphoreType.DMA
    return pl.pallas_call(
        expert_kernel,
        out_shape=[buf((128, d_model), bf), buf((8, 128), f32), buf((128, d_model), f32), buf((128, d_model), f32),
                   buf((slots, d_model), bf), buf((slots, PAIR * d_ff), bf), buf((slots, d_model), bf), buf((slots, PAIR * d_ff), bf)],
        in_specs=[hbm] * 6,
        out_specs=[vmem] * 8,
        scratch_shapes=[
            buf((128, d_model), bf), buf((128, d_model), bf), buf((8, 128), jnp.int32), buf((8, 128), f32),
            buf((4, 128, d_model), bf), buf((4, 128, d_model), bf), buf((4, 8, 128), jnp.int32), buf((4, 8, 128), f32),
            buf((8, 4, n_e, 128), f32), buf((4, n_e, 128), f32), buf((4, n_e, 128), f32),
            buf((slots, 512), bf), buf((512, slots), bf), buf((slots, 128), f32),
            buf((slots, d_model), bf), buf((slots, d_ff), f32), buf((3, slots, d_model), bf),
            buf((n_e, 128), f32), buf((4, 8, 128), f32), buf((3, 8, 128), f32),
            buf((AHEAD, PAIR, d_model, d_ff), bf), buf((AHEAD, PAIR, d_ff, d_model), bf),
            buf((4, 4, 128, 256), f32), buf((4, 2, 128, 256), f32), buf((4, 128, 256), f32), buf((4, 128, 256), f32),
            buf((4, 2, 128, 256), f32), buf((4, 2, 128, 256), f32), buf((4, 2, 128, 256), f32),
            dma((4,)), dma((AHEAD,)), dma((AHEAD,)), dma((6,)), dma((6,)), dma((2,)), dma((2,)), dma((4,)), dma((4,)),
            dma((4,)), dma((4,)), dma((4, 2)), dma((4, 2)), dma(()), dma(()), dma((4, 2)), dma((4, 2)), dma((3,)), dma((3,))],
        compiler_params=pltpu.CompilerParams(collective_id=0, has_side_effects=True, vmem_limit_bytes=53 * 1024 * 1024),
        cost_estimate=pl.CostEstimate(flops=8 * slots * d_model * d_ff, bytes_accessed=8 * n_e * d_model * d_ff, transcendentals=0),
    )(x, dy, idx_t, gate_t, w_in, w_out)


def weight_kernel(b, h, g, da, y, dg, dw_in, dw_out, y_out, dg_out, ring_in, ring_out, sem_in, sem_out, sem):
    n_steps, d_ff = dw_in.shape[0] // PAIR, dw_in.shape[2]
    passed = [pltpu.make_async_copy(y, y_out, sem.at[0]), pltpu.make_async_copy(dg, dg_out, sem.at[1])]
    for copy in passed:
        copy.start()

    def copy_in(i, p):
        slot = lax.rem(i, RING)
        return pltpu.make_async_copy(ring_in.at[slot, p], dw_in.at[i * PAIR + p], sem_in.at[slot, p])

    def copy_out(i, p):
        slot = lax.rem(i, RING)
        return pltpu.make_async_copy(ring_out.at[slot, p], dw_out.at[i * PAIR + p], sem_out.at[slot, p])

    def step(j, _):
        @pl.when(2 * j >= RING)
        def _():
            for k in range(2):
                for p in range(PAIR):
                    copy_in(2 * j + k - RING, p).wait()
                    copy_out(2 * j + k - RING, p).wait()

        for k in range(2):
            i = 2 * j + k
            slot, at = lax.rem(i, RING), pair_rows(i)
            for p in range(PAIR):
                own = slice(d_ff * p, d_ff * (p + 1))
                ring_in[slot, p] = dot(b[at, :], da[at, own], ((0,), (0,))).astype(jnp.bfloat16)
                copy_in(i, p).start()
                ring_out[slot, p] = dot(h[at, own], g[at, :], ((0,), (0,))).astype(jnp.bfloat16)
                copy_out(i, p).start()
        return 0

    lax.fori_loop(0, n_steps // 2, step, 0)
    for i in range(n_steps - RING, n_steps):
        for p in range(PAIR):
            copy_in(i, p).wait()
            copy_out(i, p).wait()
    for copy in passed:
        copy.wait()


def weight_grads(b, h, g, da, y, dg, n_e):
    d_model, d_ff = b.shape[1], h.shape[1] // PAIR
    bf, shape, dma = jnp.bfloat16, jax.ShapeDtypeStruct, pltpu.SemaphoreType.DMA
    return pl.pallas_call(
        weight_kernel,
        out_shape=[shape((n_e, d_model, d_ff), bf), shape((n_e, d_ff, d_model), bf), shape(y.shape, y.dtype), shape(dg.shape, dg.dtype)],
        in_specs=[pl.BlockSpec(memory_space=pltpu.VMEM)] * 6,
        out_specs=[pl.BlockSpec(memory_space=pl.ANY)] * 4,
        scratch_shapes=[pltpu.VMEM((RING, PAIR, d_model, d_ff), bf), pltpu.VMEM((RING, PAIR, d_ff, d_model), bf),
                        dma((RING, PAIR)), dma((RING, PAIR)), dma((2,))],
        compiler_params=pltpu.CompilerParams(vmem_limit_bytes=40 * 1024 * 1024),
        cost_estimate=pl.CostEstimate(flops=4 * n_e * CAP * d_model * d_ff, bytes_accessed=4 * n_e * d_model * d_ff, transcendentals=0),
    )(b, h, g, da, y, dg)


def solution(mesh):
    tok_spec = P(('data', 'expert'), None)
    weight_spec = P('expert', None, None)
    grad_spec = P(('data', 'expert'), None, None)
    to_cross = [(i, i ^ 2) for i in range(4)]

    def device_pass(x_in, expert_idx, gate_weight, grad_y, w_in, w_out):
        y_mid, dg, dx_own, dx_far, b, h, g, da = experts(x_in, grad_y, expert_idx.T, gate_weight.T, w_in, w_out)
        dx_got = lax.ppermute(dx_far, 'expert', to_cross)
        grad_w_in, grad_w_out, y_out, dg = weight_grads(b, h, g, da, y_mid, dg, w_in.shape[0])
        grad_x = (grad_y.astype(jnp.float32) + (dx_own + dx_got)).astype(jnp.bfloat16)
        return y_out, grad_x, dg.T, grad_w_in, grad_w_out

    return jax.shard_map(device_pass, mesh=mesh,
                         in_specs=(tok_spec, tok_spec, tok_spec, tok_spec, weight_spec, weight_spec),
                         out_specs=(tok_spec, tok_spec, tok_spec, grad_spec, grad_spec), check_vma=False)
```

```python
import functools

import jax
import jax.numpy as jnp
from jax import lax
from jax.experimental import pallas as pl
from jax.experimental.pallas import tpu as pltpu
from jax.sharding import PartitionSpec as P

MESH = pl.DeviceIdType.MESH
CAP = 40
PAIR = 2
RING = 4
AHEAD = 8
PICK, PICK_DY = 640, 640
C0 = 0.7978845608028654
C1 = 0.044715


def dot(a, b, dims=((1,), (0,))):
    return lax.dot_general(a, b, (dims, ((), ())), preferred_element_type=jnp.float32)


def tables(ids_all, first, rj, r0s, r1s):
    eid = lax.broadcasted_iota(jnp.int32, (32, 128), 0) + first
    earlier = (lax.broadcasted_iota(jnp.int32, (128, 128), 0) < lax.broadcasted_iota(jnp.int32, (128, 128), 1)).astype(jnp.bfloat16)
    offset = jnp.zeros((32, 1), jnp.float32)
    for d in range(4):
        ids = ids_all[d]
        hits = [(ids[j:j + 1, :] == eid).astype(jnp.float32) for j in range(8)]
        count = sum(hits[1:], hits[0])
        rank = dot(count.astype(jnp.bfloat16), earlier) + offset
        r0s[d] = rank
        for j in range(8):
            rj[j, d] = jnp.where((hits[j] > 0.0) & (rank < CAP), rank, -1.0)
            rank = rank + hits[j]
        r1s[d] = jnp.minimum(rank, CAP)
        offset = offset + jnp.sum(count, axis=1, keepdims=True)


def pair_rows(q):
    return pl.ds(pl.multiple_of(q * PAIR * CAP, 16), PAIR * CAP)


def expert_kernel(x_hbm, dy_hbm, idx_hbm, gate_hbm, w_in, w_out, y_out, dg_out, dx_own, dx_far, b_s, h_s, g_s, da_s,
                  x, dy, idx, gate, xa, dya, ida, ga, rj, r0s, r1s, pm, pt, gs, o_s, slope, sp, dg_tab, dgp, dgr,
                  wi, wo, yp, yr, yfar, ygot, dxs, dxm, dxr,
                  arg_sem, wi_sem, wo_sem, small_s, small_r, sib_s, sib_r, cross_s, cross_r, fwd_s, fwd_r,
                  yd_s, yd_r, yx_s, yx_r, dd_s, dd_r, dg_s, dg_r):
    me = lax.axis_index("expert")
    sib, cross = me + 1 - 2 * lax.rem(me, 2), lax.rem(me + 2, 4)
    diag, chip = lax.rem(sib + 2, 4), me // 2
    n_pairs = w_in.shape[0] // PAIR
    slots = 32 * CAP
    bf, f32 = jnp.bfloat16, jnp.float32
    d_ff = w_in.shape[2]

    def fetch_in(q):
        slot = lax.rem(q, AHEAD)
        return pltpu.make_async_copy(w_in.at[pl.ds(PAIR * q, PAIR)], wi.at[slot], wi_sem.at[slot])

    def fetch_out(q):
        slot = lax.rem(q, AHEAD)
        return pltpu.make_async_copy(w_out.at[pl.ds(PAIR * q, PAIR)], wo.at[slot], wo_sem.at[slot])

    def remote(src, dst, s, r, peer):
        return pltpu.make_async_remote_copy(src_ref=src, dst_ref=dst, send_sem=s, recv_sem=r,
                                            device_id={"expert": peer}, device_id_type=MESH)

    barrier = pltpu.get_barrier_semaphore()
    for peer in (sib, cross, diag):
        pl.semaphore_signal(barrier, inc=1, device_id={"expert": peer}, device_id_type=MESH)
    args = [pltpu.make_async_copy(src, dst, arg_sem.at[k])
            for k, (src, dst) in enumerate(((idx_hbm, idx), (gate_hbm, gate), (x_hbm, x), (dy_hbm, dy)))]
    for copy in args:
        copy.start()
    for copy in args:
        copy.wait()
    pl.semaphore_wait(barrier, 3)

    small, over, near, far = [], [], [], []
    for k, peer in enumerate((cross, diag, sib)):
        small.append(remote(idx, ida.at[me], small_s.at[2 * k], small_r.at[2 * k], peer))
        small.append(remote(gate, ga.at[me], small_s.at[2 * k + 1], small_r.at[2 * k + 1], peer))
    for a, (src, dst) in enumerate(((x, xa), (dy, dya))):
        for c in range(2):
            rows = pl.ds(64 * c, 64)
            n = 2 * a + c
            over.append(remote(src.at[rows], dst.at[me, rows], cross_s.at[n], cross_r.at[n], cross))
            far.append(remote(dst.at[cross, rows], dst.at[cross, rows], fwd_s.at[n], fwd_r.at[n], sib))
        near.append(remote(src, dst.at[me], sib_s.at[a], sib_r.at[a], sib))
    for copy in small + over[:2] + near[:1] + over[2:] + near[1:]:
        copy.start()
    for q in range(AHEAD):
        fetch_in(q).start()
        fetch_out(q).start()
    xa[me] = x[...]
    dya[me] = dy[...]
    ida[me] = idx[...]
    ga[me] = gate[...]

    def forward(n):
        over[n].wait_recv()
        far[n].start()

    for copy in small:
        copy.wait_recv()
    tables(ida, me * 32, rj, r0s, r1s)
    slot_id = lax.broadcasted_iota(jnp.int32, (CAP, 128), 0).astype(f32)

    def one(q, _):
        inside, total = [], [jnp.zeros((CAP, 128), f32) for _ in range(PAIR)]
        for d in range(4):
            for p in range(PAIR):
                e = pl.ds(q * PAIR + p, 1)
                inside.append(jnp.where((slot_id >= r0s[d, e, :]) & (slot_id < r1s[d, e, :]), 1.0, 0.0))
                for j in range(8):
                    total[p] = jnp.where(slot_id == rj[j, d, e, :], ga[d, j:j + 1, :], total[p])
            pm[pair_rows(q), 128 * d:128 * (d + 1)] = jnp.concatenate(inside[-PAIR:], axis=0).astype(bf)
        gs[pair_rows(q), :] = jnp.broadcast_to(jnp.sum(jnp.concatenate(total, axis=0), axis=1, keepdims=True), (PAIR * CAP, 128))
        return 0

    lax.fori_loop(0, n_pairs, one, 0)
    forward(0)
    near[0].wait_recv()

    def half(devices):
        return pl.ds(pl.multiple_of(devices * 256, 256), 256)

    def pick_near(c, _):
        at = pl.ds(pl.multiple_of(c * PICK, PICK), PICK)
        rows = jnp.concatenate([xa[2 * chip], xa[2 * chip + 1]], axis=0)
        b_s[at, :] = dot(pm[at, half(chip)], rows).astype(bf)
        return 0

    lax.fori_loop(0, slots // PICK, pick_near, 0)
    forward(1)
    far[0].wait_recv()
    far[1].wait_recv()

    for c in range(slots // PICK):
        at = pl.ds(c * PICK, PICK)
        rows = jnp.concatenate([xa[2 - 2 * chip], xa[3 - 2 * chip]], axis=0)
        b_s[at, :] += dot(pm[at, half(1 - chip)], rows).astype(bf)

    first = lax.broadcasted_iota(jnp.int32, (PAIR * CAP, d_ff), 0) < CAP

    def fwd_h(i):
        slot, at = lax.rem(i, AHEAD), pair_rows(i)
        rows = b_s[at, :]
        a = jnp.concatenate([dot(rows, wi[slot, 0])[:CAP], dot(rows, wi[slot, 1])[CAP:]], axis=0)
        th = jnp.tanh(C0 * (a + C1 * (a * a * a)))
        cdf = 0.5 * (1.0 + th)
        slope[at, :] = cdf + 0.5 * a * (1.0 - th * th) * (C0 * (1.0 + 3.0 * C1 * (a * a)))
        h = a * cdf
        h_s[at, :] = jnp.concatenate([jnp.where(first, h, 0.0), jnp.where(first, 0.0, h)], axis=1).astype(bf)

    def fwd_o(i):
        slot, at = lax.rem(i, AHEAD), pair_rows(i)
        o = dot(h_s[at, :], jnp.concatenate([wo[slot, 0], wo[slot, 1]], axis=0)).astype(bf)
        o_s[at, :] = o
        s = o.astype(f32) * jnp.concatenate([gs[at, :]] * 8, axis=1)
        s1 = s.astype(bf)
        s = s - s1.astype(f32)
        s2 = s.astype(bf)
        s = s - s2.astype(f32)
        sp[0, at, :] = s1
        sp[1, at, :] = s2
        sp[2, at, :] = s.astype(bf)

    for i in range(2):
        fetch_in(i).wait()
    fwd_h(0)
    fwd_h(1)
    for i in range(2):
        fetch_in(AHEAD + i).start()

    def fwd_step(j, _):
        i = 2 * j
        for k in range(2):
            fetch_in(i + k).wait()
            fetch_out(i - 2 + k).wait()
        fwd_o(i - 2)
        fwd_o(i - 1)
        fwd_h(i)
        fwd_h(i + 1)
        for k in range(2):
            tile = pl.ds(pl.multiple_of(lax.rem(i - 2 + k, slots // 128) * 128, 128), 128)
            pt[:, tile] = pm[tile, :].astype(f32).T.astype(bf)

        @pl.when(i < n_pairs - AHEAD)
        def _():
            for k in range(2):
                fetch_in(i + AHEAD + k).start()

        @pl.when(i < n_pairs - AHEAD + 2)
        def _():
            for k in range(2):
                fetch_out(i - 2 + AHEAD + k).start()

        for n, when in ((2, 2), (3, 4)):
            @pl.when(j == when)
            def _(n=n):
                forward(n)
        return 0

    lax.fori_loop(1, n_pairs // 2, fwd_step, 0)
    for i in range(n_pairs - 2, n_pairs):
        fetch_out(i).wait()
    fwd_o(n_pairs - 2)
    fwd_o(n_pairs - 1)

    def to_sib(part, got, s, r, n, k):
        return remote(part.at[n, sib if k == 0 else diag], got.at[n, k], s.at[n, k], r.at[n, k], sib)

    def y_part(c, _):
        for n in (2 * c, 2 * c + 1):
            lanes = pl.ds(pl.multiple_of(n * 256, 256), 256)
            out = dot(pt[...], sp[0, :, lanes]) + dot(pt[...], sp[1, :, lanes]) + dot(pt[...], sp[2, :, lanes])
            for d in range(4):
                yp[n, d] = out[128 * d:128 * (d + 1)]

        @pl.when(c > 0)
        def _():
            for n in range(2):
                for k in range(2):
                    to_sib(yp, yr, yd_s, yd_r, n, k).start()
        return 0

    lax.fori_loop(0, 2, y_part, 0)
    near[1].wait_recv()
    far[2].wait_recv()
    far[3].wait_recv()
    for n in range(2, 4):
        for k in range(2):
            to_sib(yp, yr, yd_s, yd_r, n, k).start()

    for c in range(slots // PICK_DY):
        at = pl.ds(c * PICK_DY, PICK_DY)
        part = jnp.zeros((PICK_DY, 128), f32)
        for n in range(4):
            lanes = slice(256 * n, 256 * (n + 1))
            rows = dot(pm[at, :], dya[:, :, lanes].reshape(512, 256))
            g_s[at, lanes] = (rows * jnp.concatenate([gs[at, :]] * 2, axis=1)).astype(bf)
            prod = rows * o_s[at, lanes].astype(f32)
            part = part + (prod[:, :128] + prod[:, 128:])
        for k in range(PICK_DY // CAP):
            dg_tab[pl.ds(c * (PICK_DY // CAP) + k, 1), :CAP] = jnp.sum(part[CAP * k:CAP * (k + 1)].T, axis=0, keepdims=True)

    for n in range(4):
        for k in range(2):
            to_sib(yp, yr, yd_s, yd_r, n, k).wait()
        yfar[n] = yp[n, cross] + yr[n, 1]
    y_cross = remote(yfar, ygot, yx_s, yx_r, cross)
    y_cross.start()
    dg_back = [remote(dgp.at[peer], dgr.at[k], dg_s.at[k], dg_r.at[k], peer) for k, peer in enumerate((cross, diag, sib))]

    mine = lax.broadcasted_iota(jnp.int32, (d_ff, PAIR * CAP), 1) < CAP
    last = n_pairs - 1

    def back_h(i):
        slot, at = lax.rem(last - i, AHEAD), pair_rows(last - i)
        g = g_s[at, :]
        dh = jnp.where(mine, dot(wo[slot, 0], g, ((1,), (1,))), dot(wo[slot, 1], g, ((1,), (1,))))
        da = dh.astype(bf).T.astype(f32) * slope[at, :]
        da_s[at, :] = jnp.concatenate([jnp.where(first, da, 0.0), jnp.where(first, 0.0, da)], axis=1).astype(bf)

    def back_x(i):
        slot, at = lax.rem(last - i, AHEAD), pair_rows(last - i)
        wide = jnp.concatenate([wi[slot, 0], wi[slot, 1]], axis=1)
        sp[0, at, :] = dot(wide, da_s[at, :], ((1,), (1,))).astype(bf).T

    back_h(0)
    back_h(1)
    for i in range(2):
        fetch_out(last - AHEAD - i).start()

    def bwd_step(j, _):
        i = 2 * j

        @pl.when(i - 2 >= n_pairs - AHEAD)
        def _():
            for k in range(2):
                fetch_in(last + 2 - i - k).wait()

        @pl.when(i >= n_pairs - AHEAD)
        def _():
            for k in range(2):
                fetch_out(last - i - k).wait()

        back_x(i - 2)
        back_x(i - 1)
        back_h(i)
        back_h(i + 1)
        for k in range(5):
            row = lax.rem(5 * j - 5 + k, 32)
            d, choice = row // 8, lax.rem(row, 8)
            at = rj[choice, d].astype(jnp.int32)
            got = jnp.take_along_axis(dg_tab[...], jnp.maximum(at, 0), axis=1)
            dgp[d, pl.ds(choice, 1), :] = jnp.sum(jnp.where(at >= 0, got, 0.0), axis=0, keepdims=True)

        @pl.when(i < n_pairs - AHEAD)
        def _():
            for k in range(2):
                fetch_out(last - AHEAD - i - k).start()

        @pl.when(i < n_pairs - AHEAD + 2)
        def _():
            for k in range(2):
                fetch_in(last + 2 - AHEAD - i - k).start()
        return 0

    lax.fori_loop(1, n_pairs // 2, bwd_step, 0)
    for copy in dg_back:
        copy.start()
    y_cross.wait()
    for i in range(2):
        fetch_in(i).wait()
    back_x(last - 1)
    back_x(last)

    def dx_send(n, k):
        return remote(dxs.at[n, k], dxr.at[n, k], dd_s.at[n, k], dd_r.at[n, k], sib)

    def dx_rows(n, into, d0, d1):
        lanes = slice(256 * n, 256 * (n + 1))
        chosen = jnp.concatenate([pt[pl.ds(pl.multiple_of(d * 128, 128), 128), :] for d in (d0, d1)], axis=0)
        out = dot(chosen, sp[0, :, lanes])
        into[n, 0] = out[:128]
        into[n, 1] = out[128:]

    for two in ((0, 1), (2, 3)):
        for n in two:
            dx_rows(n, dxs, sib, diag)
        for n in two:
            lanes = slice(256 * n, 256 * (n + 1))
            y_out[:, lanes] = (x[:, lanes].astype(f32) + (yp[n, me] + yr[n, 0] + ygot[n])).astype(bf)
        for n in two:
            for k in range(2):
                dx_send(n, k).start()
    for n in range(4):
        dx_rows(n, dxm, me, cross)
    for copy in dg_back:
        copy.wait()
    dg_out[...] = dgp[me] + (dgr[0] + (dgr[1] + dgr[2]))
    for n in range(4):
        for k in range(2):
            dx_send(n, k).wait()
    for n in range(4):
        lanes = slice(256 * n, 256 * (n + 1))
        dx_own[:, lanes] = dxm[n, 0] + dxr[n, 0]
        dx_far[:, lanes] = dxm[n, 1] + dxr[n, 1]
    for copy in small + over + near + far:
        copy.wait_send()


def experts(x, dy, idx_t, gate_t, w_in, w_out):
    n_e, d_model, d_ff = w_in.shape
    slots = n_e * CAP
    bf, f32 = jnp.bfloat16, jnp.float32
    vmem, hbm = pl.BlockSpec(memory_space=pltpu.VMEM), pl.BlockSpec(memory_space=pl.ANY)
    buf, dma = pltpu.VMEM, pltpu.SemaphoreType.DMA
    return pl.pallas_call(
        expert_kernel,
        out_shape=[buf((128, d_model), bf), buf((8, 128), f32), buf((128, d_model), f32), buf((128, d_model), f32),
                   buf((slots, d_model), bf), buf((slots, PAIR * d_ff), bf), buf((slots, d_model), bf), buf((slots, PAIR * d_ff), bf)],
        in_specs=[hbm] * 6,
        out_specs=[vmem] * 8,
        scratch_shapes=[
            buf((128, d_model), bf), buf((128, d_model), bf), buf((8, 128), jnp.int32), buf((8, 128), f32),
            buf((4, 128, d_model), bf), buf((4, 128, d_model), bf), buf((4, 8, 128), jnp.int32), buf((4, 8, 128), f32),
            buf((8, 4, n_e, 128), f32), buf((4, n_e, 128), f32), buf((4, n_e, 128), f32),
            buf((slots, 512), bf), buf((512, slots), bf), buf((slots, 128), f32),
            buf((slots, d_model), bf), buf((slots, d_ff), f32), buf((3, slots, d_model), bf),
            buf((n_e, 128), f32), buf((4, 8, 128), f32), buf((3, 8, 128), f32),
            buf((AHEAD, PAIR, d_model, d_ff), bf), buf((AHEAD, PAIR, d_ff, d_model), bf),
            buf((4, 4, 128, 256), f32), buf((4, 2, 128, 256), f32), buf((4, 128, 256), f32), buf((4, 128, 256), f32),
            buf((4, 2, 128, 256), f32), buf((4, 2, 128, 256), f32), buf((4, 2, 128, 256), f32),
            dma((4,)), dma((AHEAD,)), dma((AHEAD,)), dma((6,)), dma((6,)), dma((2,)), dma((2,)), dma((4,)), dma((4,)),
            dma((4,)), dma((4,)), dma((4, 2)), dma((4, 2)), dma(()), dma(()), dma((4, 2)), dma((4, 2)), dma((3,)), dma((3,))],
        compiler_params=pltpu.CompilerParams(collective_id=0, has_side_effects=True, vmem_limit_bytes=53 * 1024 * 1024),
        cost_estimate=pl.CostEstimate(flops=8 * slots * d_model * d_ff, bytes_accessed=8 * n_e * d_model * d_ff, transcendentals=0),
    )(x, dy, idx_t, gate_t, w_in, w_out)


def weight_kernel(b, h, g, da, y, dg, dw_in, dw_out, y_out, dg_out, ring_in, ring_out, sem_in, sem_out, sem):
    n_steps, d_ff = dw_in.shape[0] // PAIR, dw_in.shape[2]
    passed = [pltpu.make_async_copy(y, y_out, sem.at[0]), pltpu.make_async_copy(dg, dg_out, sem.at[1])]
    for copy in passed:
        copy.start()

    def copy_in(i, p):
        slot = lax.rem(i, RING)
        return pltpu.make_async_copy(ring_in.at[slot, p], dw_in.at[i * PAIR + p], sem_in.at[slot, p])

    def copy_out(i, p):
        slot = lax.rem(i, RING)
        return pltpu.make_async_copy(ring_out.at[slot, p], dw_out.at[i * PAIR + p], sem_out.at[slot, p])

    def step(j, _):
        @pl.when(2 * j >= RING)
        def _():
            for k in range(2):
                for p in range(PAIR):
                    copy_in(2 * j + k - RING, p).wait()
                    copy_out(2 * j + k - RING, p).wait()

        for k in range(2):
            i = 2 * j + k
            slot, at = lax.rem(i, RING), pair_rows(i)
            for p in range(PAIR):
                own = slice(d_ff * p, d_ff * (p + 1))
                ring_in[slot, p] = dot(b[at, :], da[at, own], ((0,), (0,))).astype(jnp.bfloat16)
                copy_in(i, p).start()
                ring_out[slot, p] = dot(h[at, own], g[at, :], ((0,), (0,))).astype(jnp.bfloat16)
                copy_out(i, p).start()
        return 0

    lax.fori_loop(0, n_steps // 2, step, 0)
    for i in range(n_steps - RING, n_steps):
        for p in range(PAIR):
            copy_in(i, p).wait()
            copy_out(i, p).wait()
    for copy in passed:
        copy.wait()


def weight_grads(b, h, g, da, y, dg, n_e):
    d_model, d_ff = b.shape[1], h.shape[1] // PAIR
    bf, shape, dma = jnp.bfloat16, jax.ShapeDtypeStruct, pltpu.SemaphoreType.DMA
    return pl.pallas_call(
        weight_kernel,
        out_shape=[shape((n_e, d_model, d_ff), bf), shape((n_e, d_ff, d_model), bf), shape(y.shape, y.dtype), shape(dg.shape, dg.dtype)],
        in_specs=[pl.BlockSpec(memory_space=pltpu.VMEM)] * 6,
        out_specs=[pl.BlockSpec(memory_space=pl.ANY)] * 4,
        scratch_shapes=[pltpu.VMEM((RING, PAIR, d_model, d_ff), bf), pltpu.VMEM((RING, PAIR, d_ff, d_model), bf),
                        dma((RING, PAIR)), dma((RING, PAIR)), dma((2,))],
        compiler_params=pltpu.CompilerParams(vmem_limit_bytes=40 * 1024 * 1024),
        cost_estimate=pl.CostEstimate(flops=4 * n_e * CAP * d_model * d_ff, bytes_accessed=4 * n_e * d_model * d_ff, transcendentals=0),
    )(b, h, g, da, y, dg)


def solution(mesh):
    tok_spec = P(('data', 'expert'), None)
    weight_spec = P('expert', None, None)
    grad_spec = P(('data', 'expert'), None, None)
    to_cross = [(i, i ^ 2) for i in range(4)]

    def device_pass(x_in, expert_idx, gate_weight, grad_y, w_in, w_out):
        y_mid, dg, dx_own, dx_far, b, h, g, da = experts(x_in, grad_y, expert_idx.T, gate_weight.T, w_in, w_out)
        dx_got = lax.ppermute(dx_far, 'expert', to_cross)
        grad_w_in, grad_w_out, y_out, dg = weight_grads(b, h, g, da, y_mid, dg, w_in.shape[0])
        grad_x = (grad_y.astype(jnp.float32) + (dx_own + dx_got)).astype(jnp.bfloat16)
        return y_out, grad_x, dg.T, grad_w_in, grad_w_out

    return jax.shard_map(device_pass, mesh=mesh,
                         in_specs=(tok_spec, tok_spec, tok_spec, tok_spec, weight_spec, weight_spec),
                         out_specs=(tok_spec, tok_spec, tok_spec, grad_spec, grad_spec), check_vma=False)
```

```python
import functools

import jax
import jax.numpy as jnp
from jax import lax
from jax.experimental import pallas as pl
from jax.experimental.pallas import tpu as pltpu
from jax.sharding import PartitionSpec as P

MESH = pl.DeviceIdType.MESH
CAP = 40
PAIR = 2
RING = 4
AHEAD, AHEAD_IN = 8, 8
PICK, PICK_DY = 640, 640
C0 = 0.7978845608028654
C1 = 0.044715


def dot(a, b, dims=((1,), (0,))):
    return lax.dot_general(a, b, (dims, ((), ())), preferred_element_type=jnp.float32)


def tables(ids_all, first, rj, r0s, r1s):
    eid = lax.broadcasted_iota(jnp.int32, (32, 128), 0) + first
    earlier = (lax.broadcasted_iota(jnp.int32, (128, 128), 0) < lax.broadcasted_iota(jnp.int32, (128, 128), 1)).astype(jnp.bfloat16)
    offset = jnp.zeros((32, 1), jnp.float32)
    for d in range(4):
        ids = ids_all[d]
        hits = [(ids[j:j + 1, :] == eid).astype(jnp.float32) for j in range(8)]
        count = sum(hits[1:], hits[0])
        rank = dot(count.astype(jnp.bfloat16), earlier) + offset
        r0s[d] = rank
        for j in range(8):
            rj[j, d] = jnp.where((hits[j] > 0.0) & (rank < CAP), rank, -1.0)
            rank = rank + hits[j]
        r1s[d] = jnp.minimum(rank, CAP)
        offset = offset + jnp.sum(count, axis=1, keepdims=True)


def pair_rows(q):
    return pl.ds(pl.multiple_of(q * PAIR * CAP, 16), PAIR * CAP)


def expert_kernel(x_hbm, dy_hbm, idx_hbm, gate_hbm, w_in, w_out, y_out, dg_out, dx_own, dx_far, b_s, h_s, g_s, da_s,
                  x, dy, idx, gate, xa, dya, ida, ga, rj, r0s, r1s, pm, pt, gs, o_s, slope, sp, dg_tab, dgp, dgr,
                  wi, wo, yp, yr, yfar, ygot, dxs, dxr,
                  arg_sem, wi_sem, wo_sem, small_s, small_r, sib_s, sib_r, cross_s, cross_r, fwd_s, fwd_r,
                  yd_s, yd_r, yx_s, yx_r, dd_s, dd_r, dg_s, dg_r):
    me = lax.axis_index("expert")
    sib, cross = me + 1 - 2 * lax.rem(me, 2), lax.rem(me + 2, 4)
    diag, chip = lax.rem(sib + 2, 4), me // 2
    n_pairs = w_in.shape[0] // PAIR
    slots = 32 * CAP
    bf, f32 = jnp.bfloat16, jnp.float32
    d_ff = w_in.shape[2]

    def fetch_in(q):
        slot = lax.rem(q, AHEAD_IN)
        return pltpu.make_async_copy(w_in.at[pl.ds(PAIR * q, PAIR)], wi.at[slot], wi_sem.at[slot])

    def fetch_out(q):
        slot = lax.rem(q, AHEAD)
        return pltpu.make_async_copy(w_out.at[pl.ds(PAIR * q, PAIR)], wo.at[slot], wo_sem.at[slot])

    def remote(src, dst, s, r, peer):
        return pltpu.make_async_remote_copy(src_ref=src, dst_ref=dst, send_sem=s, recv_sem=r,
                                            device_id={"expert": peer}, device_id_type=MESH)

    barrier = pltpu.get_barrier_semaphore()
    for peer in (sib, cross, diag):
        pl.semaphore_signal(barrier, inc=1, device_id={"expert": peer}, device_id_type=MESH)
    args = [pltpu.make_async_copy(src, dst, arg_sem.at[k])
            for k, (src, dst) in enumerate(((idx_hbm, idx), (gate_hbm, gate), (x_hbm, x), (dy_hbm, dy)))]
    for copy in args:
        copy.start()
    for copy in args:
        copy.wait()
    pl.semaphore_wait(barrier, 3)

    small, over, near, far = [], [], [], []
    for k, peer in enumerate((cross, diag, sib)):
        small.append(remote(idx, ida.at[me], small_s.at[2 * k], small_r.at[2 * k], peer))
        small.append(remote(gate, ga.at[me], small_s.at[2 * k + 1], small_r.at[2 * k + 1], peer))
    for a, (src, dst) in enumerate(((x, xa), (dy, dya))):
        for c in range(2):
            rows = pl.ds(64 * c, 64)
            n = 2 * a + c
            over.append(remote(src.at[rows], dst.at[me, rows], cross_s.at[n], cross_r.at[n], cross))
            far.append(remote(dst.at[cross, rows], dst.at[cross, rows], fwd_s.at[n], fwd_r.at[n], sib))
        near.append(remote(src, dst.at[me], sib_s.at[a], sib_r.at[a], sib))
    for copy in small + over[:2] + near[:1] + over[2:] + near[1:]:
        copy.start()
    for q in range(AHEAD):
        fetch_in(q).start()
        fetch_out(q).start()
    for q in range(AHEAD, AHEAD_IN):
        fetch_in(q).start()
    xa[me] = x[...]
    dya[me] = dy[...]
    ida[me] = idx[...]
    ga[me] = gate[...]

    def forward(n):
        over[n].wait_recv()
        far[n].start()

    for copy in small:
        copy.wait_recv()
    tables(ida, me * 32, rj, r0s, r1s)
    slot_id = lax.broadcasted_iota(jnp.int32, (CAP, 128), 0).astype(f32)

    def one(q, _):
        inside, total = [], [jnp.zeros((CAP, 128), f32) for _ in range(PAIR)]
        for d in range(4):
            for p in range(PAIR):
                e = pl.ds(q * PAIR + p, 1)
                inside.append(jnp.where((slot_id >= r0s[d, e, :]) & (slot_id < r1s[d, e, :]), 1.0, 0.0))
                for j in range(8):
                    total[p] = jnp.where(slot_id == rj[j, d, e, :], ga[d, j:j + 1, :], total[p])
            pm[pair_rows(q), 128 * d:128 * (d + 1)] = jnp.concatenate(inside[-PAIR:], axis=0).astype(bf)
        gs[pair_rows(q), :] = jnp.broadcast_to(jnp.sum(jnp.concatenate(total, axis=0), axis=1, keepdims=True), (PAIR * CAP, 128))
        return 0

    lax.fori_loop(0, n_pairs, one, 0)
    forward(0)
    near[0].wait_recv()

    def half(devices):
        return pl.ds(pl.multiple_of(devices * 256, 256), 256)

    def pick_near(c, _):
        at = pl.ds(pl.multiple_of(c * PICK, PICK), PICK)
        rows = jnp.concatenate([xa[2 * chip], xa[2 * chip + 1]], axis=0)
        b_s[at, :] = dot(pm[at, half(chip)], rows).astype(bf)
        return 0

    lax.fori_loop(0, slots // PICK, pick_near, 0)
    forward(1)
    far[0].wait_recv()
    far[1].wait_recv()

    for c in range(slots // PICK):
        at = pl.ds(c * PICK, PICK)
        rows = jnp.concatenate([xa[2 - 2 * chip], xa[3 - 2 * chip]], axis=0)
        b_s[at, :] += dot(pm[at, half(1 - chip)], rows).astype(bf)

    first = lax.broadcasted_iota(jnp.int32, (PAIR * CAP, d_ff), 0) < CAP

    def fwd_h(i):
        slot, at = lax.rem(i, AHEAD_IN), pair_rows(i)
        rows = b_s[at, :]
        a = jnp.concatenate([dot(rows, wi[slot, 0])[:CAP], dot(rows, wi[slot, 1])[CAP:]], axis=0)
        th = jnp.tanh(C0 * (a + C1 * (a * a * a)))
        cdf = 0.5 * (1.0 + th)
        slope[at, :] = cdf + 0.5 * a * (1.0 - th * th) * (C0 * (1.0 + 3.0 * C1 * (a * a)))
        h = a * cdf
        h_s[at, :] = jnp.concatenate([jnp.where(first, h, 0.0), jnp.where(first, 0.0, h)], axis=1).astype(bf)

    def fwd_o(i):
        slot, at = lax.rem(i, AHEAD), pair_rows(i)
        o = dot(h_s[at, :], jnp.concatenate([wo[slot, 0], wo[slot, 1]], axis=0)).astype(bf)
        o_s[at, :] = o
        s = o.astype(f32) * jnp.concatenate([gs[at, :]] * 8, axis=1)
        s1 = s.astype(bf)
        s = s - s1.astype(f32)
        s2 = s.astype(bf)
        s = s - s2.astype(f32)
        sp[0, at, :] = s1
        sp[1, at, :] = s2
        sp[2, at, :] = s.astype(bf)

    for i in range(2):
        fetch_in(i).wait()
    fwd_h(0)
    fwd_h(1)
    for i in range(2):
        fetch_in(AHEAD_IN + i).start()

    def fwd_step(j, _):
        i = 2 * j
        for k in range(2):
            fetch_in(i + k).wait()
            fetch_out(i - 2 + k).wait()
        fwd_o(i - 2)
        fwd_o(i - 1)
        fwd_h(i)
        fwd_h(i + 1)
        for k in range(2):
            tile = pl.ds(pl.multiple_of(lax.rem(i - 2 + k, slots // 128) * 128, 128), 128)
            pt[:, tile] = pm[tile, :].astype(f32).T.astype(bf)

        @pl.when(i < n_pairs - AHEAD_IN)
        def _():
            for k in range(2):
                fetch_in(i + AHEAD_IN + k).start()

        @pl.when(i < n_pairs - AHEAD + 2)
        def _():
            for k in range(2):
                fetch_out(i - 2 + AHEAD + k).start()

        for n, when in ((2, 2), (3, 4)):
            @pl.when(j == when)
            def _(n=n):
                forward(n)
        return 0

    lax.fori_loop(1, n_pairs // 2, fwd_step, 0)
    for i in range(n_pairs - 2, n_pairs):
        fetch_out(i).wait()
    fwd_o(n_pairs - 2)
    fwd_o(n_pairs - 1)

    def to_sib(part, got, s, r, n, k):
        return remote(part.at[n, sib if k == 0 else diag], got.at[n, k], s.at[n, k], r.at[n, k], sib)

    def y_part(c, _):
        for n in (2 * c, 2 * c + 1):
            lanes = pl.ds(pl.multiple_of(n * 256, 256), 256)
            out = dot(pt[...], sp[0, :, lanes]) + dot(pt[...], sp[1, :, lanes]) + dot(pt[...], sp[2, :, lanes])
            for d in range(4):
                yp[n, d] = out[128 * d:128 * (d + 1)]

        @pl.when(c > 0)
        def _():
            for n in range(2):
                for k in range(2):
                    to_sib(yp, yr, yd_s, yd_r, n, k).start()
        return 0

    lax.fori_loop(0, 2, y_part, 0)
    near[1].wait_recv()
    far[2].wait_recv()
    far[3].wait_recv()
    for n in range(2, 4):
        for k in range(2):
            to_sib(yp, yr, yd_s, yd_r, n, k).start()

    for c in range(slots // PICK_DY):
        at = pl.ds(c * PICK_DY, PICK_DY)
        part = jnp.zeros((PICK_DY, 128), f32)
        for n in range(4):
            lanes = slice(256 * n, 256 * (n + 1))
            rows = dot(pm[at, :], dya[:, :, lanes].reshape(512, 256))
            g_s[at, lanes] = (rows * jnp.concatenate([gs[at, :]] * 2, axis=1)).astype(bf)
            prod = rows * o_s[at, lanes].astype(f32)
            part = part + (prod[:, :128] + prod[:, 128:])
        for k in range(PICK_DY // CAP):
            dg_tab[pl.ds(c * (PICK_DY // CAP) + k, 1), :CAP] = jnp.sum(part[CAP * k:CAP * (k + 1)].T, axis=0, keepdims=True)

    for n in range(4):
        for k in range(2):
            to_sib(yp, yr, yd_s, yd_r, n, k).wait()
        yfar[n] = yp[n, cross] + yr[n, 1]
    y_cross = remote(yfar, ygot, yx_s, yx_r, cross)
    y_cross.start()
    dg_back = [remote(dgp.at[peer], dgr.at[k], dg_s.at[k], dg_r.at[k], peer) for k, peer in enumerate((cross, diag, sib))]

    mine = lax.broadcasted_iota(jnp.int32, (d_ff, PAIR * CAP), 1) < CAP
    last = n_pairs - 1

    def back_h(i):
        slot, at = lax.rem(last - i, AHEAD), pair_rows(last - i)
        g = g_s[at, :]
        dh = jnp.where(mine, dot(wo[slot, 0], g, ((1,), (1,))), dot(wo[slot, 1], g, ((1,), (1,))))
        da = dh.astype(bf).T.astype(f32) * slope[at, :]
        da_s[at, :] = jnp.concatenate([jnp.where(first, da, 0.0), jnp.where(first, 0.0, da)], axis=1).astype(bf)

    def back_x(i):
        slot, at = lax.rem(last - i, AHEAD_IN), pair_rows(last - i)
        wide = jnp.concatenate([wi[slot, 0], wi[slot, 1]], axis=1)
        sp[0, at, :] = dot(wide, da_s[at, :], ((1,), (1,))).astype(bf).T

    back_h(0)
    back_h(1)
    for i in range(2):
        fetch_out(last - AHEAD - i).start()

    def bwd_step(j, _):
        i = 2 * j

        @pl.when(i - 2 >= AHEAD_IN)
        def _():
            for k in range(2):
                fetch_in(last + 2 - i - k).wait()

        @pl.when(i >= AHEAD)
        def _():
            for k in range(2):
                fetch_out(last - i - k).wait()

        back_x(i - 2)
        back_x(i - 1)
        back_h(i)
        back_h(i + 1)
        for k in range(5):
            row = lax.rem(5 * j - 5 + k, 32)
            d, choice = row // 8, lax.rem(row, 8)
            at = rj[choice, d].astype(jnp.int32)
            got = jnp.take_along_axis(dg_tab[...], jnp.maximum(at, 0), axis=1)
            dgp[d, pl.ds(choice, 1), :] = jnp.sum(jnp.where(at >= 0, got, 0.0), axis=0, keepdims=True)

        @pl.when(i < n_pairs - AHEAD)
        def _():
            for k in range(2):
                fetch_out(last - AHEAD - i - k).start()

        @pl.when(i < n_pairs - AHEAD_IN + 2)
        def _():
            for k in range(2):
                fetch_in(last + 2 - AHEAD_IN - i - k).start()
        return 0

    lax.fori_loop(1, n_pairs // 2, bwd_step, 0)
    for copy in dg_back:
        copy.start()
    y_cross.wait()
    for i in range(2):
        fetch_in(i).wait()
    back_x(last - 1)
    back_x(last)

    def dx_send(n, k):
        return remote(dxs.at[n, k], dxr.at[n, k], dd_s.at[n, k], dd_r.at[n, k], sib)

    def dx_rows(n, d0, d1):
        lanes = slice(256 * n, 256 * (n + 1))
        chosen = jnp.concatenate([pt[pl.ds(pl.multiple_of(d * 128, 128), 128), :] for d in (d0, d1)], axis=0)
        return dot(chosen, sp[0, :, lanes])

    for two in ((0, 1), (2, 3)):
        for n in two:
            out = dx_rows(n, sib, diag)
            dxs[n, 0] = out[:128]
            dxs[n, 1] = out[128:]
        for n in two:
            lanes = slice(256 * n, 256 * (n + 1))
            y_out[:, lanes] = (x[:, lanes].astype(f32) + (yp[n, me] + yr[n, 0] + ygot[n])).astype(bf)
        for n in two:
            for k in range(2):
                dx_send(n, k).start()
    for n in range(4):
        out = dx_rows(n, me, cross)
        lanes = slice(256 * n, 256 * (n + 1))
        dx_own[:, lanes] = out[:128]
        dx_far[:, lanes] = out[128:]
    for copy in dg_back:
        copy.wait()
    dg_out[...] = dgp[me] + (dgr[0] + (dgr[1] + dgr[2]))
    for n in range(4):
        for k in range(2):
            dx_send(n, k).wait()
    for n in range(4):
        lanes = slice(256 * n, 256 * (n + 1))
        dx_own[:, lanes] += dxr[n, 0]
        dx_far[:, lanes] += dxr[n, 1]
    for copy in small + over + near + far:
        copy.wait_send()


def experts(x, dy, idx_t, gate_t, w_in, w_out):
    n_e, d_model, d_ff = w_in.shape
    slots = n_e * CAP
    bf, f32 = jnp.bfloat16, jnp.float32
    vmem, hbm = pl.BlockSpec(memory_space=pltpu.VMEM), pl.BlockSpec(memory_space=pl.ANY)
    buf, dma = pltpu.VMEM, pltpu.SemaphoreType.DMA
    return pl.pallas_call(
        expert_kernel,
        out_shape=[buf((128, d_model), bf), buf((8, 128), f32), buf((128, d_model), f32), buf((128, d_model), f32),
                   buf((slots, d_model), bf), buf((slots, PAIR * d_ff), bf), buf((slots, d_model), bf), buf((slots, PAIR * d_ff), bf)],
        in_specs=[hbm] * 6,
        out_specs=[vmem] * 8,
        scratch_shapes=[
            buf((128, d_model), bf), buf((128, d_model), bf), buf((8, 128), jnp.int32), buf((8, 128), f32),
            buf((4, 128, d_model), bf), buf((4, 128, d_model), bf), buf((4, 8, 128), jnp.int32), buf((4, 8, 128), f32),
            buf((8, 4, n_e, 128), f32), buf((4, n_e, 128), f32), buf((4, n_e, 128), f32),
            buf((slots, 512), bf), buf((512, slots), bf), buf((slots, 128), f32),
            buf((slots, d_model), bf), buf((slots, d_ff), f32), buf((3, slots, d_model), bf),
            buf((n_e, 128), f32), buf((4, 8, 128), f32), buf((3, 8, 128), f32),
            buf((AHEAD_IN, PAIR, d_model, d_ff), bf), buf((AHEAD, PAIR, d_ff, d_model), bf),
            buf((4, 4, 128, 256), f32), buf((4, 2, 128, 256), f32), buf((4, 128, 256), f32), buf((4, 128, 256), f32),
            buf((4, 2, 128, 256), f32), buf((4, 2, 128, 256), f32),
            dma((4,)), dma((AHEAD_IN,)), dma((AHEAD,)), dma((6,)), dma((6,)), dma((2,)), dma((2,)), dma((4,)), dma((4,)),
            dma((4,)), dma((4,)), dma((4, 2)), dma((4, 2)), dma(()), dma(()), dma((4, 2)), dma((4, 2)), dma((3,)), dma((3,))],
        compiler_params=pltpu.CompilerParams(collective_id=0, has_side_effects=True, vmem_limit_bytes=53 * 1024 * 1024),
        cost_estimate=pl.CostEstimate(flops=8 * slots * d_model * d_ff, bytes_accessed=8 * n_e * d_model * d_ff, transcendentals=0),
    )(x, dy, idx_t, gate_t, w_in, w_out)


def weight_kernel(b, h, g, da, y, dg, dw_in, dw_out, y_out, dg_out, ring_in, ring_out, sem_in, sem_out, sem):
    n_steps, d_ff = dw_in.shape[0] // PAIR, dw_in.shape[2]
    passed = [pltpu.make_async_copy(y, y_out, sem.at[0]), pltpu.make_async_copy(dg, dg_out, sem.at[1])]
    for copy in passed:
        copy.start()

    def copy_in(i, p):
        slot = lax.rem(i, RING)
        return pltpu.make_async_copy(ring_in.at[slot, p], dw_in.at[i * PAIR + p], sem_in.at[slot, p])

    def copy_out(i, p):
        slot = lax.rem(i, RING)
        return pltpu.make_async_copy(ring_out.at[slot, p], dw_out.at[i * PAIR + p], sem_out.at[slot, p])

    def step(j, _):
        @pl.when(2 * j >= RING)
        def _():
            for k in range(2):
                for p in range(PAIR):
                    copy_in(2 * j + k - RING, p).wait()
                    copy_out(2 * j + k - RING, p).wait()

        for k in range(2):
            i = 2 * j + k
            slot, at = lax.rem(i, RING), pair_rows(i)
            for p in range(PAIR):
                own = slice(d_ff * p, d_ff * (p + 1))
                ring_in[slot, p] = dot(b[at, :], da[at, own], ((0,), (0,))).astype(jnp.bfloat16)
                copy_in(i, p).start()
                ring_out[slot, p] = dot(h[at, own], g[at, :], ((0,), (0,))).astype(jnp.bfloat16)
                copy_out(i, p).start()
        return 0

    lax.fori_loop(0, n_steps // 2, step, 0)
    for i in range(n_steps - RING, n_steps):
        for p in range(PAIR):
            copy_in(i, p).wait()
            copy_out(i, p).wait()
    for copy in passed:
        copy.wait()


def weight_grads(b, h, g, da, y, dg, n_e):
    d_model, d_ff = b.shape[1], h.shape[1] // PAIR
    bf, shape, dma = jnp.bfloat16, jax.ShapeDtypeStruct, pltpu.SemaphoreType.DMA
    return pl.pallas_call(
        weight_kernel,
        out_shape=[shape((n_e, d_model, d_ff), bf), shape((n_e, d_ff, d_model), bf), shape(y.shape, y.dtype), shape(dg.shape, dg.dtype)],
        in_specs=[pl.BlockSpec(memory_space=pltpu.VMEM)] * 6,
        out_specs=[pl.BlockSpec(memory_space=pl.ANY)] * 4,
        scratch_shapes=[pltpu.VMEM((RING, PAIR, d_model, d_ff), bf), pltpu.VMEM((RING, PAIR, d_ff, d_model), bf),
                        dma((RING, PAIR)), dma((RING, PAIR)), dma((2,))],
        compiler_params=pltpu.CompilerParams(vmem_limit_bytes=40 * 1024 * 1024),
        cost_estimate=pl.CostEstimate(flops=4 * n_e * CAP * d_model * d_ff, bytes_accessed=4 * n_e * d_model * d_ff, transcendentals=0),
    )(b, h, g, da, y, dg)


def solution(mesh):
    tok_spec = P(('data', 'expert'), None)
    weight_spec = P('expert', None, None)
    grad_spec = P(('data', 'expert'), None, None)
    to_cross = [(i, i ^ 2) for i in range(4)]

    def device_pass(x_in, expert_idx, gate_weight, grad_y, w_in, w_out):
        y_mid, dg, dx_own, dx_far, b, h, g, da = experts(x_in, grad_y, expert_idx.T, gate_weight.T, w_in, w_out)
        dx_got = lax.ppermute(dx_far, 'expert', to_cross)
        grad_w_in, grad_w_out, y_out, dg = weight_grads(b, h, g, da, y_mid, dg, w_in.shape[0])
        grad_x = (grad_y.astype(jnp.float32) + (dx_own + dx_got)).astype(jnp.bfloat16)
        return y_out, grad_x, dg.T, grad_w_in, grad_w_out

    return jax.shard_map(device_pass, mesh=mesh,
                         in_specs=(tok_spec, tok_spec, tok_spec, tok_spec, weight_spec, weight_spec),
                         out_specs=(tok_spec, tok_spec, tok_spec, grad_spec, grad_spec), check_vma=False)
```
